128 devices in a mesh: gx: 16 (over x, z), gy: 4 (over y), gz: 2 (over core).
Axes of the slice: x: 4, y: 4, z: 4, core: 2. Of those that a mesh axis runs over, the one named last changes fastest.
Arguments:
- u_old: float32 [3, 128, 32, 256], P(None, 'gx', 'gy', 'gz'), may hold values from -1.2 to 1.2
- u_trial: float32 [3, 128, 32, 256], P(None, 'gx', 'gy', 'gz'), may hold values from -3.6 to 3.6
- jacobian_inverse: float32 [3, 3, 128, 32, 256], P(None, None, 'gx', 'gy', 'gz'), may hold values from -0.6 to 1.5
- tile_base: int32 [8192], P(('gx', 'gy', 'gz')), may hold values from 0 to 63
- pair_codes: int32 [4, 8192, 128], P(None, ('gx', 'gy', 'gz')), may hold values from 0 to 127, as said below
- pair_groups: int32 [8192, 128], P(('gx', 'gy', 'gz')), may hold values from 0 to 2, as said below
Outputs:
- u_final: float32 [3, 128, 32, 256], P(None, 'gx', 'gy', 'gz')
- residual_norms: float32 [3], replicated
The draws below stay inside these ranges and needn't reach their ends.
Inputs may be any that keep to these rules, and one draw needn't show every extreme that they name: `pair_groups`: on each device the tiles that hold a nonempty slot come first, and their first slot is never empty; every slot of the later tiles is 2. A device holds between 16 and 64 such tiles, and some device holds 64. `pair_codes`: Rows: first node 0 to 127, second direction 0 to 5, third offset 0 to 26, fourth direction 0 to 5; every node of a pair lies in the device's cells extended by one cell on every side.
All inputs are finite; a program needn't handle non-finite values.
Results may differ from the reference program's by a relative error of at most 0.0003.
Values sent between devices are 32-bit elements; how exact they have to be, the bound alone decides.
A program may use at most 64 MiB of HBM per device.

```python
import jax
import jax.numpy as jnp
from jax import lax

BX = 8
BY = 8
BZ = 128
ITERS = 3
TILES = 64
TILES_ALL = 8192
NX = 128
NY = 32
NZ = 256
N_GX = 16
N_GY = 4
N_GZ = 2


def tile_layout(key):
    keys = jax.random.split(jax.random.fold_in(key, 7), 5)
    blocks_y = BY // 4
    blocks_z = BZ // 8
    tile_anchor = jax.random.randint(keys[0], (TILES_ALL,), 0, BX // 4 * blocks_y * blocks_z)
    inside = jax.random.randint(keys[1], (TILES_ALL, 128), 0, 128)
    along_code = jax.random.randint(keys[2], (TILES_ALL, 128), 0, 6)
    offset = jax.random.randint(keys[3], (TILES_ALL, 128), 0, 27)
    across_code = jax.random.randint(keys[4], (TILES_ALL, 128), 0, 6)
    anchor = tile_anchor[:, None]
    block_x = anchor // (blocks_y * blocks_z)
    block_y = anchor // blocks_z % blocks_y
    block_z = anchor % blocks_z
    third_x = block_x * 4 + inside // 32 + 1 + offset // 9 - 1
    third_y = block_y * 4 + inside // 8 % 4 + 1 + offset // 3 % 3 - 1
    third_z = block_z * 8 + inside % 8 + 1 + offset % 3 - 1
    which_axis = across_code // 2
    negative = across_code % 2 == 1
    coordinate = jnp.where(which_axis == 0, third_x, jnp.where(which_axis == 1, third_y, third_z))
    limit = jnp.where(which_axis == 0, BX + 1, jnp.where(which_axis == 1, BY + 1, BZ + 1))
    fixed_code = jnp.where(negative & (coordinate == 0), across_code - 1, across_code)
    fixed_code = jnp.where(jnp.logical_not(negative) & (coordinate == limit), across_code + 1, fixed_code)
    codes = jnp.stack([inside, along_code, offset, fixed_code]).astype(jnp.int32)
    return (tile_anchor.astype(jnp.int32), codes)


def draw_tile_base(key, part):
    return tile_layout(key)[0]


def draw_pair_codes(key, part):
    return tile_layout(key)[1]


def draw_pair_groups(key, part):
    keys = jax.random.split(jax.random.fold_in(key, 13), 4)
    device_count = TILES_ALL // TILES
    spread = jax.random.randint(keys[0], (device_count,), 0, 1024)
    live_count = TILES // 4 + 3 * TILES // 4 * spread * spread // (1024 * 1024)
    fullest = jax.random.randint(keys[1], (), 0, device_count)
    live_count = jnp.where(jnp.arange(device_count) == fullest, TILES, live_count)
    live_count = jnp.maximum(live_count, 1)
    kinds = jax.random.randint(keys[2], (TILES_ALL, 128), 0, 10)
    groups = jnp.where(kinds < 6, 0, jnp.where(kinds < 9, 1, 2))
    first_kind = jax.random.randint(keys[3], (TILES_ALL,), 0, 2)
    groups = groups.at[:, 0].set(first_kind)
    tile_rank = jnp.arange(TILES_ALL) % TILES
    device_live = jnp.repeat(live_count, TILES, total_repeat_length=TILES_ALL)
    return jnp.where((tile_rank < device_live)[:, None], groups, 2).astype(jnp.int32)


def draw_u_trial(key, part):
    shape = (3, NX, NY, NZ)
    coord_x = lax.broadcasted_iota(jnp.float32, shape, 1) / NX
    coord_y = lax.broadcasted_iota(jnp.float32, shape, 2) / NY
    coord_z = lax.broadcasted_iota(jnp.float32, shape, 3) / NZ
    scale = 1.0 + 2.0 * (coord_x + coord_y + coord_z) / 3.0
    values = 0.3 * jnp.clip(jax.random.normal(key, shape, jnp.float32), -3.0, 3.0) * scale
    return values


def draw_jacobian_inverse(key, part):
    keys = jax.random.split(key, 2)
    shape = (3, 3, NX, NY, NZ)
    diagonal = jnp.exp(jax.random.uniform(keys[0], shape, jnp.float32, jnp.log(0.5), jnp.log(1.5)))
    beside = jnp.clip(0.25 * jax.random.normal(keys[1], shape, jnp.float32), -0.6, 0.6)
    on_diagonal = lax.broadcasted_iota(jnp.int32, shape, 0) == lax.broadcasted_iota(jnp.int32, shape, 1)
    return jnp.where(on_diagonal, diagonal, beside)


def level_of(own_key, extent, cuts, least, largest):
    def one(dim, shards_of):
        steps = jax.random.uniform(jax.random.fold_in(jax.random.fold_in(own_key, 6), dim), (shards_of,), jnp.float32, least / len(cuts), largest / len(cuts))
        return jnp.repeat(jnp.exp(steps), extent[dim] // shards_of).reshape((-1,) + (1,) * (len(extent) - dim - 1))

    level = one(*cuts[0])
    for cut in cuts[1:]:
        level = level * one(*cut)
    return level


def noise(own_key, dims, width, reach, cuts=(), kind=jnp.bfloat16):
    entries = width * jax.random.normal(own_key, dims, jnp.float32)
    if cuts:
        entries = entries * level_of(own_key, dims, cuts, -0.22, 0.18)
    return jnp.clip(entries, -reach, reach).astype(kind)


def setup_inputs(seed: int = 0) -> dict:
    splits = jax.random.split(jax.random.key(seed), 7)
    return {
        "u_old": noise(splits[0], (3, NX, NY, NZ), 0.2, 1.2, ((1, 16), (2, 4), (3, 2)), jnp.float32),
        "u_trial": draw_u_trial(jax.random.fold_in(splits[6], 71), 0),
        "jacobian_inverse": draw_jacobian_inverse(jax.random.fold_in(splits[6], 71), 0),
        "tile_base": draw_tile_base(jax.random.fold_in(splits[6], 71), 0),
        "pair_codes": draw_pair_codes(jax.random.fold_in(splits[6], 71), 0),
        "pair_groups": draw_pair_groups(jax.random.fold_in(splits[6], 71), 0),
    }


step_size = 0.5
stiffness = 0.5
core_square = 0.5

def unit_step(step_code):
    which_axis = step_code // 2
    direction = 1 - 2 * (step_code % 2)
    return [jnp.where(which_axis == k, direction, 0) for k in range(3)]

def pair_cells(tile_anchor, pair_code, blocks_y, blocks_z):
    anchor = tile_anchor[:, None]
    block_x = anchor // (blocks_y * blocks_z)
    block_y = anchor // blocks_z % blocks_y
    block_z = anchor % blocks_z
    inside = pair_code[0]
    first_node = [block_x * 4 + inside // 32 + 1, block_y * 4 + inside // 8 % 4 + 1, block_z * 8 + inside % 8 + 1]
    along_step = unit_step(pair_code[1])
    second_node = [first_node[k] + along_step[k] for k in range(3)]
    offset = pair_code[2]
    third_node = [first_node[0] + offset // 9 - 1, first_node[1] + offset // 3 % 3 - 1, first_node[2] + offset % 3 - 1]
    across_step = unit_step(pair_code[3])
    fourth_node = [third_node[k] + across_step[k] for k in range(3)]
    return [first_node, second_node, third_node, fourth_node]

def pair_terms(flat_u, node_cells, groups, frozen_too, flat_fn):
    points = []
    for node_cell in node_cells:
        lattice = jnp.stack(node_cell).astype(jnp.float32)
        points.append(lattice + flat_u[:, flat_fn(node_cell)])
    line_one = points[1] - points[0]
    line_two = points[3] - points[2]
    separation = 0.5 * (points[2] + points[3]) - 0.5 * (points[0] + points[1])
    square = lax.optimization_barrier(jnp.sum(separation * separation, 0)) + core_square
    coupling = stiffness * lax.optimization_barrier(jnp.sum(line_one * line_two, 0)) / (square * jnp.sqrt(square))
    push_force = coupling * separation
    pieces = [push_force * (groups == 0).astype(jnp.float32)]
    if frozen_too:
        pieces.append(push_force * (groups == 1).astype(jnp.float32))
    halves = 0.5 * jnp.concatenate(pieces, 0)
    return jnp.concatenate([-halves, -halves, halves, halves], 1)

def reference(u_old, u_trial, jacobian_inverse, tile_base, pair_codes, pair_groups):
    device_count = N_GX * N_GY * N_GZ
    blocks_y = BY // 4
    blocks_z = BZ // 8
    width_y = NY + 2
    width_z = NZ + 2
    anchor_dev = tile_base.reshape(device_count, TILES)
    codes_dev = jnp.transpose(pair_codes.reshape(4, device_count, TILES, 128), (1, 0, 2, 3))
    groups_dev = pair_groups.reshape(device_count, TILES, 128)

    def forces(current, frozen_too):
        padded = jnp.pad(current, ((0, 0), (1, 1), (1, 1), (1, 1))).reshape(3, -1)
        channels = 6 if frozen_too else 3

        def one_device(summed, inputs):
            device, tile_anchor, pair_code, groups = inputs
            start_x = device // (N_GY * N_GZ) * BX
            start_y = device // N_GZ % N_GY * BY
            start_z = device % N_GZ * BZ

            def flat_fn(node_cell):
                return ((start_x + node_cell[0]) * width_y + start_y + node_cell[1]) * width_z + start_z + node_cell[2]
            node_cells = pair_cells(tile_anchor, pair_code, blocks_y, blocks_z)
            values = pair_terms(padded, node_cells, groups, frozen_too, flat_fn)
            flat_index = jnp.concatenate([flat_fn(node_cell) for node_cell in node_cells], 0)
            summed = summed.at[:, flat_index.reshape(-1)].add(values.reshape(channels, -1))
            return (summed, None)
        initial = jnp.zeros((channels, padded.shape[1]), jnp.float32)
        summed, _ = lax.scan(one_device, initial, (jnp.arange(device_count, dtype=jnp.int32), anchor_dev, codes_dev, groups_dev))
        return summed.reshape(channels, NX + 2, NY + 2, NZ + 2)[:, 1:-1, 1:-1, 1:-1]
    current = u_trial
    all_forces = forces(current, True)
    frozen = all_forces[3:]
    force_sum = all_forces[:3] + frozen
    norm_list = []
    for iteration in range(ITERS):
        if iteration > 0:
            force_sum = forces(current, False) + frozen
        residual = current - u_old - step_size * force_sum
        norm_list.append(jnp.sqrt(jnp.sum(residual * residual) / (3.0 * NX * NY * NZ)))
        applied = [sum((jacobian_inverse[r, m] * residual[m] for m in range(3))) for r in range(3)]
        current = current - jnp.stack(applied)
    return (current, jnp.stack(norm_list))
```

```python
import functools

import jax
import jax.numpy as jnp
from jax import lax
from jax.experimental import pallas as pl
from jax.experimental.pallas import tpu as pltpu
from jax.sharding import PartitionSpec as P

ITERS = 3
MESH = pl.DeviceIdType.MESH
F32 = jnp.float32
BF16 = jnp.bfloat16
I32 = jnp.int32

DIRS = [
    (dx, dy, z)
    for dx in (-1, 0, 1)
    for dy in (-1, 0, 1)
    for z in (0, 1)
    if (dx, dy, z) != (0, 0, 0)
]


def slot_of(dx, dy, z):
    return ((dx + 1) * 3 + dy + 1) * 2 + z


def iota(shape, dim):
    return lax.broadcasted_iota(I32, shape, dim)


def take(x, idx):
    return jnp.take_along_axis(x, idx, axis=1, mode="promise_in_bounds")


def split(x):
    hi = x.astype(BF16).astype(F32)
    return hi, x - hi


def kernel(
    nx, ny, cells,
    tb_ref, uold, utrial, jac, codes, groups,
    uout, nout,
    uc, uy, rxz, rxx, rxy, rxd,
    pb, pz, yr, frz, frx, fry, frd,
    win, gat, kidx, lidx, geo, frozen, halves, onehot, ohg, ohs, outs, acc,
    sq, ara, arb,
    send_sem, recv_sem, asend, arecv, bsend, brecv,
):
    gx, gy, gz = lax.axis_index("gx"), lax.axis_index("gy"), lax.axis_index("gz")
    tiles = groups.shape[0]
    x_ok = {-1: gx > 0, 0: None, 1: gx < nx - 1}
    y_ok = {-1: gy > 0, 0: None, 1: gy < ny - 1}

    def exists(dx, dy):
        if dx == 0 and dy == 0:
            return None
        if dx == 0:
            return y_ok[dy]
        if dy == 0:
            return x_ok[dx]
        return jnp.logical_and(x_ok[dx], y_ok[dy])

    def guarded(cond, fn):
        if cond is None:
            fn()
        else:
            pl.when(cond)(fn)

    def valid(cond, value):
        return value if cond is None else jnp.where(cond, value, 0.0)

    def target(dx, dy, z):
        return (gx + dx, gy + dy, gz if z == 0 else 1 - gz)

    barrier = pltpu.get_barrier_semaphore()

    def greet(device):
        pl.semaphore_signal(barrier, inc=1, device_id=device, device_id_type=MESH)

    for d in DIRS:
        guarded(exists(d[0], d[1]), functools.partial(greet, target(*d)))
    for o in range(1, 2 * ny):
        greet((gx, lax.rem(gy + o // 2, ny), lax.rem(gz + o, 2)))
    for o in range(1, nx):
        greet((lax.rem(gx + o, nx), gy, gz))

    def lo_hi(d):
        return 1 if d > 0 else 0

    def displacement_message(it, d):
        dx, dy, z = d
        if dx == 0 and dy == 0:
            return uc, rxz.at[it]
        if dy == 0:
            return uc.at[:, 7 * lo_hi(dx)], rxx.at[it, 1 - lo_hi(dx), z]
        if dx == 0:
            return uy.at[lo_hi(dy)], rxy.at[it, 1 - lo_hi(dy), z]
        return uy.at[lo_hi(dy)], rxd.at[it, 1 - lo_hi(dx), 1 - lo_hi(dy), z]

    def force_message(it, d):
        dx, dy, z = d
        if dx == 0 and dy == 0:
            return pz.at[:, 1:9], frz.at[it]
        if dy == 0:
            return (pz if z else pb).at[:, 9 * lo_hi(dx)], frx.at[it, 1 - lo_hi(dx), z]
        if dx == 0:
            return yr.at[z, lo_hi(dy), :, 0:8], fry.at[it, 1 - lo_hi(dy), z]
        return yr.at[z, lo_hi(dy), :, 8:16], frd.at[it, 1 - lo_hi(dx), 1 - lo_hi(dy), z]

    def copy_of(message, it, phase, d):
        src, dst = message(it, d)
        dx, dy, z = d
        return pltpu.make_async_remote_copy(
            src_ref=src,
            dst_ref=dst,
            send_sem=send_sem.at[phase, slot_of(dx, dy, z)],
            recv_sem=recv_sem.at[phase, slot_of(-dx, -dy, z)],
            device_id=target(dx, dy, z),
            device_id_type=MESH,
        )

    def start_all(message, it, phase):
        for d in DIRS:
            guarded(exists(d[0], d[1]), lambda d=d: copy_of(message, it, phase, d).start())

    def wait_all(message, it, phase):
        for d in DIRS:
            back = (-d[0], -d[1], d[2])
            guarded(exists(d[0], d[1]), lambda d=back: copy_of(message, it, phase, d).wait_recv())
        for d in DIRS:
            guarded(exists(d[0], d[1]), lambda d=d: copy_of(message, it, phase, d).wait_send())

    row8 = iota((8, 128), 0)
    lane8 = iota((8, 128), 1)

    def store_row_packs(read):
        for c in range(3):
            for x in range(8):
                plane = read(c, x)
                uy[0, c, x : x + 1, :] = plane[0:1]
                uy[1, c, x : x + 1, :] = plane[7:8]

    lane_k = iota((8, 128), 1)
    for g in range(tiles // 8):
        base = jnp.zeros((8, 128), I32)
        for i in range(8):
            base = jnp.where(row8 == i, tb_ref[g * 8 + i], base)
        s = (base >> 4) & 1
        sz = base & 15
        par = sz & 1
        j = sz >> 1
        sx = base >> 5
        i_of = (16 - j - par) & 7
        turn = j + par + jnp.where(s == 0, -2, 2)
        place = s * 16 + par * 8 + i_of
        ohg[g * 8 : g * 8 + 8, :] = jnp.where(
            jnp.logical_and((lane_k >> 6) == sx, (lane_k & 31) == place), 1.0, 0.0
        )
        ohs[g * 8 : g * 8 + 8, :] = jnp.where(lane_k == sx * 32 + place, 1.0, 0.0)
        q0 = codes[0, g * 8 : g * 8 + 8, :]
        q1 = codes[1, g * 8 : g * 8 + 8, :]
        q2 = codes[2, g * 8 : g * 8 + 8, :]
        q3 = codes[3, g * 8 : g * 8 + 8, :]

        def unit(q):
            sign = 1 - 2 * (q & 1)
            axis = q >> 1
            return [jnp.where(axis == k, sign, 0) for k in range(3)]

        e1, e2 = unit(q1), unit(q3)
        off = [((q2 * 57) >> 9) - 1, 0, 0]
        third = (q2 * 43) >> 7
        off[1] = third - 3 * (off[0] + 1) - 1
        off[2] = q2 - 3 * third - 1
        first = [(q0 >> 5) + 2, ((q0 >> 3) & 3) + 2, (q0 & 7) + 2]
        nodes = [first, [first[k] + e1[k] for k in range(3)], [first[k] + off[k] for k in range(3)]]
        nodes.append([nodes[2][k] + e2[k] for k in range(3)])
        for n in range(4):
            x, y, z = nodes[n]
            kidx[n, g * 8 : g * 8 + 8, :] = x
            lidx[n, g * 8 : g * 8 + 8, :] = ((y + turn) & 7) * 16 + z
        for k in range(3):
            a, b = e1[k].astype(F32), e2[k].astype(F32)
            geo[k, g * 8 : g * 8 + 8, :] = a
            geo[3 + k, g * 8 : g * 8 + 8, :] = b
            geo[6 + k, g * 8 : g * 8 + 8, :] = off[k].astype(F32) + 0.5 * b - 0.5 * a
    for c in range(3):
        frozen[c] = jnp.zeros((tiles, 128), F32)
    zero_plane = jnp.zeros((64, 384), BF16)
    win[0] = zero_plane
    win[11] = zero_plane

    beside_x = (gx > 0).astype(I32) + (gx < nx - 1).astype(I32)
    beside_y = (gy > 0).astype(I32) + (gy < ny - 1).astype(I32)
    pl.semaphore_wait(barrier, 2 * (1 + beside_x) * (1 + beside_y) - 1 + 2 * ny - 1 + nx - 1)
    uc[...] = utrial[...]
    store_row_packs(lambda c, x: utrial[c, x])
    start_all(displacement_message, 0, 0)

    row128 = iota((128, 128), 0)

    def make_onehot(t, carry):
        for n in range(4):
            row = lidx[n, pl.ds(t, 1), :]
            sign = -1.0 if n < 2 else 1.0
            onehot[t, :, n * 128 : (n + 1) * 128] = jnp.where(row128 == row, sign, 0.0).astype(BF16)
        return carry

    lax.fori_loop(0, tiles, make_onehot, 0)
    pick = ohg[...].astype(BF16)
    spread_t = jnp.transpose(ohs[...])[0:64, 0:tiles].astype(BF16)
    spread = jnp.concatenate([spread_t, spread_t], axis=1)

    group_bits = [((lane8 >> 4) & bit) != 0 for bit in (1, 2, 4)]
    unroll = [(lane8 + 16 * row8 + 2 + 8 * p) & 127 for p in (0, 1)]
    edge_row = {0: row8 == 7, 1: row8 == 0}
    edge_lane = {0: lane8 == 127, 1: lane8 == 0}
    z_ok = {0: gz == 1, 1: gz == 0}
    my_edge_lane = lane8 == jnp.where(gz == 0, 0, 127)

    def iteration(it, carry):
        wait_all(displacement_message, it, 2 * it)

        for x in range(10):
            for c in range(3):
                if 1 <= x <= 8:
                    own, other = uc[c, x - 1], rxz[it, c, x - 1]
                    rows = [
                        [valid(y_ok[dy], rxy[it, lo_hi(dy), z, c, x - 1 : x, :]) for z in (0, 1)]
                        for dy in (-1, 1)
                    ]
                else:
                    dx, xi = (-1, 0) if x == 0 else (1, 1)
                    own = valid(x_ok[dx], rxx[it, xi, 0, c])
                    other = valid(x_ok[dx], rxx[it, xi, 1, c])
                    at = 7 if x == 0 else 0
                    rows = [
                        [
                            valid(exists(dx, dy), rxd[it, xi, lo_hi(dy), z, c, at : at + 1, :])
                            for z in (0, 1)
                        ]
                        for dy in (-1, 1)
                    ]
                for s in range(2):
                    near = jnp.where(edge_row[s], rows[s][0], own)
                    far = jnp.where(edge_row[s], rows[s][1], other)
                    pair = []
                    for p in range(2):
                        source = jnp.where(edge_lane[p], jnp.where(z_ok[p], far, 0.0), near)
                        v = pltpu.roll(source, 2 + 8 * p, axis=1, stride=16, stride_axis=0)
                        for bit, mask in zip((1, 2, 4), group_bits):
                            v = jnp.where(mask, pltpu.roll(v, 8 - bit, axis=0), v)
                        pair.append(v)
                    both = jnp.concatenate(pair, axis=0)
                    hi, lo = split(both)
                    win[x + 1, s * 16 : s * 16 + 16, c * 128 : (c + 1) * 128] = hi.astype(BF16)
                    win[x + 1, 32 + s * 16 : 48 + s * 16, c * 128 : (c + 1) * 128] = lo.astype(BF16)
        for k in range(8):
            both = jnp.concatenate([win[k], win[k + 4]], axis=0)
            gat[k] = jnp.dot(pick, both, preferred_element_type=F32)

        live_below = jnp.where(it == 0, 2, 1)

        def group(g, carry):
            at = pl.ds(pl.multiple_of(g * 8, 8), 8)
            points = []
            for n in range(4):
                ks = kidx[n, at, :]
                ls = lidx[n, at, :]
                least, most = ((2, 5), (1, 6), (1, 6), (0, 7))[n]
                found = []
                for c in range(3):
                    value = take(gat[least, at, c * 128 : (c + 1) * 128], ls)
                    for k in range(least + 1, most + 1):
                        value = jnp.where(ks == k, take(gat[k, at, c * 128 : (c + 1) * 128], ls), value)
                    found.append(value)
                points.append(found)
            one = [points[1][c] - points[0][c] + geo[c, at, :] for c in range(3)]
            two = [points[3][c] - points[2][c] + geo[3 + c, at, :] for c in range(3)]
            apart = [
                0.5 * (points[2][c] + points[3][c]) - 0.5 * (points[0][c] + points[1][c])
                + geo[6 + c, at, :]
                for c in range(3)
            ]
            square = apart[0] * apart[0] + apart[1] * apart[1] + apart[2] * apart[2] + 0.5
            dots = one[0] * two[0] + one[1] * two[1] + one[2] * two[2]
            coupling = 0.5 * dots / (square * jnp.sqrt(square))
            fresh = groups[at, :] < live_below
            for c in range(3):
                force = jnp.where(fresh, coupling * apart[c], frozen[c, at, :])
                frozen[c, at, :] = force
                hi, lo = split(0.5 * force)
                halves[2 * c, at, :] = hi
                halves[2 * c + 1, at, :] = lo
            for i in range(8):
                t = g * 8 + i
                values = [halves[q, pl.ds(t, 1), :] for q in range(6)]
                columns = []
                for n in range(4):
                    mask = row8 == kidx[n, pl.ds(t, 1), :]
                    columns.append(
                        jnp.concatenate([jnp.where(mask, v, 0.0) for v in values], axis=0).astype(BF16)
                    )
                lhs = jnp.concatenate(columns, axis=1)
                got = lax.dot_general(
                    lhs, onehot[t], (((1,), (1,)), ((), ())), preferred_element_type=F32
                )
                for c in range(3):
                    outs[c, pl.ds(pl.multiple_of(t * 8, 8), 8), :] = (
                        got[16 * c : 16 * c + 8] + got[16 * c + 8 : 16 * c + 16]
                    )
            return carry

        lax.fori_loop(0, tiles // 8, group, 0)

        for k in range(8):
            columns = []
            for c in range(3):
                hi, lo = split(outs[c, pl.ds(k, tiles, stride=8), :])
                columns.append(jnp.concatenate([hi, lo], axis=0).astype(BF16))
            acc[k] = jnp.dot(spread, jnp.concatenate(columns, axis=1), preferred_element_type=F32)

        for x in range(10):
            for c in range(3):
                cut = slice(c * 128, (c + 1) * 128)
                parts = []
                for s in range(2):
                    line, beyond = None, None
                    for p in range(2):
                        at = s * 16 + p * 8
                        v = None
                        if x + 1 <= 7:
                            v = acc[x + 1, at : at + 8, cut]
                        if x + 1 >= 4:
                            w = acc[x - 3, 32 + at : 40 + at, cut]
                            v = w if v is None else v + w
                        for bit, mask in zip((1, 2, 4), group_bits):
                            v = jnp.where(mask, pltpu.roll(v, bit, axis=0), v)
                        v = take(v, unroll[p])
                        inside = jnp.where(edge_lane[p], 0.0, v)
                        outside = jnp.where(z_ok[p], v, 0.0)
                        line = inside if line is None else line + inside
                        beyond = outside if beyond is None else beyond + outside
                    parts.append((line, jnp.where(my_edge_lane, beyond, 0.0)))
                row_at = (x + 15) % 16
                for z in range(2):
                    (pz if z else pb)[c, x] = jnp.where(edge_row[0], 0.0, parts[0][z]) + jnp.where(
                        edge_row[1], 0.0, parts[1][z]
                    )
                    yr[z, 0, c, row_at : row_at + 1, :] = parts[0][z][7:8]
                    yr[z, 1, c, row_at : row_at + 1, :] = parts[1][z][0:1]
        start_all(force_message, it, 2 * it + 1)
        wait_all(force_message, it, 2 * it + 1)

        squares = jnp.zeros((8, 128), F32)
        for x in range(8):
            residual = []
            for c in range(3):
                total = pb[c, x + 1] + frz[it, c, x]
                for dx, xe in ((-1, 0), (1, 7)):
                    if x == xe:
                        xi = lo_hi(dx)
                        total = total + valid(x_ok[dx], frx[it, xi, 0, c] + frx[it, xi, 1, c])
                for dy in (-1, 1):
                    yi = lo_hi(dy)
                    line = valid(
                        y_ok[dy], fry[it, yi, 0, c, x : x + 1, :] + fry[it, yi, 1, c, x : x + 1, :]
                    )
                    for dx, xe, rd in ((-1, 0, 0), (1, 7, 7)):
                        if x == xe:
                            xi = lo_hi(dx)
                            line = line + valid(
                                exists(dx, dy),
                                frd[it, xi, yi, 0, c, rd : rd + 1, :] + frd[it, xi, yi, 1, c, rd : rd + 1, :],
                            )
                    total = total + jnp.where(row8 == (0 if dy < 0 else 7), line, 0.0)
                r = uc[c, x] - uold[c, x] - 0.5 * total
                squares = squares + r * r
                residual.append(r)
            for a in range(3):
                fix = jac[a, 0, x] * residual[0] + jac[a, 1, x] * residual[1] + jac[a, 2, x] * residual[2]
                new = uc[a, x] - fix
                uc[a, x] = new
                uy[0, a, x : x + 1, :] = new[0:1]
                uy[1, a, x : x + 1, :] = new[7:8]
        sq[pl.ds(it, 1), :] = jnp.sum(squares, axis=0, keepdims=True)

        @pl.when(it < ITERS - 1)
        def _():
            start_all(displacement_message, it + 1, 2 * it + 2)

        return carry

    sq[...] = jnp.zeros((8, 128), F32)
    lax.fori_loop(0, ITERS, iteration, 0)
    uout[...] = uc[...]

    def gather_sum(value, own, table, count, target_of, ssem, rsem):
        table[own] = value

        def copy(o):
            return pltpu.make_async_remote_copy(
                src_ref=sq,
                dst_ref=table.at[own],
                send_sem=ssem.at[o],
                recv_sem=rsem.at[o],
                device_id=target_of(o),
                device_id_type=MESH,
            )

        for o in range(1, count):
            copy(o).start()
        for o in range(1, count):
            copy(o).wait()
        total = table[0]
        for k in range(1, count):
            total = total + table[k]
        return total

    plane = gather_sum(
        sq[...],
        gy * 2 + gz,
        ara,
        2 * ny,
        lambda o: (gx, lax.rem(gy + o // 2, ny), lax.rem(gz + o, 2)),
        asend,
        arecv,
    )
    sq[...] = plane
    total = gather_sum(
        plane, gx, arb, nx, lambda o: (lax.rem(gx + o, nx), gy, gz), bsend, brecv
    )
    norms = jnp.sqrt(jnp.sum(total, axis=1, keepdims=True) / cells)
    for k in range(ITERS):
        nout[k] = jnp.sum(norms[k : k + 1, :])


def solution(mesh):
    nx, ny = mesh.shape["gx"], mesh.shape["gy"]

    def step(u_old, u_trial, jacobian_inverse, tile_base, pair_codes, pair_groups):
        tiles = tile_base.shape[0]
        cells = float(3 * 8 * 8 * 128 * nx * ny * mesh.shape["gz"])
        vmem = pl.BlockSpec(memory_space=pltpu.VMEM)
        smem = pl.BlockSpec(memory_space=pltpu.SMEM)
        v = pltpu.VMEM
        return pl.pallas_call(
            functools.partial(kernel, nx, ny, cells),
            out_shape=(
                jax.ShapeDtypeStruct(u_old.shape, F32),
                jax.ShapeDtypeStruct((ITERS,), F32),
            ),
            in_specs=[smem, vmem, vmem, vmem, vmem, vmem],
            out_specs=(vmem, smem),
            scratch_shapes=[
                v((3, 8, 8, 128), F32),
                v((2, 3, 8, 128), F32),
                v((ITERS, 3, 8, 8, 128), F32),
                v((ITERS, 2, 2, 3, 8, 128), F32),
                v((ITERS, 2, 2, 3, 8, 128), F32),
                v((ITERS, 2, 2, 2, 3, 8, 128), F32),
                v((3, 10, 8, 128), F32),
                v((3, 10, 8, 128), F32),
                v((2, 2, 3, 16, 128), F32),
                v((ITERS, 3, 8, 8, 128), F32),
                v((ITERS, 2, 2, 3, 8, 128), F32),
                v((ITERS, 2, 2, 3, 8, 128), F32),
                v((ITERS, 2, 2, 2, 3, 8, 128), F32),
                v((12, 64, 384), BF16),
                v((8, tiles, 384), F32),
                v((4, tiles, 128), I32),
                v((4, tiles, 128), I32),
                v((9, tiles, 128), F32),
                v((3, tiles, 128), F32),
                v((6, tiles, 128), F32),
                v((tiles, 128, 512), BF16),
                v((tiles, 128), F32),
                v((tiles, 128), F32),
                v((3, tiles * 8, 128), F32),
                v((8, 64, 384), F32),
                v((8, 128), F32),
                v((2 * ny, 8, 128), F32),
                v((nx, 8, 128), F32),
                pltpu.SemaphoreType.DMA((2 * ITERS, 18)),
                pltpu.SemaphoreType.DMA((2 * ITERS, 18)),
                pltpu.SemaphoreType.DMA((2 * ny,)),
                pltpu.SemaphoreType.DMA((2 * ny,)),
                pltpu.SemaphoreType.DMA((nx,)),
                pltpu.SemaphoreType.DMA((nx,)),
            ],
            compiler_params=pltpu.CompilerParams(
                collective_id=0, has_side_effects=True, vmem_limit_bytes=60 * 2**20
            ),
            name="relax",
        )(tile_base, u_old, u_trial, jacobian_inverse, pair_codes, pair_groups)

    everywhere = ("gx", "gy", "gz")
    return jax.shard_map(
        step,
        mesh=mesh,
        in_specs=(
            P(None, "gx", "gy", "gz"),
            P(None, "gx", "gy", "gz"),
            P(None, None, "gx", "gy", "gz"),
            P(everywhere),
            P(None, everywhere, None),
            P(everywhere, None),
        ),
        out_specs=(P(None, "gx", "gy", "gz"), P()),
        check_vma=False,
    )
```

```python
import functools

import jax
import jax.numpy as jnp
from jax import lax
from jax.experimental import pallas as pl
from jax.experimental.pallas import tpu as pltpu
from jax.sharding import PartitionSpec as P

ITERS = 3
MESH = pl.DeviceIdType.MESH
F32 = jnp.float32
BF16 = jnp.bfloat16
I32 = jnp.int32

DIRS = sorted(
    [
        (dx, dy, z)
        for dx in (-1, 0, 1)
        for dy in (-1, 0, 1)
        for z in (0, 1)
        if (dx, dy, z) != (0, 0, 0)
    ],
    key=lambda d: (-2 * abs(d[0]) - abs(d[1]), d),
)


def slot_of(dx, dy, z):
    return ((dx + 1) * 3 + dy + 1) * 2 + z


def iota(shape, dim):
    return lax.broadcasted_iota(I32, shape, dim)


def take(x, idx):
    return jnp.take_along_axis(x, idx, axis=1, mode="promise_in_bounds")


def split(x):
    hi = x.astype(BF16).astype(F32)
    return hi, x - hi


class Gathered:
    def __init__(self, source, table, own, targets, send, recv):
        self.source, self.table, self.own, self.targets = source, table, own, targets
        self.send, self.recv = send, recv

    def copy(self, o, device):
        return pltpu.make_async_remote_copy(
            src_ref=self.source,
            dst_ref=self.table.at[self.own],
            send_sem=self.send.at[o],
            recv_sem=self.recv.at[o],
            device_id=device,
            device_id_type=MESH,
        )

    def start(self):
        for o, device in self.targets:
            self.copy(o, device).start()
        self.table[self.own] = self.source[...]

    def finish(self):
        for o, device in self.targets:
            self.copy(o, device).wait()
        total = self.table[0]
        for k in range(1, self.table.shape[0]):
            total = total + self.table[k]
        return total


def kernel(
    nx, ny, cells,
    tb_in, uold_in, utrial_in, jac_in, codes_in, groups_in,
    uout, nout,
    tb_ref, uold, jac, codes, groups, residuals,
    uc, uy, uxe, uye, ud, rxz, rxx, rxy, rxxe, rxye, rxd,
    pb, pz, yr, fxe, fye, fd, frz, frx, fry, frxe, frye, frd,
    win, gat, kidx, lidx, geo, frozen, onehot, ohg, ohs, outs, acc,
    sq, sq2, ara, arb,
    in_sem, send_sem, recv_sem, asend, arecv, bsend, brecv,
):
    gx, gy, gz = lax.axis_index("gx"), lax.axis_index("gy"), lax.axis_index("gz")
    tiles = groups.shape[0]
    x_ok = {-1: gx > 0, 0: None, 1: gx < nx - 1}
    y_ok = {-1: gy > 0, 0: None, 1: gy < ny - 1}

    def exists(dx, dy):
        if dx == 0 and dy == 0:
            return None
        if dx == 0:
            return y_ok[dy]
        if dy == 0:
            return x_ok[dx]
        return jnp.logical_and(x_ok[dx], y_ok[dy])

    def guarded(cond, fn):
        if cond is None:
            fn()
        else:
            pl.when(cond)(fn)

    def valid(cond, value):
        return value if cond is None else jnp.where(cond, value, 0.0)

    def target(dx, dy, z):
        return (gx + dx, gy + dy, gz if z == 0 else 1 - gz)

    barrier = pltpu.get_barrier_semaphore()

    def greet(device):
        pl.semaphore_signal(barrier, inc=1, device_id=device, device_id_type=MESH)

    for d in DIRS:
        guarded(exists(d[0], d[1]), functools.partial(greet, target(*d)))
    for o in range(1, 2 * ny):
        greet((gx, lax.rem(gy + o // 2, ny), lax.rem(gz + o, 2)))
    for o in range(1, nx):
        greet((lax.rem(gx + o, nx), gy, gz))

    fetches = [
        pltpu.make_async_copy(src, dst, in_sem.at[k])
        for k, (src, dst) in enumerate(
            [
                (utrial_in, uc),
                (tb_in, tb_ref),
                (codes_in, codes),
                (groups_in, groups),
                (uold_in, uold),
                (jac_in, jac),
            ]
        )
    ]
    for fetch in fetches:
        fetch.start()

    def lo_hi(d):
        return 1 if d > 0 else 0

    def displacement_message(it, d):
        dx, dy, z = d
        xi, yi = lo_hi(dx), lo_hi(dy)
        if dx == 0 and dy == 0:
            return uc, rxz.at[it]
        if dy == 0:
            if z:
                return uxe.at[xi], rxxe.at[it, 1 - xi]
            return uc.at[:, 7 * xi], rxx.at[it, 1 - xi]
        if dx == 0:
            if z:
                return uye.at[yi], rxye.at[it, 1 - yi]
            return uy.at[yi], rxy.at[it, 1 - yi]
        return ud.at[xi, yi], rxd.at[it, 1 - xi, 1 - yi, z]

    def force_message(it, d):
        dx, dy, z = d
        xi, yi = lo_hi(dx), lo_hi(dy)
        if dx == 0 and dy == 0:
            return pz.at[:, 1:9], frz.at[it]
        if dy == 0:
            if z:
                return fxe.at[xi], frxe.at[it, 1 - xi]
            return pb.at[:, 9 * xi], frx.at[it, 1 - xi]
        if dx == 0:
            if z:
                return fye.at[yi], frye.at[it, 1 - yi]
            return yr.at[0, yi], fry.at[it, 1 - yi]
        return fd.at[z, xi, yi], frd.at[it, 1 - xi, 1 - yi, z]

    def copy_of(message, it, phase, d):
        src, dst = message(it, d)
        dx, dy, z = d
        return pltpu.make_async_remote_copy(
            src_ref=src,
            dst_ref=dst,
            send_sem=send_sem.at[phase, slot_of(dx, dy, z)],
            recv_sem=recv_sem.at[phase, slot_of(-dx, -dy, z)],
            device_id=target(dx, dy, z),
            device_id_type=MESH,
        )

    def start_all(message, it, phase):
        for d in DIRS:
            guarded(exists(d[0], d[1]), lambda d=d: copy_of(message, it, phase, d).start())

    def wait_all(message, it, phase):
        for d in DIRS:
            back = (-d[0], -d[1], d[2])
            guarded(exists(d[0], d[1]), lambda d=back: copy_of(message, it, phase, d).wait_recv())
        for d in DIRS:
            guarded(exists(d[0], d[1]), lambda d=d: copy_of(message, it, phase, d).wait_send())

    row8 = iota((8, 128), 0)
    lane8 = iota((8, 128), 1)

    my_edge = jnp.where(gz == 0, 127, 0)
    other_edge = 127 - my_edge
    my_edge_index = jnp.full((8, 128), my_edge, I32)
    other_edge_index = jnp.full((8, 128), other_edge, I32)
    lane_index = [jnp.full((8, 128), c, I32) for c in range(3)]

    def edges(planes, index):
        packed = take(planes[0], index)
        for c in (1, 2):
            packed = jnp.where(lane8 == c, take(planes[c], index), packed)
        return packed

    def store_row_packs():
        for xi, x in ((0, 0), (1, 7)):
            uxe[xi] = edges([uc[c, x] for c in range(3)], my_edge_index)
            for yi in range(2):
                for c in range(3):
                    ud[xi, yi, c : c + 1, :] = uy[yi, c, x : x + 1, :]
        for yi in range(2):
            uye[yi] = edges([uy[yi, c] for c in range(3)], my_edge_index)

    fetches[0].wait()
    for c in range(3):
        for x in range(8):
            plane = uc[c, x]
            uy[0, c, x : x + 1, :] = plane[0:1]
            uy[1, c, x : x + 1, :] = plane[7:8]
    store_row_packs()
    beside_x = (gx > 0).astype(I32) + (gx < nx - 1).astype(I32)
    beside_y = (gy > 0).astype(I32) + (gy < ny - 1).astype(I32)
    pl.semaphore_wait(barrier, 2 * (1 + beside_x) * (1 + beside_y) - 1 + 2 * ny - 1 + nx - 1)
    start_all(displacement_message, 0, 0)

    for fetch in fetches[1:]:
        fetch.wait()
    lane_k = iota((8, 128), 1)
    for g in range(tiles // 8):
        base = jnp.zeros((8, 128), I32)
        for i in range(8):
            base = jnp.where(row8 == i, tb_ref[g * 8 + i], base)
        s = (base >> 4) & 1
        sz = base & 15
        par = sz & 1
        j = sz >> 1
        sx = base >> 5
        i_of = (16 - j - par) & 7
        turn = j + par + jnp.where(s == 0, -2, 2)
        place = s * 16 + par * 8 + i_of
        ohg[g * 8 : g * 8 + 8, :] = jnp.where(
            jnp.logical_and((lane_k >> 6) == sx, (lane_k & 31) == place), 1.0, 0.0
        )
        ohs[g * 8 : g * 8 + 8, :] = jnp.where(lane_k == sx * 32 + place, 1.0, 0.0)
        q0 = codes[0, g * 8 : g * 8 + 8, :]
        q1 = codes[1, g * 8 : g * 8 + 8, :]
        q2 = codes[2, g * 8 : g * 8 + 8, :]
        q3 = codes[3, g * 8 : g * 8 + 8, :]

        def unit(q):
            sign = 1 - 2 * (q & 1)
            axis = q >> 1
            return [jnp.where(axis == k, sign, 0) for k in range(3)]

        e1, e2 = unit(q1), unit(q3)
        off = [((q2 * 57) >> 9) - 1, 0, 0]
        third = (q2 * 43) >> 7
        off[1] = third - 3 * (off[0] + 1) - 1
        off[2] = q2 - 3 * third - 1
        first = [(q0 >> 5) + 2, ((q0 >> 3) & 3) + 2, (q0 & 7) + 2]
        nodes = [first, [first[k] + e1[k] for k in range(3)], [first[k] + off[k] for k in range(3)]]
        nodes.append([nodes[2][k] + e2[k] for k in range(3)])
        for n in range(4):
            x, y, z = nodes[n]
            kidx[n, g * 8 : g * 8 + 8, :] = x
            lidx[n, g * 8 : g * 8 + 8, :] = ((y + turn) & 7) * 16 + z
        for k in range(3):
            a, b = e1[k].astype(F32), e2[k].astype(F32)
            geo[k, g * 8 : g * 8 + 8, :] = a
            geo[3 + k, g * 8 : g * 8 + 8, :] = b
            geo[6 + k, g * 8 : g * 8 + 8, :] = off[k].astype(F32) + 0.5 * b - 0.5 * a
    for c in range(3):
        frozen[c] = jnp.zeros((tiles, 128), F32)
    zero_plane = jnp.zeros((64, 384), BF16)
    win[0] = zero_plane
    win[11] = zero_plane

    row128 = iota((128, 128), 0)

    def make_onehot(t, carry):
        for n in range(2):
            first = lidx[2 * n, pl.ds(t, 1), :]
            second = lidx[2 * n + 1, pl.ds(t, 1), :]
            sign = 1.0 if n else -1.0
            flat = jnp.where(jnp.logical_or(row128 == first, row128 == second), sign, 0.0).astype(BF16)
            onehot[t, n * 128 : (n + 1) * 128, :] = jnp.transpose(flat)
        return carry

    lax.fori_loop(0, tiles, make_onehot, 0, unroll=4)
    pick = ohg[...].astype(BF16)
    spread_t = jnp.transpose(ohs[...])[0:64, 0:tiles].astype(BF16)
    spread = jnp.concatenate([spread_t, spread_t], axis=1)

    group_bits = [((lane8 >> 4) & bit) != 0 for bit in (1, 2, 4)]
    unroll = [(lane8 + 16 * row8 + 2 + 8 * p) & 127 for p in (0, 1)]
    edge_row = {0: row8 == 7, 1: row8 == 0}
    edge_lane = {0: lane8 == 127, 1: lane8 == 0}
    z_ok = {0: gz == 1, 1: gz == 0}
    my_edge_lane = lane8 == other_edge
    at_edge = lane8 == my_edge

    first_sum = Gathered(
        sq,
        ara,
        gy * 2 + gz,
        [(o, (gx, lax.rem(gy + o // 2, ny), lax.rem(gz + o, 2))) for o in range(1, 2 * ny)],
        asend,
        arecv,
    )
    second_sum = Gathered(
        sq2, arb, gx, [(o, (lax.rem(gx + o, nx), gy, gz)) for o in range(1, nx)], bsend, brecv
    )

    def iteration(it, carry):
        wait_all(displacement_message, it, 2 * it)

        beyond_rows = [
            [take(valid(y_ok[dy], rxye[it, lo_hi(dy)]), lane_index[c]) for c in range(3)] for dy in (-1, 1)
        ]
        for x in range(10):
            for c in range(3):
                if 1 <= x <= 8:
                    own, other = uc[c, x - 1], rxz[it, c, x - 1]
                    rows = [
                        [
                            valid(y_ok[dy], rxy[it, lo_hi(dy), c, x - 1 : x, :]),
                            beyond_rows[lo_hi(dy)][c][x - 1 : x],
                        ]
                        for dy in (-1, 1)
                    ]
                else:
                    dx, xi = (-1, 0) if x == 0 else (1, 1)
                    own = valid(x_ok[dx], rxx[it, xi, c])
                    other = take(valid(x_ok[dx], rxxe[it, xi]), lane_index[c])
                    rows = [
                        [
                            valid(exists(dx, dy), rxd[it, xi, lo_hi(dy), z, c : c + 1, :])
                            for z in (0, 1)
                        ]
                        for dy in (-1, 1)
                    ]
                for s in range(2):
                    near = jnp.where(edge_row[s], rows[s][0], own)
                    far = jnp.where(edge_row[s], rows[s][1], other)
                    pair = []
                    for p in range(2):
                        source = jnp.where(edge_lane[p], jnp.where(z_ok[p], far, 0.0), near)
                        v = pltpu.roll(source, 2 + 8 * p, axis=1, stride=16, stride_axis=0)
                        for bit, mask in zip((1, 2, 4), group_bits):
                            v = jnp.where(mask, pltpu.roll(v, 8 - bit, axis=0), v)
                        pair.append(v)
                    both = jnp.concatenate(pair, axis=0)
                    hi, lo = split(both)
                    win[x + 1, s * 16 : s * 16 + 16, c * 128 : (c + 1) * 128] = hi.astype(BF16)
                    win[x + 1, 32 + s * 16 : 48 + s * 16, c * 128 : (c + 1) * 128] = lo.astype(BF16)
        for k in range(8):
            both = jnp.concatenate([win[k], win[k + 4]], axis=0)
            gat[k] = jnp.dot(pick, both, preferred_element_type=F32)

        live_below = jnp.where(it == 0, 2, 1)

        def pair_forces(g):
            at = pl.ds(pl.multiple_of(g * 8, 8), 8)
            points = []
            for n in range(4):
                ks = kidx[n, at, :]
                ls = lidx[n, at, :]
                least, most = ((2, 5), (1, 6), (1, 6), (0, 7))[n]
                found = []
                for c in range(3):
                    value = take(gat[least, at, c * 128 : (c + 1) * 128], ls)
                    for k in range(least + 1, most + 1):
                        value = jnp.where(ks == k, take(gat[k, at, c * 128 : (c + 1) * 128], ls), value)
                    found.append(value)
                points.append(found)
            one = [points[1][c] - points[0][c] + geo[c, at, :] for c in range(3)]
            two = [points[3][c] - points[2][c] + geo[3 + c, at, :] for c in range(3)]
            apart = [
                0.5 * (points[2][c] + points[3][c]) - 0.5 * (points[0][c] + points[1][c])
                + geo[6 + c, at, :]
                for c in range(3)
            ]
            square = apart[0] * apart[0] + apart[1] * apart[1] + apart[2] * apart[2] + 0.5
            dots = one[0] * two[0] + one[1] * two[1] + one[2] * two[2]
            coupling = 0.5 * dots / (square * jnp.sqrt(square))
            fresh = groups[at, :] < live_below
            values = []
            for c in range(3):
                force = jnp.where(fresh, coupling * apart[c], frozen[c, at, :])
                frozen[c, at, :] = force
                values.extend(split(0.5 * force))
            return tuple(values)

        def spread_forces(g, values):
            for i in range(8):
                t = g * 8 + i
                columns = []
                for n in range(2):
                    mask = jnp.logical_or(
                        row8 == kidx[2 * n, pl.ds(t, 1), :], row8 == kidx[2 * n + 1, pl.ds(t, 1), :]
                    )
                    columns.append(
                        jnp.concatenate(
                            [jnp.where(mask, v[i : i + 1], 0.0) for v in values], axis=0
                        ).astype(BF16)
                    )
                lhs = jnp.concatenate(columns, axis=1)
                got = jnp.dot(lhs, onehot[t], preferred_element_type=F32)
                for c in range(3):
                    outs[c, pl.ds(pl.multiple_of(t * 8, 8), 8), :] = (
                        got[16 * c : 16 * c + 8] + got[16 * c + 8 : 16 * c + 16]
                    )

        def group(g, values):
            later = pair_forces(g)
            spread_forces(g - 1, values)
            return later

        values = lax.fori_loop(1, tiles // 8, group, pair_forces(0))
        spread_forces(tiles // 8 - 1, values)

        for k in range(8):
            columns = []
            for c in range(3):
                hi, lo = split(outs[c, pl.ds(k, tiles, stride=8), :])
                columns.append(jnp.concatenate([hi, lo], axis=0).astype(BF16))
            acc[k] = jnp.dot(spread, jnp.concatenate(columns, axis=1), preferred_element_type=F32)

        for x in range(10):
            for c in range(3):
                cut = slice(c * 128, (c + 1) * 128)
                parts = []
                for s in range(2):
                    line, beyond = None, None
                    for p in range(2):
                        at = s * 16 + p * 8
                        v = None
                        if x + 1 <= 7:
                            v = acc[x + 1, at : at + 8, cut]
                        if x + 1 >= 4:
                            w = acc[x - 3, 32 + at : 40 + at, cut]
                            v = w if v is None else v + w
                        for bit, mask in zip((1, 2, 4), group_bits):
                            v = jnp.where(mask, pltpu.roll(v, bit, axis=0), v)
                        v = take(v, unroll[p])
                        inside = jnp.where(edge_lane[p], 0.0, v)
                        outside = jnp.where(z_ok[p], v, 0.0)
                        line = inside if line is None else line + inside
                        beyond = outside if beyond is None else beyond + outside
                    parts.append((line, jnp.where(my_edge_lane, beyond, 0.0)))
                for z in range(2):
                    (pz if z else pb)[c, x] = jnp.where(edge_row[0], 0.0, parts[0][z]) + jnp.where(
                        edge_row[1], 0.0, parts[1][z]
                    )
                    ends = (parts[0][z][7:8], parts[1][z][0:1])
                    for yi in range(2):
                        if 1 <= x <= 8:
                            yr[z, yi, c, x - 1 : x, :] = ends[yi]
                        else:
                            fd[z, 0 if x == 0 else 1, yi, c : c + 1, :] = ends[yi]
        for i in range(2):
            fxe[i] = edges([pz[c, 9 * i] for c in range(3)], other_edge_index)
            fye[i] = edges([yr[1, i, c] for c in range(3)], other_edge_index)
        start_all(force_message, it, 2 * it + 1)
        wait_all(force_message, it, 2 * it + 1)

        squares = jnp.zeros((8, 128), F32)
        lines = []
        for dy in (-1, 1):
            yi = lo_hi(dy)
            lines.append(
                [
                    valid(
                        y_ok[dy],
                        fry[it, yi, c] + jnp.where(at_edge, take(frye[it, yi], lane_index[c]), 0.0),
                    )
                    for c in range(3)
                ]
            )
        for x in range(8):
            for c in range(3):
                total = pb[c, x + 1] + frz[it, c, x]
                for dx, xe in ((-1, 0), (1, 7)):
                    if x == xe:
                        xi = lo_hi(dx)
                        total = total + valid(
                            x_ok[dx],
                            frx[it, xi, c] + jnp.where(at_edge, take(frxe[it, xi], lane_index[c]), 0.0),
                        )
                for dy in (-1, 1):
                    yi = lo_hi(dy)
                    line = lines[yi][c][x : x + 1]
                    for dx, xe in ((-1, 0), (1, 7)):
                        if x == xe:
                            xi = lo_hi(dx)
                            line = line + valid(
                                exists(dx, dy),
                                frd[it, xi, yi, 0, c : c + 1, :] + frd[it, xi, yi, 1, c : c + 1, :],
                            )
                    total = total + jnp.where(row8 == (0 if dy < 0 else 7), line, 0.0)
                r = uc[c, x] - uold[c, x] - 0.5 * total
                squares = squares + r * r
                residuals[c, x] = r
        sq[pl.ds(it, 1), :] = jnp.sum(squares, axis=0, keepdims=True)

        @pl.when(it == ITERS - 1)
        def _():
            first_sum.start()

        for x in range(8):
            residual = [residuals[c, x] for c in range(3)]
            for a in range(3):
                fix = jac[a, 0, x] * residual[0] + jac[a, 1, x] * residual[1] + jac[a, 2, x] * residual[2]
                new = uc[a, x] - fix
                uc[a, x] = new
                uy[0, a, x : x + 1, :] = new[0:1]
                uy[1, a, x : x + 1, :] = new[7:8]

        @pl.when(it < ITERS - 1)
        def _():
            store_row_packs()
            start_all(displacement_message, it + 1, 2 * it + 2)

        return carry

    sq[...] = jnp.zeros((8, 128), F32)
    lax.fori_loop(0, ITERS, iteration, 0)
    store_result = pltpu.make_async_copy(uc, uout, in_sem.at[0])
    store_result.start()
    plane = first_sum.finish()
    second_sum.source[...] = plane
    second_sum.start()
    total = second_sum.finish()
    norms = jnp.sqrt(jnp.sum(total, axis=1, keepdims=True) / cells)
    for k in range(ITERS):
        nout[k] = jnp.sum(norms[k : k + 1, :])
    store_result.wait()


def solution(mesh):
    nx, ny = mesh.shape["gx"], mesh.shape["gy"]

    def step(u_old, u_trial, jacobian_inverse, tile_base, pair_codes, pair_groups):
        tiles = tile_base.shape[0]
        cells = float(3 * 8 * 8 * 128 * nx * ny * mesh.shape["gz"])
        smem = pl.BlockSpec(memory_space=pltpu.SMEM)
        v = pltpu.VMEM
        return pl.pallas_call(
            functools.partial(kernel, nx, ny, cells),
            out_shape=(
                jax.ShapeDtypeStruct(u_old.shape, F32),
                jax.ShapeDtypeStruct((ITERS,), F32),
            ),
            in_specs=[pl.BlockSpec(memory_space=pl.ANY)] * 6,
            out_specs=(pl.BlockSpec(memory_space=pl.ANY), smem),
            scratch_shapes=[
                pltpu.SMEM(tile_base.shape, I32),
                v(u_old.shape, F32),
                v(jacobian_inverse.shape, F32),
                v(pair_codes.shape, I32),
                v(pair_groups.shape, I32),
                v(u_old.shape, F32),
                v((3, 8, 8, 128), F32),
                v((2, 3, 8, 128), F32),
                v((2, 8, 128), F32),
                v((2, 8, 128), F32),
                v((2, 2, 8, 128), F32),
                v((ITERS, 3, 8, 8, 128), F32),
                v((ITERS, 2, 3, 8, 128), F32),
                v((ITERS, 2, 3, 8, 128), F32),
                v((ITERS, 2, 8, 128), F32),
                v((ITERS, 2, 8, 128), F32),
                v((ITERS, 2, 2, 2, 8, 128), F32),
                v((3, 10, 8, 128), F32),
                v((3, 10, 8, 128), F32),
                v((2, 2, 3, 8, 128), F32),
                v((2, 8, 128), F32),
                v((2, 8, 128), F32),
                v((2, 2, 2, 8, 128), F32),
                v((ITERS, 3, 8, 8, 128), F32),
                v((ITERS, 2, 3, 8, 128), F32),
                v((ITERS, 2, 3, 8, 128), F32),
                v((ITERS, 2, 8, 128), F32),
                v((ITERS, 2, 8, 128), F32),
                v((ITERS, 2, 2, 2, 8, 128), F32),
                v((12, 64, 384), BF16),
                v((8, tiles, 384), F32),
                v((4, tiles, 128), I32),
                v((4, tiles, 128), I32),
                v((9, tiles, 128), F32),
                v((3, tiles, 128), F32),
                v((tiles, 256, 128), BF16),
                v((tiles, 128), F32),
                v((tiles, 128), F32),
                v((3, tiles * 8, 128), F32),
                v((8, 64, 384), F32),
                v((8, 128), F32),
                v((8, 128), F32),
                v((2 * ny, 8, 128), F32),
                v((nx, 8, 128), F32),
                pltpu.SemaphoreType.DMA((6,)),
                pltpu.SemaphoreType.DMA((2 * ITERS, 18)),
                pltpu.SemaphoreType.DMA((2 * ITERS, 18)),
                pltpu.SemaphoreType.DMA((2 * ny,)),
                pltpu.SemaphoreType.DMA((2 * ny,)),
                pltpu.SemaphoreType.DMA((nx,)),
                pltpu.SemaphoreType.DMA((nx,)),
            ],
            compiler_params=pltpu.CompilerParams(
                collective_id=0, has_side_effects=True, vmem_limit_bytes=60 * 2**20
            ),
            name="relax",
        )(tile_base, u_old, u_trial, jacobian_inverse, pair_codes, pair_groups)

    everywhere = ("gx", "gy", "gz")
    return jax.shard_map(
        step,
        mesh=mesh,
        in_specs=(
            P(None, "gx", "gy", "gz"),
            P(None, "gx", "gy", "gz"),
            P(None, None, "gx", "gy", "gz"),
            P(everywhere),
            P(None, everywhere, None),
            P(everywhere, None),
        ),
        out_specs=(P(None, "gx", "gy", "gz"), P()),
        check_vma=False,
    )
```

```python
import functools

import jax
import jax.numpy as jnp
from jax import lax
from jax.experimental import pallas as pl
from jax.experimental.pallas import tpu as pltpu
from jax.sharding import PartitionSpec as P

ITERS = 3
MESH = pl.DeviceIdType.MESH
F32 = jnp.float32
BF16 = jnp.bfloat16
I32 = jnp.int32

DIRS = sorted(
    [
        (dx, dy, z)
        for dx in (-1, 0, 1)
        for dy in (-1, 0, 1)
        for z in (0, 1)
        if (dx, dy, z) != (0, 0, 0)
    ],
    key=lambda d: (-2 * abs(d[0]) - abs(d[1]), d),
)


FAR = [d for d in DIRS if d[0] != 0]
NEAR = [d for d in DIRS if d[0] == 0]


def slot_of(dx, dy, z):
    return ((dx + 1) * 3 + dy + 1) * 2 + z


def iota(shape, dim):
    return lax.broadcasted_iota(I32, shape, dim)


def take(x, idx):
    return jnp.take_along_axis(x, idx, axis=1, mode="promise_in_bounds")


def split(x):
    hi = x.astype(BF16).astype(F32)
    return hi, x - hi


class Gathered:
    def __init__(self, source, table, own, targets, send, recv):
        self.source, self.table, self.own, self.targets = source, table, own, targets
        self.send, self.recv = send, recv

    def copy(self, o, device):
        return pltpu.make_async_remote_copy(
            src_ref=self.source,
            dst_ref=self.table.at[self.own],
            send_sem=self.send.at[o],
            recv_sem=self.recv.at[o],
            device_id=device,
            device_id_type=MESH,
        )

    def start(self):
        for o, device in self.targets:
            self.copy(o, device).start()
        self.table[self.own] = self.source[...]

    def finish(self):
        for o, device in self.targets:
            self.copy(o, device).wait()
        total = self.table[0]
        for k in range(1, self.table.shape[0]):
            total = total + self.table[k]
        return total


def kernel(
    nx, ny, cells,
    tb_in, uold_in, utrial_in, jac_in, codes_in, groups_in,
    uout, nout,
    tb_ref, uold, jac, codes, groups, residuals,
    uc, uy, uxe, uye, ud, rxz, rxx, rxy, rxxe, rxye, rxd,
    pb, pz, yr, fxe, fye, fd, frz, frx, fry, frxe, frye, frd,
    win, gat, kidx, lidx, geo, frozen, onehot, ohg, ohs, outs, acc,
    sq, sq2, ara, arb,
    hail_four, hail_eight, in_sem, send_sem, recv_sem, asend, arecv, bsend, brecv,
):
    gx, gy, gz = lax.axis_index("gx"), lax.axis_index("gy"), lax.axis_index("gz")
    tiles = groups.shape[0]
    x_ok = {-1: gx > 0, 0: None, 1: gx < nx - 1}
    y_ok = {-1: gy > 0, 0: None, 1: gy < ny - 1}

    def exists(dx, dy):
        if dx == 0 and dy == 0:
            return None
        if dx == 0:
            return y_ok[dy]
        if dy == 0:
            return x_ok[dx]
        return jnp.logical_and(x_ok[dx], y_ok[dy])

    def guarded(cond, fn):
        if cond is None:
            fn()
        else:
            pl.when(cond)(fn)

    def valid(cond, value):
        return value if cond is None else jnp.where(cond, value, 0.0)

    def target(dx, dy, z):
        return (gx + dx, gy + dy, gz if z == 0 else 1 - gz)

    barrier = pltpu.get_barrier_semaphore()

    def greet(device):
        pl.semaphore_signal(barrier, inc=1, device_id=device, device_id_type=MESH)

    for d in DIRS:
        guarded(exists(d[0], d[1]), functools.partial(greet, target(*d)))

    fetches = [
        pltpu.make_async_copy(src, dst, in_sem.at[k])
        for k, (src, dst) in enumerate(
            [
                (utrial_in, uc),
                (tb_in, tb_ref),
                (codes_in, codes),
                (groups_in, groups),
                (uold_in, uold),
                (jac_in, jac),
            ]
        )
    ]
    for fetch in fetches:
        fetch.start()

    def lo_hi(d):
        return 1 if d > 0 else 0

    def displacement_message(it, d):
        dx, dy, z = d
        xi, yi = lo_hi(dx), lo_hi(dy)
        if dx == 0 and dy == 0:
            return uc, rxz.at[it]
        if dy == 0:
            if z:
                return uxe.at[xi], rxxe.at[it, 1 - xi]
            return uc.at[:, 7 * xi], rxx.at[it, 1 - xi]
        if dx == 0:
            if z:
                return uye.at[yi], rxye.at[it, 1 - yi]
            return uy.at[yi], rxy.at[it, 1 - yi]
        return ud.at[xi, yi], rxd.at[it, 1 - xi, 1 - yi, z]

    def force_message(it, d):
        dx, dy, z = d
        xi, yi = lo_hi(dx), lo_hi(dy)
        if dx == 0 and dy == 0:
            return pz.at[:, 1:9], frz.at[it]
        if dy == 0:
            if z:
                return fxe.at[xi], frxe.at[it, 1 - xi]
            return pb.at[:, 9 * xi], frx.at[it, 1 - xi]
        if dx == 0:
            if z:
                return fye.at[yi], frye.at[it, 1 - yi]
            return yr.at[0, yi], fry.at[it, 1 - yi]
        return fd.at[z, xi, yi], frd.at[it, 1 - xi, 1 - yi, z]

    def copy_of(message, it, phase, d):
        src, dst = message(it, d)
        dx, dy, z = d
        return pltpu.make_async_remote_copy(
            src_ref=src,
            dst_ref=dst,
            send_sem=send_sem.at[phase, slot_of(dx, dy, z)],
            recv_sem=recv_sem.at[phase, slot_of(-dx, -dy, z)],
            device_id=target(dx, dy, z),
            device_id_type=MESH,
        )

    def start(message, it, phase, dirs):
        for d in dirs:
            guarded(exists(d[0], d[1]), lambda d=d: copy_of(message, it, phase, d).start())

    def wait_arrivals(message, it, phase, dirs):
        for d in dirs:
            back = (-d[0], -d[1], d[2])
            guarded(exists(d[0], d[1]), lambda d=back: copy_of(message, it, phase, d).wait_recv())

    def wait_sends(message, it, phase):
        for d in DIRS:
            guarded(exists(d[0], d[1]), lambda d=d: copy_of(message, it, phase, d).wait_send())

    row8 = iota((8, 128), 0)
    lane8 = iota((8, 128), 1)

    my_edge = jnp.where(gz == 0, 127, 0)
    other_edge = 127 - my_edge
    my_edge_index = jnp.full((8, 128), my_edge, I32)
    other_edge_index = jnp.full((8, 128), other_edge, I32)
    lane_index = [jnp.full((8, 128), c, I32) for c in range(3)]

    def edges(planes, index):
        packed = take(planes[0], index)
        for c in (1, 2):
            packed = jnp.where(lane8 == c, take(planes[c], index), packed)
        return packed

    def pack_far():
        for xi, x in ((0, 0), (1, 7)):
            uxe[xi] = edges([uc[c, x] for c in range(3)], my_edge_index)
            for yi in range(2):
                for c in range(3):
                    ud[xi, yi, c : c + 1, :] = uy[yi, c, x : x + 1, :]

    def pack_near():
        for yi in range(2):
            uye[yi] = edges([uy[yi, c] for c in range(3)], my_edge_index)

    fetches[0].wait()
    for c in range(3):
        for x in range(8):
            plane = uc[c, x]
            uy[0, c, x : x + 1, :] = plane[0:1]
            uy[1, c, x : x + 1, :] = plane[7:8]
    pack_far()
    pack_near()
    beside_x = (gx > 0).astype(I32) + (gx < nx - 1).astype(I32)
    beside_y = (gy > 0).astype(I32) + (gy < ny - 1).astype(I32)
    pl.semaphore_wait(barrier, 2 * (1 + beside_x) * (1 + beside_y) - 1)
    start(displacement_message, 0, 0, DIRS)

    for fetch in fetches[1:]:
        fetch.wait()
    lane_k = iota((8, 128), 1)
    for g in range(tiles // 8):
        base = jnp.zeros((8, 128), I32)
        for i in range(8):
            base = jnp.where(row8 == i, tb_ref[g * 8 + i], base)
        s = (base >> 4) & 1
        sz = base & 15
        par = sz & 1
        j = sz >> 1
        sx = base >> 5
        i_of = (16 - j - par) & 7
        turn = j + par + jnp.where(s == 0, -2, 2)
        place = s * 16 + par * 8 + i_of
        ohg[g * 8 : g * 8 + 8, :] = jnp.where(
            jnp.logical_and((lane_k >> 6) == sx, (lane_k & 31) == place), 1.0, 0.0
        )
        ohs[g * 8 : g * 8 + 8, :] = jnp.where(lane_k == sx * 32 + place, 1.0, 0.0)
        q0 = codes[0, g * 8 : g * 8 + 8, :]
        q1 = codes[1, g * 8 : g * 8 + 8, :]
        q2 = codes[2, g * 8 : g * 8 + 8, :]
        q3 = codes[3, g * 8 : g * 8 + 8, :]

        def unit(q):
            sign = 1 - 2 * (q & 1)
            axis = q >> 1
            return [jnp.where(axis == k, sign, 0) for k in range(3)]

        e1, e2 = unit(q1), unit(q3)
        off = [((q2 * 57) >> 9) - 1, 0, 0]
        third = (q2 * 43) >> 7
        off[1] = third - 3 * (off[0] + 1) - 1
        off[2] = q2 - 3 * third - 1
        first = [(q0 >> 5) + 2, ((q0 >> 3) & 3) + 2, (q0 & 7) + 2]
        nodes = [first, [first[k] + e1[k] for k in range(3)], [first[k] + off[k] for k in range(3)]]
        nodes.append([nodes[2][k] + e2[k] for k in range(3)])
        for n in range(4):
            x, y, z = nodes[n]
            kidx[n, g * 8 : g * 8 + 8, :] = x
            lidx[n, g * 8 : g * 8 + 8, :] = ((y + turn) & 7) * 16 + z
        for k in range(3):
            a, b = e1[k].astype(F32), e2[k].astype(F32)
            geo[k, g * 8 : g * 8 + 8, :] = a
            geo[3 + k, g * 8 : g * 8 + 8, :] = b
            geo[6 + k, g * 8 : g * 8 + 8, :] = off[k].astype(F32) + 0.5 * b - 0.5 * a
    for c in range(3):
        frozen[c] = jnp.zeros((tiles, 128), F32)
    zero_plane = jnp.zeros((64, 384), BF16)
    win[0] = zero_plane
    win[11] = zero_plane

    row128 = iota((128, 128), 0)

    def make_onehot(t, carry):
        for n in range(2):
            first = lidx[2 * n, pl.ds(t, 1), :]
            second = lidx[2 * n + 1, pl.ds(t, 1), :]
            sign = 1.0 if n else -1.0
            flat = jnp.where(jnp.logical_or(row128 == first, row128 == second), sign, 0.0).astype(BF16)
            onehot[t, n * 128 : (n + 1) * 128, :] = jnp.transpose(flat)
        return carry

    lax.fori_loop(0, tiles, make_onehot, 0, unroll=4)
    pick = ohg[...].astype(BF16)
    spread_t = jnp.transpose(ohs[...])[0:64, 0:tiles].astype(BF16)
    spread = jnp.concatenate([spread_t, spread_t], axis=1)

    group_bits = [((lane8 >> 4) & bit) != 0 for bit in (1, 2, 4)]
    unroll = [(lane8 + 16 * row8 + 2 + 8 * p) & 127 for p in (0, 1)]
    edge_row = {0: row8 == 7, 1: row8 == 0}
    edge_lane = {0: lane8 == 127, 1: lane8 == 0}
    z_ok = {0: gz == 1, 1: gz == 0}
    my_edge_lane = lane8 == other_edge
    at_edge = lane8 == my_edge

    first_sum = Gathered(
        sq,
        ara,
        gy * 2 + gz,
        [(o, (gx, lax.rem(gy + o // 2, ny), lax.rem(gz + o, 2))) for o in range(1, 2 * ny)],
        asend,
        arecv,
    )
    second_sum = Gathered(
        sq2, arb, gx, [(o, (lax.rem(gx + o, nx), gy, gz)) for o in range(1, nx)], bsend, brecv
    )

    def hail(semaphore, width):
        for dx in (-width, width):
            cond = gx + dx >= 0 if dx < 0 else gx + dx < nx

            def signal(dx=dx):
                pl.semaphore_signal(
                    semaphore, inc=1, device_id=(gx + dx, gy, gz), device_id_type=MESH
                )

            pl.when(cond)(signal)

    def hear(semaphore, width):
        pl.semaphore_wait(semaphore, (gx >= width).astype(I32) + (gx + width < nx).astype(I32))

    def iteration(it, carry):
        wait_arrivals(displacement_message, it, 2 * it, NEAR)

        beyond_rows = [
            [take(valid(y_ok[dy], rxye[it, lo_hi(dy)]), lane_index[c]) for c in range(3)] for dy in (-1, 1)
        ]
        def make_windows(x):
            for c in range(3):
                if 1 <= x <= 8:
                    own, other = uc[c, x - 1], rxz[it, c, x - 1]
                    rows = [
                        [
                            valid(y_ok[dy], rxy[it, lo_hi(dy), c, x - 1 : x, :]),
                            beyond_rows[lo_hi(dy)][c][x - 1 : x],
                        ]
                        for dy in (-1, 1)
                    ]
                else:
                    dx, xi = (-1, 0) if x == 0 else (1, 1)
                    own = valid(x_ok[dx], rxx[it, xi, c])
                    other = take(valid(x_ok[dx], rxxe[it, xi]), lane_index[c])
                    rows = [
                        [
                            valid(exists(dx, dy), rxd[it, xi, lo_hi(dy), z, c : c + 1, :])
                            for z in (0, 1)
                        ]
                        for dy in (-1, 1)
                    ]
                for s in range(2):
                    near = jnp.where(edge_row[s], rows[s][0], own)
                    far = jnp.where(edge_row[s], rows[s][1], other)
                    pair = []
                    for p in range(2):
                        source = jnp.where(edge_lane[p], jnp.where(z_ok[p], far, 0.0), near)
                        v = pltpu.roll(source, 2 + 8 * p, axis=1, stride=16, stride_axis=0)
                        for bit, mask in zip((1, 2, 4), group_bits):
                            v = jnp.where(mask, pltpu.roll(v, 8 - bit, axis=0), v)
                        pair.append(v)
                    both = jnp.concatenate(pair, axis=0)
                    hi, lo = split(both)
                    win[x + 1, s * 16 : s * 16 + 16, c * 128 : (c + 1) * 128] = hi.astype(BF16)
                    win[x + 1, 32 + s * 16 : 48 + s * 16, c * 128 : (c + 1) * 128] = lo.astype(BF16)

        def hand_out(k):
            both = jnp.concatenate([win[k], win[k + 4]], axis=0)
            gat[k] = jnp.dot(pick, both, preferred_element_type=F32)

        for x in range(1, 9):
            make_windows(x)
        for k in (0, 2, 3, 4, 5, 7):
            hand_out(k)
        wait_arrivals(displacement_message, it, 2 * it, FAR)
        for x in (0, 9):
            make_windows(x)
        for k in (1, 6):
            hand_out(k)

        @pl.when(it == 2)
        def _():
            hear(hail_four, 4)
            hail(hail_eight, 8)

        wait_sends(displacement_message, it, 2 * it)

        live_below = jnp.where(it == 0, 2, 1)

        def pair_forces(g):
            at = pl.ds(pl.multiple_of(g * 8, 8), 8)
            points = []
            for n in range(4):
                ks = kidx[n, at, :]
                ls = lidx[n, at, :]
                least, most = ((2, 5), (1, 6), (1, 6), (0, 7))[n]
                found = []
                for c in range(3):
                    value = take(gat[least, at, c * 128 : (c + 1) * 128], ls)
                    for k in range(least + 1, most + 1):
                        value = jnp.where(ks == k, take(gat[k, at, c * 128 : (c + 1) * 128], ls), value)
                    found.append(value)
                points.append(found)
            one = [points[1][c] - points[0][c] + geo[c, at, :] for c in range(3)]
            two = [points[3][c] - points[2][c] + geo[3 + c, at, :] for c in range(3)]
            apart = [
                0.5 * (points[2][c] + points[3][c]) - 0.5 * (points[0][c] + points[1][c])
                + geo[6 + c, at, :]
                for c in range(3)
            ]
            square = apart[0] * apart[0] + apart[1] * apart[1] + apart[2] * apart[2] + 0.5
            dots = one[0] * two[0] + one[1] * two[1] + one[2] * two[2]
            coupling = 0.5 * dots / (square * jnp.sqrt(square))
            fresh = groups[at, :] < live_below
            values = []
            for c in range(3):
                force = jnp.where(fresh, coupling * apart[c], frozen[c, at, :])
                frozen[c, at, :] = force
                values.extend(split(0.5 * force))
            return tuple(values)

        def spread_forces(g, values):
            for i in range(8):
                t = g * 8 + i
                columns = []
                for n in range(2):
                    mask = jnp.logical_or(
                        row8 == kidx[2 * n, pl.ds(t, 1), :], row8 == kidx[2 * n + 1, pl.ds(t, 1), :]
                    )
                    columns.append(
                        jnp.concatenate(
                            [jnp.where(mask, v[i : i + 1], 0.0) for v in values], axis=0
                        ).astype(BF16)
                    )
                lhs = jnp.concatenate(columns, axis=1)
                got = jnp.dot(lhs, onehot[t], preferred_element_type=F32)
                for c in range(3):
                    outs[c, pl.ds(pl.multiple_of(t * 8, 8), 8), :] = (
                        got[16 * c : 16 * c + 8] + got[16 * c + 8 : 16 * c + 16]
                    )

        def group(g, values):
            later = pair_forces(g)
            spread_forces(g - 1, values)
            return later

        values = lax.fori_loop(1, tiles // 8, group, pair_forces(0))
        spread_forces(tiles // 8 - 1, values)

        def collect(k):
            columns = []
            for c in range(3):
                hi, lo = split(outs[c, pl.ds(k, tiles, stride=8), :])
                columns.append(jnp.concatenate([hi, lo], axis=0).astype(BF16))
            acc[k] = jnp.dot(spread, jnp.concatenate(columns, axis=1), preferred_element_type=F32)

        def fold(x):
            for c in range(3):
                cut = slice(c * 128, (c + 1) * 128)
                parts = []
                for s in range(2):
                    line, beyond = None, None
                    for p in range(2):
                        at = s * 16 + p * 8
                        v = None
                        if x + 1 <= 7:
                            v = acc[x + 1, at : at + 8, cut]
                        if x + 1 >= 4:
                            w = acc[x - 3, 32 + at : 40 + at, cut]
                            v = w if v is None else v + w
                        for bit, mask in zip((1, 2, 4), group_bits):
                            v = jnp.where(mask, pltpu.roll(v, bit, axis=0), v)
                        v = take(v, unroll[p])
                        inside = jnp.where(edge_lane[p], 0.0, v)
                        outside = jnp.where(z_ok[p], v, 0.0)
                        line = inside if line is None else line + inside
                        beyond = outside if beyond is None else beyond + outside
                    parts.append((line, jnp.where(my_edge_lane, beyond, 0.0)))
                for z in range(2):
                    (pz if z else pb)[c, x] = jnp.where(edge_row[0], 0.0, parts[0][z]) + jnp.where(
                        edge_row[1], 0.0, parts[1][z]
                    )
                    ends = (parts[0][z][7:8], parts[1][z][0:1])
                    for yi in range(2):
                        if 1 <= x <= 8:
                            yr[z, yi, c, x - 1 : x, :] = ends[yi]
                        else:
                            fd[z, 0 if x == 0 else 1, yi, c : c + 1, :] = ends[yi]

        for k in (1, 6):
            collect(k)
        for x in (0, 9):
            fold(x)
        for i in range(2):
            fxe[i] = edges([pz[c, 9 * i] for c in range(3)], other_edge_index)
        start(force_message, it, 2 * it + 1, FAR)
        for k in (0, 2, 3, 4, 5, 7):
            collect(k)
        for x in range(1, 9):
            fold(x)
        for i in range(2):
            fye[i] = edges([yr[1, i, c] for c in range(3)], other_edge_index)
        start(force_message, it, 2 * it + 1, NEAR)
        wait_arrivals(force_message, it, 2 * it + 1, NEAR)

        lines = []
        for dy in (-1, 1):
            yi = lo_hi(dy)
            lines.append(
                [
                    valid(
                        y_ok[dy],
                        fry[it, yi, c] + jnp.where(at_edge, take(frye[it, yi], lane_index[c]), 0.0),
                    )
                    for c in range(3)
                ]
            )
        def residual_of(x, squares):
            for c in range(3):
                total = pb[c, x + 1] + frz[it, c, x]
                for dx, xe in ((-1, 0), (1, 7)):
                    if x == xe:
                        xi = lo_hi(dx)
                        total = total + valid(
                            x_ok[dx],
                            frx[it, xi, c] + jnp.where(at_edge, take(frxe[it, xi], lane_index[c]), 0.0),
                        )
                for dy in (-1, 1):
                    yi = lo_hi(dy)
                    line = lines[yi][c][x : x + 1]
                    for dx, xe in ((-1, 0), (1, 7)):
                        if x == xe:
                            xi = lo_hi(dx)
                            line = line + valid(
                                exists(dx, dy),
                                frd[it, xi, yi, 0, c : c + 1, :] + frd[it, xi, yi, 1, c : c + 1, :],
                            )
                    total = total + jnp.where(row8 == (0 if dy < 0 else 7), line, 0.0)
                r = uc[c, x] - uold[c, x] - 0.5 * total
                squares = squares + r * r
                residuals[c, x] = r
            return squares

        def update(x):
            residual = [residuals[c, x] for c in range(3)]
            for a in range(3):
                fix = jac[a, 0, x] * residual[0] + jac[a, 1, x] * residual[1] + jac[a, 2, x] * residual[2]
                new = uc[a, x] - fix
                uc[a, x] = new
                uy[0, a, x : x + 1, :] = new[0:1]
                uy[1, a, x : x + 1, :] = new[7:8]

        squares = jnp.zeros((8, 128), F32)
        for x in range(1, 7):
            squares = residual_of(x, squares)
        for x in range(1, 7):
            update(x)
        wait_arrivals(force_message, it, 2 * it + 1, FAR)

        @pl.when(it == 1)
        def _():
            hail(hail_four, 4)

        @pl.when(it == 2)
        def _():
            hear(hail_eight, 8)

        for x in (0, 7):
            squares = residual_of(x, squares)
        sq[pl.ds(it, 1), :] = jnp.sum(squares, axis=0, keepdims=True)

        @pl.when(it == ITERS - 1)
        def _():
            first_sum.start()

        for x in (0, 7):
            update(x)
        wait_sends(force_message, it, 2 * it + 1)

        @pl.when(it < ITERS - 1)
        def _():
            pack_far()
            start(displacement_message, it + 1, 2 * it + 2, FAR)
            pack_near()
            start(displacement_message, it + 1, 2 * it + 2, NEAR)

        return carry

    sq[...] = jnp.zeros((8, 128), F32)
    lax.fori_loop(0, ITERS, iteration, 0)
    store_result = pltpu.make_async_copy(uc, uout, in_sem.at[0])
    store_result.start()
    plane = first_sum.finish()
    second_sum.source[...] = plane
    second_sum.start()
    total = second_sum.finish()
    norms = jnp.sqrt(jnp.sum(total, axis=1, keepdims=True) / cells)
    for k in range(ITERS):
        nout[k] = jnp.sum(norms[k : k + 1, :])
    store_result.wait()


def solution(mesh):
    nx, ny = mesh.shape["gx"], mesh.shape["gy"]

    def step(u_old, u_trial, jacobian_inverse, tile_base, pair_codes, pair_groups):
        tiles = tile_base.shape[0]
        cells = float(3 * 8 * 8 * 128 * nx * ny * mesh.shape["gz"])
        smem = pl.BlockSpec(memory_space=pltpu.SMEM)
        v = pltpu.VMEM
        return pl.pallas_call(
            functools.partial(kernel, nx, ny, cells),
            out_shape=(
                jax.ShapeDtypeStruct(u_old.shape, F32),
                jax.ShapeDtypeStruct((ITERS,), F32),
            ),
            in_specs=[pl.BlockSpec(memory_space=pltpu.HBM)] * 6,
            out_specs=(pl.BlockSpec(memory_space=pl.ANY), smem),
            scratch_shapes=[
                pltpu.SMEM(tile_base.shape, I32),
                v(u_old.shape, F32),
                v(jacobian_inverse.shape, F32),
                v(pair_codes.shape, I32),
                v(pair_groups.shape, I32),
                v(u_old.shape, F32),
                v((3, 8, 8, 128), F32),
                v((2, 3, 8, 128), F32),
                v((2, 8, 128), F32),
                v((2, 8, 128), F32),
                v((2, 2, 8, 128), F32),
                v((ITERS, 3, 8, 8, 128), F32),
                v((ITERS, 2, 3, 8, 128), F32),
                v((ITERS, 2, 3, 8, 128), F32),
                v((ITERS, 2, 8, 128), F32),
                v((ITERS, 2, 8, 128), F32),
                v((ITERS, 2, 2, 2, 8, 128), F32),
                v((3, 10, 8, 128), F32),
                v((3, 10, 8, 128), F32),
                v((2, 2, 3, 8, 128), F32),
                v((2, 8, 128), F32),
                v((2, 8, 128), F32),
                v((2, 2, 2, 8, 128), F32),
                v((ITERS, 3, 8, 8, 128), F32),
                v((ITERS, 2, 3, 8, 128), F32),
                v((ITERS, 2, 3, 8, 128), F32),
                v((ITERS, 2, 8, 128), F32),
                v((ITERS, 2, 8, 128), F32),
                v((ITERS, 2, 2, 2, 8, 128), F32),
                v((12, 64, 384), BF16),
                v((8, tiles, 384), F32),
                v((4, tiles, 128), I32),
                v((4, tiles, 128), I32),
                v((9, tiles, 128), F32),
                v((3, tiles, 128), F32),
                v((tiles, 256, 128), BF16),
                v((tiles, 128), F32),
                v((tiles, 128), F32),
                v((3, tiles * 8, 128), F32),
                v((8, 64, 384), F32),
                v((8, 128), F32),
                v((8, 128), F32),
                v((2 * ny, 8, 128), F32),
                v((nx, 8, 128), F32),
                pltpu.SemaphoreType.REGULAR,
                pltpu.SemaphoreType.REGULAR,
                pltpu.SemaphoreType.DMA((6,)),
                pltpu.SemaphoreType.DMA((2 * ITERS, 18)),
                pltpu.SemaphoreType.DMA((2 * ITERS, 18)),
                pltpu.SemaphoreType.DMA((2 * ny,)),
                pltpu.SemaphoreType.DMA((2 * ny,)),
                pltpu.SemaphoreType.DMA((nx,)),
                pltpu.SemaphoreType.DMA((nx,)),
            ],
            compiler_params=pltpu.CompilerParams(
                collective_id=0, has_side_effects=True, vmem_limit_bytes=24 * 2**20
            ),
            name="relax",
        )(
            *(
                pltpu.with_memory_space_constraint(a, pltpu.HBM)
                for a in (tile_base, u_old, u_trial, jacobian_inverse, pair_codes, pair_groups)
            )
        )

    everywhere = ("gx", "gy", "gz")
    return jax.shard_map(
        step,
        mesh=mesh,
        in_specs=(
            P(None, "gx", "gy", "gz"),
            P(None, "gx", "gy", "gz"),
            P(None, None, "gx", "gy", "gz"),
            P(everywhere),
            P(None, everywhere, None),
            P(everywhere, None),
        ),
        out_specs=(P(None, "gx", "gy", "gz"), P()),
        check_vma=False,
    )
```

```python
import functools

import jax
import jax.numpy as jnp
from jax import lax
from jax.experimental import pallas as pl
from jax.experimental.pallas import tpu as pltpu
from jax.sharding import PartitionSpec as P

ITERS = 3
MESH = pl.DeviceIdType.MESH
F32 = jnp.float32
BF16 = jnp.bfloat16
I32 = jnp.int32

DIRS = sorted(
    [
        (dx, dy, z)
        for dx in (-1, 0, 1)
        for dy in (-1, 0, 1)
        for z in (0, 1)
        if (dx, dy, z) != (0, 0, 0)
    ],
    key=lambda d: (-2 * abs(d[0]) - abs(d[1]), d),
)


FAR = [d for d in DIRS if d[0] != 0]
NEAR = [d for d in DIRS if d[0] == 0]


def slot_of(dx, dy, z):
    return ((dx + 1) * 3 + dy + 1) * 2 + z


def iota(shape, dim):
    return lax.broadcasted_iota(I32, shape, dim)


def take(x, idx):
    return jnp.take_along_axis(x, idx, axis=1, mode="promise_in_bounds")


def split(x):
    hi = x.astype(BF16).astype(F32)
    return hi, x - hi


def kernel(
    nx, ny, cells,
    tb_in, uold_in, utrial_in, jac_in, codes_in, groups_in,
    uout, nout,
    tb_ref, uold, jac, codes, groups, residuals,
    uc, uy, uxe, uye, ud, rxz, rxx, rxy, rxxe, rxye, rxd,
    pb, pz, yr, fxe, fye, fd, frz, frx, fry, frxe, frye, frd,
    win, gat, kidx, lidx, geo, frozen, onehot, ohg, ohs, outs, acc,
    sq, total_row, table,
    hail_four, hail_eight, in_sem, send_sem, recv_sem, total_send, total_recv,
):
    gx, gy, gz = lax.axis_index("gx"), lax.axis_index("gy"), lax.axis_index("gz")
    tiles = groups.shape[0]
    x_ok = {-1: gx > 0, 0: None, 1: gx < nx - 1}
    y_ok = {-1: gy > 0, 0: None, 1: gy < ny - 1}

    def exists(dx, dy):
        if dx == 0 and dy == 0:
            return None
        if dx == 0:
            return y_ok[dy]
        if dy == 0:
            return x_ok[dx]
        return jnp.logical_and(x_ok[dx], y_ok[dy])

    def guarded(cond, fn):
        if cond is None:
            fn()
        else:
            pl.when(cond)(fn)

    def valid(cond, value):
        return value if cond is None else jnp.where(cond, value, 0.0)

    def target(dx, dy, z):
        return (gx + dx, gy + dy, gz if z == 0 else 1 - gz)

    barrier = pltpu.get_barrier_semaphore()

    def greet(device):
        pl.semaphore_signal(barrier, inc=1, device_id=device, device_id_type=MESH)

    for d in DIRS:
        guarded(exists(d[0], d[1]), functools.partial(greet, target(*d)))

    fetches = [
        pltpu.make_async_copy(src, dst, in_sem.at[k])
        for k, (src, dst) in enumerate(
            [
                (utrial_in, uc),
                (tb_in, tb_ref),
                (codes_in, codes),
                (groups_in, groups),
                (uold_in, uold),
                (jac_in, jac),
            ]
        )
    ]
    for fetch in fetches:
        fetch.start()

    def lo_hi(d):
        return 1 if d > 0 else 0

    def displacement_message(it, d):
        dx, dy, z = d
        xi, yi = lo_hi(dx), lo_hi(dy)
        if dx == 0 and dy == 0:
            return uc, rxz.at[it]
        if dy == 0:
            if z:
                return uxe.at[xi], rxxe.at[it, 1 - xi]
            return uc.at[:, 7 * xi], rxx.at[it, 1 - xi]
        if dx == 0:
            if z:
                return uye.at[yi], rxye.at[it, 1 - yi]
            return uy.at[yi], rxy.at[it, 1 - yi]
        return ud.at[xi, yi], rxd.at[it, 1 - xi, 1 - yi, z]

    def force_message(it, d):
        dx, dy, z = d
        xi, yi = lo_hi(dx), lo_hi(dy)
        if dx == 0 and dy == 0:
            return pz.at[:, 1:9], frz.at[it]
        if dy == 0:
            if z:
                return fxe.at[xi], frxe.at[it, 1 - xi]
            return pb.at[:, 9 * xi], frx.at[it, 1 - xi]
        if dx == 0:
            if z:
                return fye.at[yi], frye.at[it, 1 - yi]
            return yr.at[0, yi], fry.at[it, 1 - yi]
        return fd.at[z, xi, yi], frd.at[it, 1 - xi, 1 - yi, z]

    def copy_of(message, it, phase, d):
        src, dst = message(it, d)
        dx, dy, z = d
        return pltpu.make_async_remote_copy(
            src_ref=src,
            dst_ref=dst,
            send_sem=send_sem.at[phase, slot_of(dx, dy, z)],
            recv_sem=recv_sem.at[phase, slot_of(-dx, -dy, z)],
            device_id=target(dx, dy, z),
            device_id_type=MESH,
        )

    def grouped(dirs, act):
        for dx, dy in dict.fromkeys((d[0], d[1]) for d in dirs):

            def both(dx=dx, dy=dy):
                for d in dirs:
                    if (d[0], d[1]) == (dx, dy):
                        act(d)

            guarded(exists(dx, dy), both)

    def start(message, it, phase, dirs):
        grouped(dirs, lambda d: copy_of(message, it, phase, d).start())

    def wait_arrivals(message, it, phase, dirs):
        grouped(dirs, lambda d: copy_of(message, it, phase, (-d[0], -d[1], d[2])).wait_recv())

    def wait_sends(message, it, phase):
        grouped(DIRS, lambda d: copy_of(message, it, phase, d).wait_send())

    row8 = iota((8, 128), 0)
    lane8 = iota((8, 128), 1)

    my_edge = jnp.where(gz == 0, 127, 0)
    other_edge = 127 - my_edge
    my_edge_index = jnp.full((8, 128), my_edge, I32)
    other_edge_index = jnp.full((8, 128), other_edge, I32)
    lane_index = [jnp.full((8, 128), c, I32) for c in range(3)]

    def edges(planes, index):
        packed = take(planes[0], index)
        for c in (1, 2):
            packed = jnp.where(lane8 == c, take(planes[c], index), packed)
        return packed

    def pack_far():
        for xi, x in ((0, 0), (1, 7)):
            uxe[xi] = edges([uc[c, x] for c in range(3)], my_edge_index)
            for yi in range(2):
                for c in range(3):
                    ud[xi, yi, c : c + 1, :] = uy[yi, c, x : x + 1, :]

    def pack_near():
        for yi in range(2):
            uye[yi] = edges([uy[yi, c] for c in range(3)], my_edge_index)

    fetches[0].wait()
    for c in range(3):
        for x in range(8):
            plane = uc[c, x]
            uy[0, c, x : x + 1, :] = plane[0:1]
            uy[1, c, x : x + 1, :] = plane[7:8]
    pack_far()
    pack_near()
    beside_x = (gx > 0).astype(I32) + (gx < nx - 1).astype(I32)
    beside_y = (gy > 0).astype(I32) + (gy < ny - 1).astype(I32)
    pl.semaphore_wait(barrier, 2 * (1 + beside_x) * (1 + beside_y) - 1)
    start(displacement_message, 0, 0, DIRS)

    for fetch in fetches[1:]:
        fetch.wait()
    lane_k = iota((8, 128), 1)
    for g in range(tiles // 8):
        base = jnp.zeros((8, 128), I32)
        for i in range(8):
            base = jnp.where(row8 == i, tb_ref[g * 8 + i], base)
        s = (base >> 4) & 1
        sz = base & 15
        par = sz & 1
        j = sz >> 1
        sx = base >> 5
        i_of = (16 - j - par) & 7
        turn = j + par + jnp.where(s == 0, -2, 2)
        place = s * 16 + par * 8 + i_of
        ohg[g * 8 : g * 8 + 8, :] = jnp.where(
            jnp.logical_and((lane_k >> 6) == sx, (lane_k & 31) == place), 1.0, 0.0
        )
        ohs[g * 8 : g * 8 + 8, :] = jnp.where(lane_k == sx * 32 + place, 1.0, 0.0)
        q0 = codes[0, g * 8 : g * 8 + 8, :]
        q1 = codes[1, g * 8 : g * 8 + 8, :]
        q2 = codes[2, g * 8 : g * 8 + 8, :]
        q3 = codes[3, g * 8 : g * 8 + 8, :]

        def unit(q):
            sign = 1 - 2 * (q & 1)
            axis = q >> 1
            return [jnp.where(axis == k, sign, 0) for k in range(3)]

        e1, e2 = unit(q1), unit(q3)
        off = [((q2 * 57) >> 9) - 1, 0, 0]
        third = (q2 * 43) >> 7
        off[1] = third - 3 * (off[0] + 1) - 1
        off[2] = q2 - 3 * third - 1
        first = [(q0 >> 5) + 2, ((q0 >> 3) & 3) + 2, (q0 & 7) + 2]
        nodes = [first, [first[k] + e1[k] for k in range(3)], [first[k] + off[k] for k in range(3)]]
        nodes.append([nodes[2][k] + e2[k] for k in range(3)])
        for n in range(4):
            x, y, z = nodes[n]
            kidx[n, g * 8 : g * 8 + 8, :] = x
            lidx[n, g * 8 : g * 8 + 8, :] = ((y + turn) & 7) * 16 + z
        for k in range(3):
            a, b = e1[k].astype(F32), e2[k].astype(F32)
            geo[k, g * 8 : g * 8 + 8, :] = a
            geo[3 + k, g * 8 : g * 8 + 8, :] = b
            geo[6 + k, g * 8 : g * 8 + 8, :] = off[k].astype(F32) + 0.5 * b - 0.5 * a
    for c in range(3):
        frozen[c] = jnp.zeros((tiles, 128), F32)
    zero_plane = jnp.zeros((64, 384), BF16)
    win[0] = zero_plane
    win[11] = zero_plane

    row128 = iota((128, 128), 0)

    def make_onehot(t, carry):
        for n in range(2):
            first = lidx[2 * n, pl.ds(t, 1), :]
            second = lidx[2 * n + 1, pl.ds(t, 1), :]
            sign = 1.0 if n else -1.0
            flat = jnp.where(jnp.logical_or(row128 == first, row128 == second), sign, 0.0).astype(BF16)
            onehot[t, n * 128 : (n + 1) * 128, :] = jnp.transpose(flat)
        return carry

    lax.fori_loop(0, tiles, make_onehot, 0, unroll=4)
    pick = ohg[...].astype(BF16)
    spread_t = jnp.transpose(ohs[...])[0:64, 0:tiles].astype(BF16)
    spread = jnp.concatenate([spread_t, spread_t], axis=1)

    group_bits = [((lane8 >> 4) & bit) != 0 for bit in (1, 2, 4)]
    unroll = [(lane8 + 16 * row8 + 2 + 8 * p) & 127 for p in (0, 1)]
    edge_row = {0: row8 == 7, 1: row8 == 0}
    edge_lane = {0: lane8 == 127, 1: lane8 == 0}
    z_ok = {0: gz == 1, 1: gz == 0}
    my_edge_lane = lane8 == other_edge
    at_edge = lane8 == my_edge

    count = 2 * nx * ny
    me = (gx * ny + gy) * 2 + gz

    xs = [lax.rem(gx + a, nx) for a in range(nx)]
    ys = [lax.rem(gy + b, ny) for b in range(ny)]

    def ring(o, n):
        return min(o, n - o)

    offsets = [(a, b, c) for a in range(nx) for b in range(ny) for c in range(2) if (a, b, c) != (0, 0, 0)]
    offsets.sort(
        key=lambda o: -(ring(o[0] // 4, nx // 4) + ring(o[0] % 4, 4) + ring(o[1], ny))
    )

    def send_squares():
        for a, b, c in offsets:
            pltpu.make_async_remote_copy(
                src_ref=total_row,
                dst_ref=table.at[me],
                send_sem=total_send,
                recv_sem=total_recv,
                device_id=(xs[a], ys[b], 1 - gz if c else gz),
                device_id_type=MESH,
            ).start()

    def hail(semaphore, width):
        for dx in (-width, width):
            cond = gx + dx >= 0 if dx < 0 else gx + dx < nx

            def signal(dx=dx):
                pl.semaphore_signal(
                    semaphore, inc=1, device_id=(gx + dx, gy, gz), device_id_type=MESH
                )

            pl.when(cond)(signal)

    def hear(semaphore, width):
        pl.semaphore_wait(semaphore, (gx >= width).astype(I32) + (gx + width < nx).astype(I32))

    def iteration(it, carry):
        wait_arrivals(displacement_message, it, 2 * it, NEAR)

        beyond_rows = [
            [take(valid(y_ok[dy], rxye[it, lo_hi(dy)]), lane_index[c]) for c in range(3)] for dy in (-1, 1)
        ]
        def make_windows(x):
            for c in range(3):
                if 1 <= x <= 8:
                    own, other = uc[c, x - 1], rxz[it, c, x - 1]
                    rows = [
                        [
                            valid(y_ok[dy], rxy[it, lo_hi(dy), c, x - 1 : x, :]),
                            beyond_rows[lo_hi(dy)][c][x - 1 : x],
                        ]
                        for dy in (-1, 1)
                    ]
                else:
                    dx, xi = (-1, 0) if x == 0 else (1, 1)
                    own = valid(x_ok[dx], rxx[it, xi, c])
                    other = take(valid(x_ok[dx], rxxe[it, xi]), lane_index[c])
                    rows = [
                        [
                            valid(exists(dx, dy), rxd[it, xi, lo_hi(dy), z, c : c + 1, :])
                            for z in (0, 1)
                        ]
                        for dy in (-1, 1)
                    ]
                for s in range(2):
                    near = jnp.where(edge_row[s], rows[s][0], own)
                    far = jnp.where(edge_row[s], rows[s][1], other)
                    pair = []
                    for p in range(2):
                        source = jnp.where(edge_lane[p], jnp.where(z_ok[p], far, 0.0), near)
                        v = pltpu.roll(source, 2 + 8 * p, axis=1, stride=16, stride_axis=0)
                        for bit, mask in zip((1, 2, 4), group_bits):
                            v = jnp.where(mask, pltpu.roll(v, 8 - bit, axis=0), v)
                        pair.append(v)
                    both = jnp.concatenate(pair, axis=0)
                    hi, lo = split(both)
                    win[x + 1, s * 16 : s * 16 + 16, c * 128 : (c + 1) * 128] = hi.astype(BF16)
                    win[x + 1, 32 + s * 16 : 48 + s * 16, c * 128 : (c + 1) * 128] = lo.astype(BF16)

        def hand_out(k):
            both = jnp.concatenate([win[k], win[k + 4]], axis=0)
            gat[k] = jnp.dot(pick, both, preferred_element_type=F32)

        for x in range(1, 9):
            make_windows(x)
        for k in (0, 2, 3, 4, 5, 7):
            hand_out(k)

        @pl.when(it > 0)
        def _():
            wait_sends(force_message, it - 1, 2 * it - 1)

        wait_arrivals(displacement_message, it, 2 * it, FAR)
        for x in (0, 9):
            make_windows(x)
        for k in (1, 6):
            hand_out(k)

        @pl.when(it == 2)
        def _():
            hear(hail_four, 4)
            hail(hail_eight, 8)

        live_below = jnp.where(it == 0, 2, 1)

        def pair_forces(g):
            at = pl.ds(pl.multiple_of(g * 8, 8), 8)
            points = []
            for n in range(4):
                ks = kidx[n, at, :]
                ls = lidx[n, at, :]
                least, most = ((2, 5), (1, 6), (1, 6), (0, 7))[n]
                found = []
                for c in range(3):
                    value = take(gat[least, at, c * 128 : (c + 1) * 128], ls)
                    for k in range(least + 1, most + 1):
                        value = jnp.where(ks == k, take(gat[k, at, c * 128 : (c + 1) * 128], ls), value)
                    found.append(value)
                points.append(found)
            one = [points[1][c] - points[0][c] + geo[c, at, :] for c in range(3)]
            two = [points[3][c] - points[2][c] + geo[3 + c, at, :] for c in range(3)]
            apart = [
                0.5 * (points[2][c] + points[3][c]) - 0.5 * (points[0][c] + points[1][c])
                + geo[6 + c, at, :]
                for c in range(3)
            ]
            square = apart[0] * apart[0] + apart[1] * apart[1] + apart[2] * apart[2] + 0.5
            dots = one[0] * two[0] + one[1] * two[1] + one[2] * two[2]
            coupling = 0.5 * dots / (square * jnp.sqrt(square))
            fresh = groups[at, :] < live_below
            values = []
            for c in range(3):
                force = jnp.where(fresh, coupling * apart[c], frozen[c, at, :])
                frozen[c, at, :] = force
                values.extend(split(0.5 * force))
            return tuple(values)

        def spread_forces(g, values):
            for i in range(8):
                t = g * 8 + i
                columns = []
                for n in range(2):
                    mask = jnp.logical_or(
                        row8 == kidx[2 * n, pl.ds(t, 1), :], row8 == kidx[2 * n + 1, pl.ds(t, 1), :]
                    )
                    columns.append(
                        jnp.concatenate(
                            [jnp.where(mask, v[i : i + 1], 0.0) for v in values], axis=0
                        ).astype(BF16)
                    )
                lhs = jnp.concatenate(columns, axis=1)
                got = jnp.dot(lhs, onehot[t], preferred_element_type=F32)
                for c in range(3):
                    outs[c, pl.ds(pl.multiple_of(t * 8, 8), 8), :] = (
                        got[16 * c : 16 * c + 8] + got[16 * c + 8 : 16 * c + 16]
                    )

        def group(g, values):
            later = pair_forces(g)
            spread_forces(g - 1, values)
            return later

        values = lax.fori_loop(1, tiles // 8, group, pair_forces(0))
        spread_forces(tiles // 8 - 1, values)

        def collect(k):
            columns = []
            for c in range(3):
                hi, lo = split(outs[c, pl.ds(k, tiles, stride=8), :])
                columns.append(jnp.concatenate([hi, lo], axis=0).astype(BF16))
            acc[k] = jnp.dot(spread, jnp.concatenate(columns, axis=1), preferred_element_type=F32)

        def fold(x):
            for c in range(3):
                cut = slice(c * 128, (c + 1) * 128)
                parts = []
                for s in range(2):
                    line, beyond = None, None
                    for p in range(2):
                        at = s * 16 + p * 8
                        v = None
                        if x + 1 <= 7:
                            v = acc[x + 1, at : at + 8, cut]
                        if x + 1 >= 4:
                            w = acc[x - 3, 32 + at : 40 + at, cut]
                            v = w if v is None else v + w
                        for bit, mask in zip((1, 2, 4), group_bits):
                            v = jnp.where(mask, pltpu.roll(v, bit, axis=0), v)
                        v = take(v, unroll[p])
                        inside = jnp.where(edge_lane[p], 0.0, v)
                        outside = jnp.where(z_ok[p], v, 0.0)
                        line = inside if line is None else line + inside
                        beyond = outside if beyond is None else beyond + outside
                    parts.append((line, jnp.where(my_edge_lane, beyond, 0.0)))
                for z in range(2):
                    (pz if z else pb)[c, x] = jnp.where(edge_row[0], 0.0, parts[0][z]) + jnp.where(
                        edge_row[1], 0.0, parts[1][z]
                    )
                    ends = (parts[0][z][7:8], parts[1][z][0:1])
                    for yi in range(2):
                        if 1 <= x <= 8:
                            yr[z, yi, c, x - 1 : x, :] = ends[yi]
                        else:
                            fd[z, 0 if x == 0 else 1, yi, c : c + 1, :] = ends[yi]

        for k in (1, 6):
            collect(k)
        for x in (0, 9):
            fold(x)
        for i in range(2):
            fxe[i] = edges([pz[c, 9 * i] for c in range(3)], other_edge_index)
        start(force_message, it, 2 * it + 1, FAR)
        for k in (0, 2, 3, 4, 5, 7):
            collect(k)
        for x in range(1, 9):
            fold(x)
        for i in range(2):
            fye[i] = edges([yr[1, i, c] for c in range(3)], other_edge_index)
        start(force_message, it, 2 * it + 1, NEAR)
        wait_sends(displacement_message, it, 2 * it)
        wait_arrivals(force_message, it, 2 * it + 1, NEAR)

        lines = []
        for dy in (-1, 1):
            yi = lo_hi(dy)
            lines.append(
                [
                    valid(
                        y_ok[dy],
                        fry[it, yi, c] + jnp.where(at_edge, take(frye[it, yi], lane_index[c]), 0.0),
                    )
                    for c in range(3)
                ]
            )
        def residual_of(x, squares):
            for c in range(3):
                total = pb[c, x + 1] + frz[it, c, x]
                for dx, xe in ((-1, 0), (1, 7)):
                    if x == xe:
                        xi = lo_hi(dx)
                        total = total + valid(
                            x_ok[dx],
                            frx[it, xi, c] + jnp.where(at_edge, take(frxe[it, xi], lane_index[c]), 0.0),
                        )
                for dy in (-1, 1):
                    yi = lo_hi(dy)
                    line = lines[yi][c][x : x + 1]
                    for dx, xe in ((-1, 0), (1, 7)):
                        if x == xe:
                            xi = lo_hi(dx)
                            line = line + valid(
                                exists(dx, dy),
                                frd[it, xi, yi, 0, c : c + 1, :] + frd[it, xi, yi, 1, c : c + 1, :],
                            )
                    total = total + jnp.where(row8 == (0 if dy < 0 else 7), line, 0.0)
                r = uc[c, x] - uold[c, x] - 0.5 * total
                squares = squares + r * r
                residuals[c, x] = r
            return squares

        def update(x):
            residual = [residuals[c, x] for c in range(3)]
            for a in range(3):
                fix = jac[a, 0, x] * residual[0] + jac[a, 1, x] * residual[1] + jac[a, 2, x] * residual[2]
                new = uc[a, x] - fix
                uc[a, x] = new
                uy[0, a, x : x + 1, :] = new[0:1]
                uy[1, a, x : x + 1, :] = new[7:8]

        squares = jnp.zeros((8, 128), F32)
        for x in range(1, 7):
            squares = residual_of(x, squares)
        for x in range(1, 7):
            update(x)
        wait_arrivals(force_message, it, 2 * it + 1, FAR)

        @pl.when(it == 1)
        def _():
            hail(hail_four, 4)

        @pl.when(it == 2)
        def _():
            hear(hail_eight, 8)

        for x in (0, 7):
            squares = residual_of(x, squares)
        sq[pl.ds(it, 1), :] = jnp.sum(squares, axis=0, keepdims=True)

        @pl.when(it == ITERS - 1)
        def _():
            sums = jnp.sum(sq[...], axis=1, keepdims=True)
            row = jnp.sum(jnp.where(row8 == lane8, sums, 0.0), axis=0, keepdims=True)
            total_row[...] = row
            table[me] = row
            send_squares()

        for x in (0, 7):
            update(x)
        @pl.when(it < ITERS - 1)
        def _():
            pack_far()
            start(displacement_message, it + 1, 2 * it + 2, FAR)
            pack_near()
            start(displacement_message, it + 1, 2 * it + 2, NEAR)

        return carry

    sq[...] = jnp.zeros((8, 128), F32)
    lax.fori_loop(0, ITERS, iteration, 0)
    store_result = pltpu.make_async_copy(uc, uout, in_sem.at[0])
    store_result.start()
    wait_sends(force_message, ITERS - 1, 2 * ITERS - 1)
    others = table.at[0 : count - 1]
    pltpu.make_async_copy(others, others, total_recv).wait()
    pltpu.make_async_copy(others, others, total_send).wait()
    total = jnp.sum(table[...], axis=0)
    norms = jnp.sqrt(total / cells)
    for k in range(ITERS):
        nout[k] = jnp.sum(norms[:, k : k + 1])
    store_result.wait()


def solution(mesh):
    nx, ny = mesh.shape["gx"], mesh.shape["gy"]

    def step(u_old, u_trial, jacobian_inverse, tile_base, pair_codes, pair_groups):
        tiles = tile_base.shape[0]
        cells = float(3 * 8 * 8 * 128 * nx * ny * mesh.shape["gz"])
        smem = pl.BlockSpec(memory_space=pltpu.SMEM)
        v = pltpu.VMEM
        return pl.pallas_call(
            functools.partial(kernel, nx, ny, cells),
            out_shape=(
                jax.ShapeDtypeStruct(u_old.shape, F32),
                jax.ShapeDtypeStruct((ITERS,), F32),
            ),
            in_specs=[pl.BlockSpec(memory_space=pltpu.HBM)] * 6,
            out_specs=(pl.BlockSpec(memory_space=pl.ANY), smem),
            scratch_shapes=[
                pltpu.SMEM(tile_base.shape, I32),
                v(u_old.shape, F32),
                v(jacobian_inverse.shape, F32),
                v(pair_codes.shape, I32),
                v(pair_groups.shape, I32),
                v(u_old.shape, F32),
                v((3, 8, 8, 128), F32),
                v((2, 3, 8, 128), F32),
                v((2, 8, 128), F32),
                v((2, 8, 128), F32),
                v((2, 2, 8, 128), F32),
                v((ITERS, 3, 8, 8, 128), F32),
                v((ITERS, 2, 3, 8, 128), F32),
                v((ITERS, 2, 3, 8, 128), F32),
                v((ITERS, 2, 8, 128), F32),
                v((ITERS, 2, 8, 128), F32),
                v((ITERS, 2, 2, 2, 8, 128), F32),
                v((3, 10, 8, 128), F32),
                v((3, 10, 8, 128), F32),
                v((2, 2, 3, 8, 128), F32),
                v((2, 8, 128), F32),
                v((2, 8, 128), F32),
                v((2, 2, 2, 8, 128), F32),
                v((ITERS, 3, 8, 8, 128), F32),
                v((ITERS, 2, 3, 8, 128), F32),
                v((ITERS, 2, 3, 8, 128), F32),
                v((ITERS, 2, 8, 128), F32),
                v((ITERS, 2, 8, 128), F32),
                v((ITERS, 2, 2, 2, 8, 128), F32),
                v((12, 64, 384), BF16),
                v((8, tiles, 384), F32),
                v((4, tiles, 128), I32),
                v((4, tiles, 128), I32),
                v((9, tiles, 128), F32),
                v((3, tiles, 128), F32),
                v((tiles, 256, 128), BF16),
                v((tiles, 128), F32),
                v((tiles, 128), F32),
                v((3, tiles * 8, 128), F32),
                v((8, 64, 384), F32),
                v((8, 128), F32),
                v((1, 128), F32),
                v((2 * nx * ny, 1, 128), F32),
                pltpu.SemaphoreType.REGULAR,
                pltpu.SemaphoreType.REGULAR,
                pltpu.SemaphoreType.DMA((6,)),
                pltpu.SemaphoreType.DMA((2 * ITERS, 18)),
                pltpu.SemaphoreType.DMA((2 * ITERS, 18)),
                pltpu.SemaphoreType.DMA,
                pltpu.SemaphoreType.DMA,
            ],
            compiler_params=pltpu.CompilerParams(
                collective_id=0, has_side_effects=True, vmem_limit_bytes=24 * 2**20
            ),
            name="relax",
        )(
            *(
                pltpu.with_memory_space_constraint(a, pltpu.HBM)
                for a in (tile_base, u_old, u_trial, jacobian_inverse, pair_codes, pair_groups)
            )
        )

    everywhere = ("gx", "gy", "gz")
    return jax.shard_map(
        step,
        mesh=mesh,
        in_specs=(
            P(None, "gx", "gy", "gz"),
            P(None, "gx", "gy", "gz"),
            P(None, None, "gx", "gy", "gz"),
            P(everywhere),
            P(None, everywhere, None),
            P(everywhere, None),
        ),
        out_specs=(P(None, "gx", "gy", "gz"), P()),
        check_vma=False,
    )
```

```python
import functools

import jax
import jax.numpy as jnp
from jax import lax
from jax.experimental import pallas as pl
from jax.experimental.pallas import tpu as pltpu
from jax.sharding import PartitionSpec as P

ITERS = 3
MESH = pl.DeviceIdType.MESH
F32 = jnp.float32
BF16 = jnp.bfloat16
I32 = jnp.int32

DIRS = sorted(
    [
        (dx, dy, z)
        for dx in (-1, 0, 1)
        for dy in (-1, 0, 1)
        for z in (0, 1)
        if (dx, dy, z) != (0, 0, 0)
    ],
    key=lambda d: (-2 * abs(d[0]) - abs(d[1]), d),
)


FAR = [d for d in DIRS if d[0] != 0]
NEAR = [d for d in DIRS if d[0] == 0]


def slot_of(dx, dy, z):
    return ((dx + 1) * 3 + dy + 1) * 2 + z


def iota(shape, dim):
    return lax.broadcasted_iota(I32, shape, dim)


def take(x, idx):
    return jnp.take_along_axis(x, idx, axis=1, mode="promise_in_bounds")


def split(x):
    hi = x.astype(BF16).astype(F32)
    return hi, x - hi


def kernel(
    nx, ny, cells,
    tb_in, uold_in, utrial_in, jac_in, codes_in, groups_in,
    uout, nout,
    tb_ref, uold, jac, codes, groups, residuals,
    uc, uy, uxe, uye, ud, rxz, rxx, rxy, rxxe, rxye, rxd,
    pb, pz, yr, fxe, fye, fd, frz, frx, fry, frxe, frye, frd,
    win, gat, early, kidx, lidx, geo, frozen, onehot, ohg, ohs, outs, acc,
    sq, total_row, table,
    hail_four, hail_eight, in_sem, send_sem, recv_sem, total_send, total_recv,
):
    gx, gy, gz = lax.axis_index("gx"), lax.axis_index("gy"), lax.axis_index("gz")
    tiles = groups.shape[0]
    x_ok = {-1: gx > 0, 0: None, 1: gx < nx - 1}
    y_ok = {-1: gy > 0, 0: None, 1: gy < ny - 1}

    def exists(dx, dy):
        if dx == 0 and dy == 0:
            return None
        if dx == 0:
            return y_ok[dy]
        if dy == 0:
            return x_ok[dx]
        return jnp.logical_and(x_ok[dx], y_ok[dy])

    def guarded(cond, fn):
        if cond is None:
            fn()
        else:
            pl.when(cond)(fn)

    def valid(cond, value):
        return value if cond is None else jnp.where(cond, value, 0.0)

    def target(dx, dy, z):
        return (gx + dx, gy + dy, gz if z == 0 else 1 - gz)

    barrier = pltpu.get_barrier_semaphore()

    def greet(device):
        pl.semaphore_signal(barrier, inc=1, device_id=device, device_id_type=MESH)

    for d in DIRS:
        guarded(exists(d[0], d[1]), functools.partial(greet, target(*d)))

    fetches = [
        pltpu.make_async_copy(src, dst, in_sem.at[k])
        for k, (src, dst) in enumerate(
            [
                (utrial_in, uc),
                (tb_in, tb_ref),
                (codes_in, codes),
                (groups_in, groups),
                (uold_in, uold),
                (jac_in, jac),
            ]
        )
    ]
    for fetch in fetches:
        fetch.start()

    def lo_hi(d):
        return 1 if d > 0 else 0

    def displacement_message(it, d):
        dx, dy, z = d
        xi, yi = lo_hi(dx), lo_hi(dy)
        if dx == 0 and dy == 0:
            return uc, rxz.at[it]
        if dy == 0:
            if z:
                return uxe.at[xi], rxxe.at[it, 1 - xi]
            return uc.at[:, 7 * xi], rxx.at[it, 1 - xi]
        if dx == 0:
            if z:
                return uye.at[yi], rxye.at[it, 1 - yi]
            return uy.at[yi], rxy.at[it, 1 - yi]
        return ud.at[xi, yi], rxd.at[it, 1 - xi, 1 - yi, z]

    def force_message(it, d):
        dx, dy, z = d
        xi, yi = lo_hi(dx), lo_hi(dy)
        if dx == 0 and dy == 0:
            return pz.at[:, 1:9], frz.at[it]
        if dy == 0:
            if z:
                return fxe.at[xi], frxe.at[it, 1 - xi]
            return pb.at[:, 9 * xi], frx.at[it, 1 - xi]
        if dx == 0:
            if z:
                return fye.at[yi], frye.at[it, 1 - yi]
            return yr.at[0, yi], fry.at[it, 1 - yi]
        return fd.at[z, xi, yi], frd.at[it, 1 - xi, 1 - yi, z]

    def copy_of(message, it, phase, d):
        src, dst = message(it, d)
        dx, dy, z = d
        return pltpu.make_async_remote_copy(
            src_ref=src,
            dst_ref=dst,
            send_sem=send_sem.at[phase, slot_of(dx, dy, z)],
            recv_sem=recv_sem.at[phase, slot_of(-dx, -dy, z)],
            device_id=target(dx, dy, z),
            device_id_type=MESH,
        )

    def grouped(dirs, act):
        for dx, dy in dict.fromkeys((d[0], d[1]) for d in dirs):

            def both(dx=dx, dy=dy):
                for d in dirs:
                    if (d[0], d[1]) == (dx, dy):
                        act(d)

            guarded(exists(dx, dy), both)

    def start(message, it, phase, dirs):
        grouped(dirs, lambda d: copy_of(message, it, phase, d).start())

    def wait_arrivals(message, it, phase, dirs):
        grouped(dirs, lambda d: copy_of(message, it, phase, (-d[0], -d[1], d[2])).wait_recv())

    def wait_sends(message, it, phase):
        grouped(DIRS, lambda d: copy_of(message, it, phase, d).wait_send())

    row8 = iota((8, 128), 0)
    lane8 = iota((8, 128), 1)

    my_edge = jnp.where(gz == 0, 127, 0)
    other_edge = 127 - my_edge
    my_edge_index = jnp.full((8, 128), my_edge, I32)
    other_edge_index = jnp.full((8, 128), other_edge, I32)
    lane_index = [jnp.full((8, 128), c, I32) for c in range(3)]

    def edges(planes, index):
        packed = take(planes[0], index)
        for c in (1, 2):
            packed = jnp.where(lane8 == c, take(planes[c], index), packed)
        return packed

    def pack_far():
        for xi, x in ((0, 0), (1, 7)):
            uxe[xi] = edges([uc[c, x] for c in range(3)], my_edge_index)
            for yi in range(2):
                for c in range(3):
                    ud[xi, yi, c : c + 1, :] = uy[yi, c, x : x + 1, :]

    def pack_near():
        for yi in range(2):
            uye[yi] = edges([uy[yi, c] for c in range(3)], my_edge_index)

    fetches[0].wait()
    for c in range(3):
        for x in range(8):
            plane = uc[c, x]
            uy[0, c, x : x + 1, :] = plane[0:1]
            uy[1, c, x : x + 1, :] = plane[7:8]
    pack_far()
    pack_near()
    beside_x = (gx > 0).astype(I32) + (gx < nx - 1).astype(I32)
    beside_y = (gy > 0).astype(I32) + (gy < ny - 1).astype(I32)
    pl.semaphore_wait(barrier, 2 * (1 + beside_x) * (1 + beside_y) - 1)
    start(displacement_message, 0, 0, DIRS)

    for fetch in fetches[1:]:
        fetch.wait()
    lane_k = iota((8, 128), 1)
    for g in range(tiles // 8):
        base = jnp.zeros((8, 128), I32)
        for i in range(8):
            base = jnp.where(row8 == i, tb_ref[g * 8 + i], base)
        s = (base >> 4) & 1
        sz = base & 15
        par = sz & 1
        j = sz >> 1
        sx = base >> 5
        i_of = (16 - j - par) & 7
        turn = j + par + jnp.where(s == 0, -2, 2)
        place = s * 16 + par * 8 + i_of
        ohg[g * 8 : g * 8 + 8, :] = jnp.where(
            jnp.logical_and((lane_k >> 6) == sx, (lane_k & 31) == place), 1.0, 0.0
        )
        ohs[g * 8 : g * 8 + 8, :] = jnp.where(lane_k == sx * 32 + place, 1.0, 0.0)
        q0 = codes[0, g * 8 : g * 8 + 8, :]
        q1 = codes[1, g * 8 : g * 8 + 8, :]
        q2 = codes[2, g * 8 : g * 8 + 8, :]
        q3 = codes[3, g * 8 : g * 8 + 8, :]

        def unit(q):
            sign = 1 - 2 * (q & 1)
            axis = q >> 1
            return [jnp.where(axis == k, sign, 0) for k in range(3)]

        e1, e2 = unit(q1), unit(q3)
        off = [((q2 * 57) >> 9) - 1, 0, 0]
        third = (q2 * 43) >> 7
        off[1] = third - 3 * (off[0] + 1) - 1
        off[2] = q2 - 3 * third - 1
        first = [(q0 >> 5) + 2, ((q0 >> 3) & 3) + 2, (q0 & 7) + 2]
        nodes = [first, [first[k] + e1[k] for k in range(3)], [first[k] + off[k] for k in range(3)]]
        nodes.append([nodes[2][k] + e2[k] for k in range(3)])
        for n in range(4):
            x, y, z = nodes[n]
            kidx[n, g * 8 : g * 8 + 8, :] = x
            lidx[n, g * 8 : g * 8 + 8, :] = ((y + turn) & 7) * 16 + z
        for k in range(3):
            a, b = e1[k].astype(F32), e2[k].astype(F32)
            geo[k, g * 8 : g * 8 + 8, :] = a
            geo[3 + k, g * 8 : g * 8 + 8, :] = b
            geo[6 + k, g * 8 : g * 8 + 8, :] = off[k].astype(F32) + 0.5 * b - 0.5 * a
    for c in range(3):
        frozen[c] = jnp.zeros((tiles, 128), F32)
    zero_plane = jnp.zeros((64, 384), BF16)
    win[0] = zero_plane
    win[11] = zero_plane

    row128 = iota((128, 128), 0)

    def make_onehot(t, carry):
        for n in range(2):
            first = lidx[2 * n, pl.ds(t, 1), :]
            second = lidx[2 * n + 1, pl.ds(t, 1), :]
            sign = 1.0 if n else -1.0
            flat = jnp.where(jnp.logical_or(row128 == first, row128 == second), sign, 0.0).astype(BF16)
            onehot[t, n * 128 : (n + 1) * 128, :] = jnp.transpose(flat)
        return carry

    lax.fori_loop(0, tiles, make_onehot, 0, unroll=4)
    pick = ohg[...].astype(BF16)
    spread_t = jnp.transpose(ohs[...])[0:64, 0:tiles].astype(BF16)
    spread = jnp.concatenate([spread_t, spread_t], axis=1)

    group_bits = [((lane8 >> 4) & bit) != 0 for bit in (1, 2, 4)]
    unroll = [(lane8 + 16 * row8 + 2 + 8 * p) & 127 for p in (0, 1)]
    edge_row = {0: row8 == 7, 1: row8 == 0}
    edge_lane = {0: lane8 == 127, 1: lane8 == 0}
    z_ok = {0: gz == 1, 1: gz == 0}
    my_edge_lane = lane8 == other_edge
    at_edge = lane8 == my_edge

    count = 2 * nx * ny
    me = (gx * ny + gy) * 2 + gz

    xs = [lax.rem(gx + a, nx) for a in range(nx)]
    ys = [lax.rem(gy + b, ny) for b in range(ny)]

    def ring(o, n):
        return min(o, n - o)

    offsets = [(a, b, c) for a in range(nx) for b in range(ny) for c in range(2) if (a, b, c) != (0, 0, 0)]
    offsets.sort(
        key=lambda o: -(ring(o[0] // 4, nx // 4) + ring(o[0] % 4, 4) + ring(o[1], ny))
    )

    def send_squares():
        for a, b, c in offsets:
            pltpu.make_async_remote_copy(
                src_ref=total_row,
                dst_ref=table.at[me],
                send_sem=total_send,
                recv_sem=total_recv,
                device_id=(xs[a], ys[b], 1 - gz if c else gz),
                device_id_type=MESH,
            ).start()

    def hail(semaphore, width):
        for dx in (-width, width):
            cond = gx + dx >= 0 if dx < 0 else gx + dx < nx

            def signal(dx=dx):
                pl.semaphore_signal(
                    semaphore, inc=1, device_id=(gx + dx, gy, gz), device_id_type=MESH
                )

            pl.when(cond)(signal)

    def hear(semaphore, width):
        pl.semaphore_wait(semaphore, (gx >= width).astype(I32) + (gx + width < nx).astype(I32))

    def iteration(it, carry):
        wait_arrivals(displacement_message, it, 2 * it, NEAR)

        beyond_rows = [
            [take(valid(y_ok[dy], rxye[it, lo_hi(dy)]), lane_index[c]) for c in range(3)] for dy in (-1, 1)
        ]
        def make_windows(x):
            for c in range(3):
                if 1 <= x <= 8:
                    own, other = uc[c, x - 1], rxz[it, c, x - 1]
                    rows = [
                        [
                            valid(y_ok[dy], rxy[it, lo_hi(dy), c, x - 1 : x, :]),
                            beyond_rows[lo_hi(dy)][c][x - 1 : x],
                        ]
                        for dy in (-1, 1)
                    ]
                else:
                    dx, xi = (-1, 0) if x == 0 else (1, 1)
                    own = valid(x_ok[dx], rxx[it, xi, c])
                    other = take(valid(x_ok[dx], rxxe[it, xi]), lane_index[c])
                    rows = [
                        [
                            valid(exists(dx, dy), rxd[it, xi, lo_hi(dy), z, c : c + 1, :])
                            for z in (0, 1)
                        ]
                        for dy in (-1, 1)
                    ]
                for s in range(2):
                    near = jnp.where(edge_row[s], rows[s][0], own)
                    far = jnp.where(edge_row[s], rows[s][1], other)
                    pair = []
                    for p in range(2):
                        source = jnp.where(edge_lane[p], jnp.where(z_ok[p], far, 0.0), near)
                        v = pltpu.roll(source, 2 + 8 * p, axis=1, stride=16, stride_axis=0)
                        for bit, mask in zip((1, 2, 4), group_bits):
                            v = jnp.where(mask, pltpu.roll(v, 8 - bit, axis=0), v)
                        pair.append(v)
                    both = jnp.concatenate(pair, axis=0)
                    hi, lo = split(both)
                    win[x + 1, s * 16 : s * 16 + 16, c * 128 : (c + 1) * 128] = hi.astype(BF16)
                    win[x + 1, 32 + s * 16 : 48 + s * 16, c * 128 : (c + 1) * 128] = lo.astype(BF16)

        def hand_out(k):
            both = jnp.concatenate([win[k], win[k + 4]], axis=0)
            gat[k] = jnp.dot(pick, both, preferred_element_type=F32)

        def look_up(n, at, planes, found):
            ks = kidx[n, at, :]
            ls = lidx[n, at, :]
            for k in planes:
                for c in range(3):
                    value = take(gat[k, at, c * 128 : (c + 1) * 128], ls)
                    found[c] = value if found[c] is None else jnp.where(ks == k, value, found[c])
            return found

        for x in range(1, 9):
            make_windows(x)
        for k in (0, 2, 3, 4, 5, 7):
            hand_out(k)
        for g in range(tiles // 8):
            at = pl.ds(g * 8, 8)
            for n in range(4):
                planes = (0, 2, 3, 4, 5, 7) if n == 3 else (2, 3, 4, 5)
                found = look_up(n, at, planes, [None] * 3)
                for c in range(3):
                    early[3 * n + c, at, :] = found[c]

        @pl.when(it > 0)
        def _():
            wait_sends(force_message, it - 1, 2 * it - 1)

        wait_arrivals(displacement_message, it, 2 * it, FAR)
        for x in (0, 9):
            make_windows(x)
        for k in (1, 6):
            hand_out(k)

        @pl.when(it == 2)
        def _():
            hear(hail_four, 4)
            hail(hail_eight, 8)

        live_below = jnp.where(it == 0, 2, 1)

        def pair_forces(g):
            at = pl.ds(pl.multiple_of(g * 8, 8), 8)
            points = []
            for n in range(4):
                found = [early[3 * n + c, at, :] for c in range(3)]
                if n > 0:
                    found = look_up(n, at, (1, 6), found)
                points.append(found)
            one = [points[1][c] - points[0][c] + geo[c, at, :] for c in range(3)]
            two = [points[3][c] - points[2][c] + geo[3 + c, at, :] for c in range(3)]
            apart = [
                0.5 * (points[2][c] + points[3][c]) - 0.5 * (points[0][c] + points[1][c])
                + geo[6 + c, at, :]
                for c in range(3)
            ]
            square = apart[0] * apart[0] + apart[1] * apart[1] + apart[2] * apart[2] + 0.5
            dots = one[0] * two[0] + one[1] * two[1] + one[2] * two[2]
            coupling = 0.5 * dots / (square * jnp.sqrt(square))
            fresh = groups[at, :] < live_below
            values = []
            for c in range(3):
                force = jnp.where(fresh, coupling * apart[c], frozen[c, at, :])
                frozen[c, at, :] = force
                values.extend(split(0.5 * force))
            return tuple(values)

        def spread_forces(g, values):
            for i in range(8):
                t = g * 8 + i
                columns = []
                for n in range(2):
                    mask = jnp.logical_or(
                        row8 == kidx[2 * n, pl.ds(t, 1), :], row8 == kidx[2 * n + 1, pl.ds(t, 1), :]
                    )
                    columns.append(
                        jnp.concatenate(
                            [jnp.where(mask, v[i : i + 1], 0.0) for v in values], axis=0
                        ).astype(BF16)
                    )
                lhs = jnp.concatenate(columns, axis=1)
                got = jnp.dot(lhs, onehot[t], preferred_element_type=F32)
                for c in range(3):
                    outs[c, pl.ds(pl.multiple_of(t * 8, 8), 8), :] = (
                        got[16 * c : 16 * c + 8] + got[16 * c + 8 : 16 * c + 16]
                    )

        def group(g, values):
            later = pair_forces(g)
            spread_forces(g - 1, values)
            return later

        values = lax.fori_loop(1, tiles // 8, group, pair_forces(0), unroll=7)
        spread_forces(tiles // 8 - 1, values)

        def collect(k):
            columns = []
            for c in range(3):
                hi, lo = split(outs[c, pl.ds(k, tiles, stride=8), :])
                columns.append(jnp.concatenate([hi, lo], axis=0).astype(BF16))
            acc[k] = jnp.dot(spread, jnp.concatenate(columns, axis=1), preferred_element_type=F32)

        def fold(x):
            for c in range(3):
                cut = slice(c * 128, (c + 1) * 128)
                parts = []
                for s in range(2):
                    line, beyond = None, None
                    for p in range(2):
                        at = s * 16 + p * 8
                        v = None
                        if x + 1 <= 7:
                            v = acc[x + 1, at : at + 8, cut]
                        if x + 1 >= 4:
                            w = acc[x - 3, 32 + at : 40 + at, cut]
                            v = w if v is None else v + w
                        for bit, mask in zip((1, 2, 4), group_bits):
                            v = jnp.where(mask, pltpu.roll(v, bit, axis=0), v)
                        v = take(v, unroll[p])
                        inside = jnp.where(edge_lane[p], 0.0, v)
                        outside = jnp.where(z_ok[p], v, 0.0)
                        line = inside if line is None else line + inside
                        beyond = outside if beyond is None else beyond + outside
                    parts.append((line, jnp.where(my_edge_lane, beyond, 0.0)))
                for z in range(2):
                    (pz if z else pb)[c, x] = jnp.where(edge_row[0], 0.0, parts[0][z]) + jnp.where(
                        edge_row[1], 0.0, parts[1][z]
                    )
                    ends = (parts[0][z][7:8], parts[1][z][0:1])
                    for yi in range(2):
                        if 1 <= x <= 8:
                            yr[z, yi, c, x - 1 : x, :] = ends[yi]
                        else:
                            fd[z, 0 if x == 0 else 1, yi, c : c + 1, :] = ends[yi]

        for k in (1, 6):
            collect(k)
        for x in (0, 9):
            fold(x)
        for i in range(2):
            fxe[i] = edges([pz[c, 9 * i] for c in range(3)], other_edge_index)
        start(force_message, it, 2 * it + 1, FAR)
        for k in (0, 2, 3, 4, 5, 7):
            collect(k)
        for x in range(1, 9):
            fold(x)
        for i in range(2):
            fye[i] = edges([yr[1, i, c] for c in range(3)], other_edge_index)
        start(force_message, it, 2 * it + 1, NEAR)
        wait_sends(displacement_message, it, 2 * it)
        wait_arrivals(force_message, it, 2 * it + 1, NEAR)

        lines = []
        for dy in (-1, 1):
            yi = lo_hi(dy)
            lines.append(
                [
                    valid(
                        y_ok[dy],
                        fry[it, yi, c] + jnp.where(at_edge, take(frye[it, yi], lane_index[c]), 0.0),
                    )
                    for c in range(3)
                ]
            )
        def residual_of(x, squares):
            for c in range(3):
                total = pb[c, x + 1] + frz[it, c, x]
                for dx, xe in ((-1, 0), (1, 7)):
                    if x == xe:
                        xi = lo_hi(dx)
                        total = total + valid(
                            x_ok[dx],
                            frx[it, xi, c] + jnp.where(at_edge, take(frxe[it, xi], lane_index[c]), 0.0),
                        )
                for dy in (-1, 1):
                    yi = lo_hi(dy)
                    line = lines[yi][c][x : x + 1]
                    for dx, xe in ((-1, 0), (1, 7)):
                        if x == xe:
                            xi = lo_hi(dx)
                            line = line + valid(
                                exists(dx, dy),
                                frd[it, xi, yi, 0, c : c + 1, :] + frd[it, xi, yi, 1, c : c + 1, :],
                            )
                    total = total + jnp.where(row8 == (0 if dy < 0 else 7), line, 0.0)
                r = uc[c, x] - uold[c, x] - 0.5 * total
                squares = squares + r * r
                residuals[c, x] = r
            return squares

        def update(x):
            residual = [residuals[c, x] for c in range(3)]
            for a in range(3):
                fix = jac[a, 0, x] * residual[0] + jac[a, 1, x] * residual[1] + jac[a, 2, x] * residual[2]
                new = uc[a, x] - fix
                uc[a, x] = new
                uy[0, a, x : x + 1, :] = new[0:1]
                uy[1, a, x : x + 1, :] = new[7:8]

        squares = jnp.zeros((8, 128), F32)
        for x in range(1, 7):
            squares = residual_of(x, squares)
        for x in range(1, 7):
            update(x)
        wait_arrivals(force_message, it, 2 * it + 1, FAR)

        @pl.when(it == 1)
        def _():
            hail(hail_four, 4)

        @pl.when(it == 2)
        def _():
            hear(hail_eight, 8)

        for x in (0, 7):
            squares = residual_of(x, squares)
        sq[pl.ds(it, 1), :] = jnp.sum(squares, axis=0, keepdims=True)

        @pl.when(it == ITERS - 1)
        def _():
            sums = jnp.sum(sq[...], axis=1, keepdims=True)
            row = jnp.sum(jnp.where(row8 == lane8, sums, 0.0), axis=0, keepdims=True)
            total_row[...] = row
            table[me] = row
            send_squares()

        for x in (0, 7):
            update(x)
        @pl.when(it < ITERS - 1)
        def _():
            pack_far()
            start(displacement_message, it + 1, 2 * it + 2, FAR)
            pack_near()
            start(displacement_message, it + 1, 2 * it + 2, NEAR)

        return carry

    sq[...] = jnp.zeros((8, 128), F32)
    lax.fori_loop(0, ITERS, iteration, 0)
    store_result = pltpu.make_async_copy(uc, uout, in_sem.at[0])
    store_result.start()
    wait_sends(force_message, ITERS - 1, 2 * ITERS - 1)
    others = table.at[0 : count - 1]
    pltpu.make_async_copy(others, others, total_recv).wait()
    pltpu.make_async_copy(others, others, total_send).wait()
    total = jnp.sum(table[...], axis=0)
    norms = jnp.sqrt(total / cells)
    for k in range(ITERS):
        nout[k] = jnp.sum(norms[:, k : k + 1])
    store_result.wait()


def solution(mesh):
    nx, ny = mesh.shape["gx"], mesh.shape["gy"]

    def step(u_old, u_trial, jacobian_inverse, tile_base, pair_codes, pair_groups):
        tiles = tile_base.shape[0]
        cells = float(3 * 8 * 8 * 128 * nx * ny * mesh.shape["gz"])
        smem = pl.BlockSpec(memory_space=pltpu.SMEM)
        v = pltpu.VMEM
        return pl.pallas_call(
            functools.partial(kernel, nx, ny, cells),
            out_shape=(
                jax.ShapeDtypeStruct(u_old.shape, F32),
                jax.ShapeDtypeStruct((ITERS,), F32),
            ),
            in_specs=[pl.BlockSpec(memory_space=pltpu.HBM)] * 6,
            out_specs=(pl.BlockSpec(memory_space=pl.ANY), smem),
            scratch_shapes=[
                pltpu.SMEM(tile_base.shape, I32),
                v(u_old.shape, F32),
                v(jacobian_inverse.shape, F32),
                v(pair_codes.shape, I32),
                v(pair_groups.shape, I32),
                v(u_old.shape, F32),
                v((3, 8, 8, 128), F32),
                v((2, 3, 8, 128), F32),
                v((2, 8, 128), F32),
                v((2, 8, 128), F32),
                v((2, 2, 8, 128), F32),
                v((ITERS, 3, 8, 8, 128), F32),
                v((ITERS, 2, 3, 8, 128), F32),
                v((ITERS, 2, 3, 8, 128), F32),
                v((ITERS, 2, 8, 128), F32),
                v((ITERS, 2, 8, 128), F32),
                v((ITERS, 2, 2, 2, 8, 128), F32),
                v((3, 10, 8, 128), F32),
                v((3, 10, 8, 128), F32),
                v((2, 2, 3, 8, 128), F32),
                v((2, 8, 128), F32),
                v((2, 8, 128), F32),
                v((2, 2, 2, 8, 128), F32),
                v((ITERS, 3, 8, 8, 128), F32),
                v((ITERS, 2, 3, 8, 128), F32),
                v((ITERS, 2, 3, 8, 128), F32),
                v((ITERS, 2, 8, 128), F32),
                v((ITERS, 2, 8, 128), F32),
                v((ITERS, 2, 2, 2, 8, 128), F32),
                v((12, 64, 384), BF16),
                v((8, tiles, 384), F32),
                v((12, tiles, 128), F32),
                v((4, tiles, 128), I32),
                v((4, tiles, 128), I32),
                v((9, tiles, 128), F32),
                v((3, tiles, 128), F32),
                v((tiles, 256, 128), BF16),
                v((tiles, 128), F32),
                v((tiles, 128), F32),
                v((3, tiles * 8, 128), F32),
                v((8, 64, 384), F32),
                v((8, 128), F32),
                v((1, 128), F32),
                v((2 * nx * ny, 1, 128), F32),
                pltpu.SemaphoreType.REGULAR,
                pltpu.SemaphoreType.REGULAR,
                pltpu.SemaphoreType.DMA((6,)),
                pltpu.SemaphoreType.DMA((2 * ITERS, 18)),
                pltpu.SemaphoreType.DMA((2 * ITERS, 18)),
                pltpu.SemaphoreType.DMA,
                pltpu.SemaphoreType.DMA,
            ],
            compiler_params=pltpu.CompilerParams(
                collective_id=0, has_side_effects=True, vmem_limit_bytes=24 * 2**20
            ),
            name="relax",
        )(
            *(
                pltpu.with_memory_space_constraint(a, pltpu.HBM)
                for a in (tile_base, u_old, u_trial, jacobian_inverse, pair_codes, pair_groups)
            )
        )

    everywhere = ("gx", "gy", "gz")
    return jax.shard_map(
        step,
        mesh=mesh,
        in_specs=(
            P(None, "gx", "gy", "gz"),
            P(None, "gx", "gy", "gz"),
            P(None, None, "gx", "gy", "gz"),
            P(everywhere),
            P(None, everywhere, None),
            P(everywhere, None),
        ),
        out_specs=(P(None, "gx", "gy", "gz"), P()),
        check_vma=False,
    )
```

```python
import functools

import jax
import jax.numpy as jnp
from jax import lax
from jax.experimental import pallas as pl
from jax.experimental.pallas import tpu as pltpu
from jax.sharding import PartitionSpec as P

ITERS = 3
MESH = pl.DeviceIdType.MESH
F32 = jnp.float32
BF16 = jnp.bfloat16
I32 = jnp.int32

DIRS = sorted(
    [
        (dx, dy, z)
        for dx in (-1, 0, 1)
        for dy in (-1, 0, 1)
        for z in (0, 1)
        if (dx, dy, z) != (0, 0, 0)
    ],
    key=lambda d: (-2 * abs(d[0]) - abs(d[1]), d),
)


FAR = [d for d in DIRS if d[0] != 0]
NEAR = [d for d in DIRS if d[0] == 0]
PACKED_FAR = [d for d in FAR if d[1] == 0 and d[2] == 1]
PACKED_NEAR = [d for d in NEAR if d[1] != 0 and d[2] == 1]
PLAIN_FAR = [d for d in FAR if d not in PACKED_FAR]
PLAIN_NEAR = [d for d in NEAR if d not in PACKED_NEAR]


def slot_of(dx, dy, z):
    return ((dx + 1) * 3 + dy + 1) * 2 + z


def iota(shape, dim):
    return lax.broadcasted_iota(I32, shape, dim)


def take(x, idx):
    return jnp.take_along_axis(x, idx, axis=1, mode="promise_in_bounds")


def split(x):
    hi = x.astype(BF16).astype(F32)
    return hi, x - hi


def finish(cells, u, total, uout, nout, sem):
    store = pltpu.make_async_copy(u, uout, sem)
    store.start()
    norms = jnp.sqrt(total[...] / cells)
    for k in range(ITERS):
        nout[k] = jnp.sum(norms[:, k : k + 1])
    store.wait()


def kernel(
    nx, ny,
    tb_in, uold_in, utrial_in, jac_in, codes_in, groups_in,
    uout, nout,
    tb_ref, uold, jac, codes, groups, residuals,
    uc, uy, uxe, uye, ud, rxz, rxx, rxy, rxxe, rxye, rxd,
    pb, pz, yr, fxe, fye, fd, frz, frx, fry, frxe, frye, frd,
    win, gat, early, kidx, lidx, geo, frozen, onehot, ohg, ohs, outs, acc,
    sq, total_row, table,
    hail_four, hail_eight, in_sem, send_sem, recv_sem, total_send, total_recv,
):
    gx, gy, gz = lax.axis_index("gx"), lax.axis_index("gy"), lax.axis_index("gz")
    tiles = groups.shape[0]
    x_ok = {-1: gx > 0, 0: None, 1: gx < nx - 1}
    y_ok = {-1: gy > 0, 0: None, 1: gy < ny - 1}

    def exists(dx, dy):
        if dx == 0 and dy == 0:
            return None
        if dx == 0:
            return y_ok[dy]
        if dy == 0:
            return x_ok[dx]
        return jnp.logical_and(x_ok[dx], y_ok[dy])

    def guarded(cond, fn):
        if cond is None:
            fn()
        else:
            pl.when(cond)(fn)

    def valid(cond, value):
        return value if cond is None else jnp.where(cond, value, 0.0)

    def target(dx, dy, z):
        return (gx + dx, gy + dy, gz if z == 0 else 1 - gz)

    barrier = pltpu.get_barrier_semaphore()

    def greet(device):
        pl.semaphore_signal(barrier, inc=1, device_id=device, device_id_type=MESH)

    for d in DIRS:
        guarded(exists(d[0], d[1]), functools.partial(greet, target(*d)))

    fetches = [
        pltpu.make_async_copy(src, dst, in_sem.at[k])
        for k, (src, dst) in enumerate(
            [
                (utrial_in, uc),
                (tb_in, tb_ref),
                (codes_in, codes),
                (groups_in, groups),
                (uold_in, uold),
                (jac_in, jac),
            ]
        )
    ]
    for fetch in fetches:
        fetch.start()

    def lo_hi(d):
        return 1 if d > 0 else 0

    def displacement_message(it, d):
        dx, dy, z = d
        xi, yi = lo_hi(dx), lo_hi(dy)
        if dx == 0 and dy == 0:
            return uc, rxz.at[it]
        if dy == 0:
            if z:
                return uxe.at[xi], rxxe.at[it, 1 - xi]
            return uc.at[:, 7 * xi], rxx.at[it, 1 - xi]
        if dx == 0:
            if z:
                return uye.at[yi], rxye.at[it, 1 - yi]
            return uy.at[yi], rxy.at[it, 1 - yi]
        return ud.at[xi, yi], rxd.at[it, 1 - xi, 1 - yi, z]

    def force_message(it, d):
        dx, dy, z = d
        xi, yi = lo_hi(dx), lo_hi(dy)
        if dx == 0 and dy == 0:
            return pz.at[:, 1:9], frz.at[it]
        if dy == 0:
            if z:
                return fxe.at[xi], frxe.at[it, 1 - xi]
            return pb.at[:, 9 * xi], frx.at[it, 1 - xi]
        if dx == 0:
            if z:
                return fye.at[yi], frye.at[it, 1 - yi]
            return yr.at[0, yi], fry.at[it, 1 - yi]
        return fd.at[z, xi, yi], frd.at[it, 1 - xi, 1 - yi, z]

    def copy_of(message, it, phase, d):
        src, dst = message(it, d)
        dx, dy, z = d
        return pltpu.make_async_remote_copy(
            src_ref=src,
            dst_ref=dst,
            send_sem=send_sem.at[phase, slot_of(dx, dy, z)],
            recv_sem=recv_sem.at[phase, slot_of(-dx, -dy, z)],
            device_id=target(dx, dy, z),
            device_id_type=MESH,
        )

    def grouped(dirs, act):
        for dx, dy in dict.fromkeys((d[0], d[1]) for d in dirs):

            def both(dx=dx, dy=dy):
                for d in dirs:
                    if (d[0], d[1]) == (dx, dy):
                        act(d)

            guarded(exists(dx, dy), both)

    def start(message, it, phase, dirs):
        grouped(dirs, lambda d: copy_of(message, it, phase, d).start())

    def wait_arrivals(message, it, phase, dirs):
        grouped(dirs, lambda d: copy_of(message, it, phase, (-d[0], -d[1], d[2])).wait_recv())

    def wait_sends(message, it, phase):
        grouped(DIRS, lambda d: copy_of(message, it, phase, d).wait_send())

    row8 = iota((8, 128), 0)
    lane8 = iota((8, 128), 1)

    my_edge = jnp.where(gz == 0, 127, 0)
    other_edge = 127 - my_edge
    my_edge_index = jnp.full((8, 128), my_edge, I32)
    other_edge_index = jnp.full((8, 128), other_edge, I32)
    column_lane = [row8 + 8 * c for c in range(3)]

    def edges(planes, index):
        packed = jnp.zeros((8, 128), F32)
        for c in range(3):
            packed = jnp.where(lane8 == column_lane[c], take(planes[c], index), packed)
        return jnp.sum(packed, axis=0, keepdims=True)

    def column(row, c):
        return take(jnp.broadcast_to(row, (8, 128)), column_lane[c])

    def corner_rows():
        for xi, x in ((0, 0), (1, 7)):
            for yi in range(2):
                for c in range(3):
                    ud[xi, yi, c] = uy[yi, c, x : x + 1, :]

    def send_displacements(it, phase):
        start(displacement_message, it, phase, PLAIN_FAR)
        start(displacement_message, it, phase, PLAIN_NEAR)
        for i in range(2):
            uxe[i] = edges([uc[c, 7 * i] for c in range(3)], my_edge_index)
            uye[i] = edges([uy[i, c] for c in range(3)], my_edge_index)
        start(displacement_message, it, phase, PACKED_FAR)
        start(displacement_message, it, phase, PACKED_NEAR)

    fetches[0].wait()
    for c in range(3):
        for x in range(8):
            plane = uc[c, x]
            uy[0, c, x : x + 1, :] = plane[0:1]
            uy[1, c, x : x + 1, :] = plane[7:8]
    corner_rows()
    beside_x = (gx > 0).astype(I32) + (gx < nx - 1).astype(I32)
    beside_y = (gy > 0).astype(I32) + (gy < ny - 1).astype(I32)
    pl.semaphore_wait(barrier, 2 * (1 + beside_x) * (1 + beside_y) - 1)
    send_displacements(0, 0)

    for fetch in fetches[1:]:
        fetch.wait()
    lane_k = iota((8, 128), 1)
    for g in range(tiles // 8):
        base = jnp.zeros((8, 128), I32)
        for i in range(8):
            base = jnp.where(row8 == i, tb_ref[g * 8 + i], base)
        s = (base >> 4) & 1
        sz = base & 15
        par = sz & 1
        j = sz >> 1
        sx = base >> 5
        i_of = (16 - j - par) & 7
        turn = j + par + jnp.where(s == 0, -2, 2)
        place = s * 16 + par * 8 + i_of
        ohg[g * 8 : g * 8 + 8, :] = jnp.where(
            jnp.logical_and((lane_k >> 6) == sx, (lane_k & 31) == place), 1.0, 0.0
        )
        ohs[g * 8 : g * 8 + 8, :] = jnp.where(lane_k == sx * 32 + place, 1.0, 0.0)
        q0 = codes[0, g * 8 : g * 8 + 8, :]
        q1 = codes[1, g * 8 : g * 8 + 8, :]
        q2 = codes[2, g * 8 : g * 8 + 8, :]
        q3 = codes[3, g * 8 : g * 8 + 8, :]

        def unit(q):
            sign = 1 - 2 * (q & 1)
            axis = q >> 1
            return [jnp.where(axis == k, sign, 0) for k in range(3)]

        e1, e2 = unit(q1), unit(q3)
        off = [((q2 * 57) >> 9) - 1, 0, 0]
        third = (q2 * 43) >> 7
        off[1] = third - 3 * (off[0] + 1) - 1
        off[2] = q2 - 3 * third - 1
        first = [(q0 >> 5) + 2, ((q0 >> 3) & 3) + 2, (q0 & 7) + 2]
        nodes = [first, [first[k] + e1[k] for k in range(3)], [first[k] + off[k] for k in range(3)]]
        nodes.append([nodes[2][k] + e2[k] for k in range(3)])
        for n in range(4):
            x, y, z = nodes[n]
            kidx[n, g * 8 : g * 8 + 8, :] = x
            lidx[n, g * 8 : g * 8 + 8, :] = ((y + turn) & 7) * 16 + z
        for k in range(3):
            a, b = e1[k].astype(F32), e2[k].astype(F32)
            geo[k, g * 8 : g * 8 + 8, :] = a
            geo[3 + k, g * 8 : g * 8 + 8, :] = b
            geo[6 + k, g * 8 : g * 8 + 8, :] = off[k].astype(F32) + 0.5 * b - 0.5 * a
    for c in range(3):
        frozen[c] = jnp.zeros((tiles, 128), F32)
    zero_plane = jnp.zeros((64, 384), BF16)
    win[0] = zero_plane
    win[11] = zero_plane

    row128 = iota((128, 128), 0)

    def make_onehot(t, carry):
        for n in range(2):
            first = lidx[2 * n, pl.ds(t, 1), :]
            second = lidx[2 * n + 1, pl.ds(t, 1), :]
            sign = 1.0 if n else -1.0
            flat = jnp.where(jnp.logical_or(row128 == first, row128 == second), sign, 0.0).astype(BF16)
            onehot[t, n * 128 : (n + 1) * 128, :] = jnp.transpose(flat)
        return carry

    lax.fori_loop(0, tiles, make_onehot, 0, unroll=4)
    pick = ohg[...].astype(BF16)
    spread_t = jnp.transpose(ohs[...])[0:64, 0:tiles].astype(BF16)
    spread = jnp.concatenate([spread_t, spread_t], axis=1)

    group_bits = [((lane8 >> 4) & bit) != 0 for bit in (1, 2, 4)]
    unroll = [(lane8 + 16 * row8 + 2 + 8 * p) & 127 for p in (0, 1)]
    edge_row = {0: row8 == 7, 1: row8 == 0}
    edge_lane = {0: lane8 == 127, 1: lane8 == 0}
    z_ok = {0: gz == 1, 1: gz == 0}
    my_edge_lane = lane8 == other_edge
    at_edge = lane8 == my_edge

    count = 2 * nx * ny
    me = (gx * ny + gy) * 2 + gz

    xs = [lax.rem(gx + a, nx) for a in range(nx)]
    ys = [lax.rem(gy + b, ny) for b in range(ny)]

    def ring(o, n):
        return min(o, n - o)

    offsets = [(a, b, c) for a in range(nx) for b in range(ny) for c in range(2) if (a, b, c) != (0, 0, 0)]
    offsets.sort(
        key=lambda o: -(ring(o[0] // 4, nx // 4) + ring(o[0] % 4, 4) + ring(o[1], ny))
    )

    def send_squares():
        for a, b, c in offsets:
            pltpu.make_async_remote_copy(
                src_ref=total_row,
                dst_ref=table.at[me],
                send_sem=total_send,
                recv_sem=total_recv,
                device_id=(xs[a], ys[b], 1 - gz if c else gz),
                device_id_type=MESH,
            ).start()

    def hail(semaphore, width):
        for dx in (-width, width):
            cond = gx + dx >= 0 if dx < 0 else gx + dx < nx

            def signal(dx=dx):
                pl.semaphore_signal(
                    semaphore, inc=1, device_id=(gx + dx, gy, gz), device_id_type=MESH
                )

            pl.when(cond)(signal)

    def hear(semaphore, width):
        pl.semaphore_wait(semaphore, (gx >= width).astype(I32) + (gx + width < nx).astype(I32))

    def iteration(it, carry):
        wait_arrivals(displacement_message, it, 2 * it, NEAR)

        beyond_rows = [
            [column(valid(y_ok[dy], rxye[it, lo_hi(dy)]), c) for c in range(3)] for dy in (-1, 1)
        ]
        def make_windows(x):
            for c in range(3):
                if 1 <= x <= 8:
                    own, other = uc[c, x - 1], rxz[it, c, x - 1]
                    rows = [
                        [
                            valid(y_ok[dy], rxy[it, lo_hi(dy), c, x - 1 : x, :]),
                            beyond_rows[lo_hi(dy)][c][x - 1 : x],
                        ]
                        for dy in (-1, 1)
                    ]
                else:
                    dx, xi = (-1, 0) if x == 0 else (1, 1)
                    own = valid(x_ok[dx], rxx[it, xi, c])
                    other = column(valid(x_ok[dx], rxxe[it, xi]), c)
                    rows = [
                        [
                            valid(exists(dx, dy), rxd[it, xi, lo_hi(dy), z, c])
                            for z in (0, 1)
                        ]
                        for dy in (-1, 1)
                    ]
                for s in range(2):
                    near = jnp.where(edge_row[s], rows[s][0], own)
                    far = jnp.where(edge_row[s], rows[s][1], other)
                    pair = []
                    for p in range(2):
                        source = jnp.where(edge_lane[p], jnp.where(z_ok[p], far, 0.0), near)
                        v = pltpu.roll(source, 2 + 8 * p, axis=1, stride=16, stride_axis=0)
                        for bit, mask in zip((1, 2, 4), group_bits):
                            v = jnp.where(mask, pltpu.roll(v, 8 - bit, axis=0), v)
                        pair.append(v)
                    both = jnp.concatenate(pair, axis=0)
                    hi, lo = split(both)
                    win[x + 1, s * 16 : s * 16 + 16, c * 128 : (c + 1) * 128] = hi.astype(BF16)
                    win[x + 1, 32 + s * 16 : 48 + s * 16, c * 128 : (c + 1) * 128] = lo.astype(BF16)

        def hand_out(k):
            both = jnp.concatenate([win[k], win[k + 4]], axis=0)
            gat[k] = jnp.dot(pick, both, preferred_element_type=F32)

        def look_up(n, at, planes, found):
            ks = kidx[n, at, :]
            ls = lidx[n, at, :]
            for k in planes:
                for c in range(3):
                    value = take(gat[k, at, c * 128 : (c + 1) * 128], ls)
                    found[c] = value if found[c] is None else jnp.where(ks == k, value, found[c])
            return found

        for x in range(1, 9):
            make_windows(x)
        for k in (0, 2, 3, 4, 5, 7):
            hand_out(k)
        for g in range(tiles // 8):
            at = pl.ds(g * 8, 8)
            for n in range(4):
                planes = (0, 2, 3, 4, 5, 7) if n == 3 else (2, 3, 4, 5)
                found = look_up(n, at, planes, [None] * 3)
                for c in range(3):
                    early[3 * n + c, at, :] = found[c]

        @pl.when(it > 0)
        def _():
            wait_sends(force_message, it - 1, 2 * it - 1)

        wait_arrivals(displacement_message, it, 2 * it, FAR)
        for x in (0, 9):
            make_windows(x)
        for k in (1, 6):
            hand_out(k)

        @pl.when(it == 2)
        def _():
            hear(hail_four, 4)
            hail(hail_eight, 8)

        live_below = jnp.where(it == 0, 2, 1)

        def pair_forces(g):
            at = pl.ds(pl.multiple_of(g * 8, 8), 8)
            points = []
            for n in range(4):
                found = [early[3 * n + c, at, :] for c in range(3)]
                if n > 0:
                    found = look_up(n, at, (1, 6), found)
                points.append(found)
            one = [points[1][c] - points[0][c] + geo[c, at, :] for c in range(3)]
            two = [points[3][c] - points[2][c] + geo[3 + c, at, :] for c in range(3)]
            apart = [
                0.5 * (points[2][c] + points[3][c]) - 0.5 * (points[0][c] + points[1][c])
                + geo[6 + c, at, :]
                for c in range(3)
            ]
            square = apart[0] * apart[0] + apart[1] * apart[1] + apart[2] * apart[2] + 0.5
            dots = one[0] * two[0] + one[1] * two[1] + one[2] * two[2]
            coupling = 0.5 * dots / (square * jnp.sqrt(square))
            fresh = groups[at, :] < live_below
            values = []
            for c in range(3):
                force = jnp.where(fresh, coupling * apart[c], frozen[c, at, :])
                frozen[c, at, :] = force
                values.extend(split(0.5 * force))
            return tuple(values)

        def spread_forces(g, values):
            for i in range(8):
                t = g * 8 + i
                columns = []
                for n in range(2):
                    mask = jnp.logical_or(
                        row8 == kidx[2 * n, pl.ds(t, 1), :], row8 == kidx[2 * n + 1, pl.ds(t, 1), :]
                    )
                    columns.append(
                        jnp.concatenate(
                            [jnp.where(mask, v[i : i + 1], 0.0) for v in values], axis=0
                        ).astype(BF16)
                    )
                lhs = jnp.concatenate(columns, axis=1)
                got = jnp.dot(lhs, onehot[t], preferred_element_type=F32)
                for c in range(3):
                    outs[c, pl.ds(pl.multiple_of(t * 8, 8), 8), :] = (
                        got[16 * c : 16 * c + 8] + got[16 * c + 8 : 16 * c + 16]
                    )

        def group(g, values):
            later = pair_forces(g)
            spread_forces(g - 1, values)
            return later

        values = lax.fori_loop(1, tiles // 8, group, pair_forces(0), unroll=7)
        spread_forces(tiles // 8 - 1, values)

        def collect(k):
            columns = []
            for c in range(3):
                hi, lo = split(outs[c, pl.ds(k, tiles, stride=8), :])
                columns.append(jnp.concatenate([hi, lo], axis=0).astype(BF16))
            acc[k] = jnp.dot(spread, jnp.concatenate(columns, axis=1), preferred_element_type=F32)

        def fold(x):
            for c in range(3):
                cut = slice(c * 128, (c + 1) * 128)
                parts = []
                for s in range(2):
                    line, beyond = None, None
                    for p in range(2):
                        at = s * 16 + p * 8
                        v = None
                        if x + 1 <= 7:
                            v = acc[x + 1, at : at + 8, cut]
                        if x + 1 >= 4:
                            w = acc[x - 3, 32 + at : 40 + at, cut]
                            v = w if v is None else v + w
                        for bit, mask in zip((1, 2, 4), group_bits):
                            v = jnp.where(mask, pltpu.roll(v, bit, axis=0), v)
                        v = take(v, unroll[p])
                        inside = jnp.where(edge_lane[p], 0.0, v)
                        outside = jnp.where(z_ok[p], v, 0.0)
                        line = inside if line is None else line + inside
                        beyond = outside if beyond is None else beyond + outside
                    parts.append((line, jnp.where(my_edge_lane, beyond, 0.0)))
                for z in range(2):
                    (pz if z else pb)[c, x] = jnp.where(edge_row[0], 0.0, parts[0][z]) + jnp.where(
                        edge_row[1], 0.0, parts[1][z]
                    )
                    ends = (parts[0][z][7:8], parts[1][z][0:1])
                    for yi in range(2):
                        if 1 <= x <= 8:
                            yr[z, yi, c, x - 1 : x, :] = ends[yi]
                        else:
                            fd[z, 0 if x == 0 else 1, yi, c] = ends[yi]

        for k in (1, 6):
            collect(k)
        for x in (0, 9):
            fold(x)
        start(force_message, it, 2 * it + 1, PLAIN_FAR)
        for i in range(2):
            fxe[i] = edges([pz[c, 9 * i] for c in range(3)], other_edge_index)
        start(force_message, it, 2 * it + 1, PACKED_FAR)
        for k in (0, 2, 3, 4, 5, 7):
            collect(k)
        for x in range(1, 9):
            fold(x)
        start(force_message, it, 2 * it + 1, PLAIN_NEAR)
        for i in range(2):
            fye[i] = edges([yr[1, i, c] for c in range(3)], other_edge_index)
        start(force_message, it, 2 * it + 1, PACKED_NEAR)
        wait_sends(displacement_message, it, 2 * it)
        wait_arrivals(force_message, it, 2 * it + 1, NEAR)

        lines = []
        for dy in (-1, 1):
            yi = lo_hi(dy)
            lines.append(
                [
                    valid(
                        y_ok[dy],
                        fry[it, yi, c] + jnp.where(at_edge, column(frye[it, yi], c), 0.0),
                    )
                    for c in range(3)
                ]
            )
        def residual_of(x, squares):
            for c in range(3):
                total = pb[c, x + 1] + frz[it, c, x]
                for dx, xe in ((-1, 0), (1, 7)):
                    if x == xe:
                        xi = lo_hi(dx)
                        total = total + valid(
                            x_ok[dx],
                            frx[it, xi, c] + jnp.where(at_edge, column(frxe[it, xi], c), 0.0),
                        )
                for dy in (-1, 1):
                    yi = lo_hi(dy)
                    line = lines[yi][c][x : x + 1]
                    for dx, xe in ((-1, 0), (1, 7)):
                        if x == xe:
                            xi = lo_hi(dx)
                            line = line + valid(
                                exists(dx, dy),
                                frd[it, xi, yi, 0, c] + frd[it, xi, yi, 1, c],
                            )
                    total = total + jnp.where(row8 == (0 if dy < 0 else 7), line, 0.0)
                r = uc[c, x] - uold[c, x] - 0.5 * total
                squares = squares + r * r
                residuals[c, x] = r
            return squares

        def update(x):
            residual = [residuals[c, x] for c in range(3)]
            for a in range(3):
                fix = jac[a, 0, x] * residual[0] + jac[a, 1, x] * residual[1] + jac[a, 2, x] * residual[2]
                new = uc[a, x] - fix
                uc[a, x] = new
                uy[0, a, x : x + 1, :] = new[0:1]
                uy[1, a, x : x + 1, :] = new[7:8]

        squares = jnp.zeros((8, 128), F32)
        for x in range(1, 7):
            squares = residual_of(x, squares)
        for x in range(1, 7):
            update(x)
        wait_arrivals(force_message, it, 2 * it + 1, FAR)

        @pl.when(it == 1)
        def _():
            hail(hail_four, 4)

        @pl.when(it == 2)
        def _():
            hear(hail_eight, 8)

        for x in (0, 7):
            squares = residual_of(x, squares)
        sq[pl.ds(it, 1), :] = jnp.sum(squares, axis=0, keepdims=True)

        @pl.when(it == ITERS - 1)
        def _():
            sums = jnp.sum(sq[...], axis=1, keepdims=True)
            row = jnp.sum(jnp.where(row8 == lane8, sums, 0.0), axis=0, keepdims=True)
            total_row[...] = row
            table[me] = row
            send_squares()

        for x in (0, 7):
            update(x)
        @pl.when(it < ITERS - 1)
        def _():
            corner_rows()
            send_displacements(it + 1, 2 * it + 2)

        return carry

    sq[...] = jnp.zeros((8, 128), F32)
    lax.fori_loop(0, ITERS, iteration, 0)
    store_result = pltpu.make_async_copy(uc, uout, in_sem.at[0])
    store_result.start()
    wait_sends(force_message, ITERS - 1, 2 * ITERS - 1)
    others = table.at[0 : count - 1]
    pltpu.make_async_copy(others, others, total_recv).wait()
    pltpu.make_async_copy(others, others, total_send).wait()
    total_row[...] = jnp.sum(table[...], axis=0)
    store_total = pltpu.make_async_copy(total_row, nout, in_sem.at[1])
    store_total.start()
    store_total.wait()
    store_result.wait()


def solution(mesh):
    nx, ny = mesh.shape["gx"], mesh.shape["gy"]

    def step(u_old, u_trial, jacobian_inverse, tile_base, pair_codes, pair_groups):
        tiles = tile_base.shape[0]
        cells = float(3 * 8 * 8 * 128 * nx * ny * mesh.shape["gz"])
        smem = pl.BlockSpec(memory_space=pltpu.SMEM)
        v = pltpu.VMEM
        u_final, total = pl.pallas_call(
            functools.partial(kernel, nx, ny),
            out_shape=(
                jax.ShapeDtypeStruct(u_old.shape, F32),
                jax.ShapeDtypeStruct((1, 128), F32),
            ),
            in_specs=[pl.BlockSpec(memory_space=pltpu.HBM)] * 6,
            out_specs=[pl.BlockSpec(memory_space=pl.ANY)] * 2,
            scratch_shapes=[
                pltpu.SMEM(tile_base.shape, I32),
                v(u_old.shape, F32),
                v(jacobian_inverse.shape, F32),
                v(pair_codes.shape, I32),
                v(pair_groups.shape, I32),
                v(u_old.shape, F32),
                v((3, 8, 8, 128), F32),
                v((2, 3, 8, 128), F32),
                v((2, 1, 128), F32),
                v((2, 1, 128), F32),
                v((2, 2, 3, 1, 128), F32),
                v((ITERS, 3, 8, 8, 128), F32),
                v((ITERS, 2, 3, 8, 128), F32),
                v((ITERS, 2, 3, 8, 128), F32),
                v((ITERS, 2, 1, 128), F32),
                v((ITERS, 2, 1, 128), F32),
                v((ITERS, 2, 2, 2, 3, 1, 128), F32),
                v((3, 10, 8, 128), F32),
                v((3, 10, 8, 128), F32),
                v((2, 2, 3, 8, 128), F32),
                v((2, 1, 128), F32),
                v((2, 1, 128), F32),
                v((2, 2, 2, 3, 1, 128), F32),
                v((ITERS, 3, 8, 8, 128), F32),
                v((ITERS, 2, 3, 8, 128), F32),
                v((ITERS, 2, 3, 8, 128), F32),
                v((ITERS, 2, 1, 128), F32),
                v((ITERS, 2, 1, 128), F32),
                v((ITERS, 2, 2, 2, 3, 1, 128), F32),
                v((12, 64, 384), BF16),
                v((8, tiles, 384), F32),
                v((12, tiles, 128), F32),
                v((4, tiles, 128), I32),
                v((4, tiles, 128), I32),
                v((9, tiles, 128), F32),
                v((3, tiles, 128), F32),
                v((tiles, 256, 128), BF16),
                v((tiles, 128), F32),
                v((tiles, 128), F32),
                v((3, tiles * 8, 128), F32),
                v((8, 64, 384), F32),
                v((8, 128), F32),
                v((1, 128), F32),
                v((2 * nx * ny, 1, 128), F32),
                pltpu.SemaphoreType.REGULAR,
                pltpu.SemaphoreType.REGULAR,
                pltpu.SemaphoreType.DMA((6,)),
                pltpu.SemaphoreType.DMA((2 * ITERS, 18)),
                pltpu.SemaphoreType.DMA((2 * ITERS, 18)),
                pltpu.SemaphoreType.DMA,
                pltpu.SemaphoreType.DMA,
            ],
            compiler_params=pltpu.CompilerParams(
                collective_id=0, has_side_effects=True, vmem_limit_bytes=24 * 2**20
            ),
            name="relax",
        )(
            *(
                pltpu.with_memory_space_constraint(a, pltpu.HBM)
                for a in (tile_base, u_old, u_trial, jacobian_inverse, pair_codes, pair_groups)
            )
        )
        return pl.pallas_call(
            functools.partial(finish, cells),
            out_shape=(
                jax.ShapeDtypeStruct(u_old.shape, F32),
                jax.ShapeDtypeStruct((ITERS,), F32),
            ),
            in_specs=[pl.BlockSpec(memory_space=pl.ANY), pl.BlockSpec(memory_space=pltpu.VMEM)],
            out_specs=(pl.BlockSpec(memory_space=pl.ANY), smem),
            scratch_shapes=[pltpu.SemaphoreType.DMA],
            compiler_params=pltpu.CompilerParams(vmem_limit_bytes=2**20),
            name="finish",
        )(u_final, total)

    everywhere = ("gx", "gy", "gz")
    return jax.shard_map(
        step,
        mesh=mesh,
        in_specs=(
            P(None, "gx", "gy", "gz"),
            P(None, "gx", "gy", "gz"),
            P(None, None, "gx", "gy", "gz"),
            P(everywhere),
            P(None, everywhere, None),
            P(everywhere, None),
        ),
        out_specs=(P(None, "gx", "gy", "gz"), P()),
        check_vma=False,
    )
```

```python
import functools

import jax
import jax.numpy as jnp
from jax import lax
from jax.experimental import pallas as pl
from jax.experimental.pallas import tpu as pltpu
from jax.sharding import PartitionSpec as P

ITERS = 3
MESH = pl.DeviceIdType.MESH
F32 = jnp.float32
BF16 = jnp.bfloat16
I32 = jnp.int32

DIRS = sorted(
    [
        (dx, dy, z)
        for dx in (-1, 0, 1)
        for dy in (-1, 0, 1)
        for z in (0, 1)
        if (dx, dy, z) != (0, 0, 0)
    ],
    key=lambda d: (-2 * abs(d[0]) - abs(d[1]), d),
)


FAR = [d for d in DIRS if d[0] != 0]
NEAR = [d for d in DIRS if d[0] == 0]
PACKED_FAR = [d for d in FAR if d[1] == 0 and d[2] == 1]
PACKED_NEAR = [d for d in NEAR if d[1] != 0 and d[2] == 1]
PLAIN_FAR = [d for d in FAR if d not in PACKED_FAR]
PLAIN_NEAR = [d for d in NEAR if d not in PACKED_NEAR]


def slot_of(dx, dy, z):
    return ((dx + 1) * 3 + dy + 1) * 2 + z


def iota(shape, dim):
    return lax.broadcasted_iota(I32, shape, dim)


def take(x, idx):
    return jnp.take_along_axis(x, idx, axis=1, mode="promise_in_bounds")


def split(x):
    hi = x.astype(BF16).astype(F32)
    return hi, x - hi


def finish(cells, u, total, uout, nout, sem):
    store = pltpu.make_async_copy(u, uout, sem)
    store.start()
    norms = jnp.sqrt(total[...] / cells)
    for k in range(ITERS):
        nout[k] = jnp.sum(norms[:, k : k + 1])
    store.wait()


def kernel(
    nx, ny,
    tb_in, uold_in, utrial_in, jac_in, codes_in, groups_in,
    uout, nout,
    tb_ref, uold, jac, codes, groups, residuals,
    uc, uy, uxe, uye, ud, rxz, rxx, rxy, rxxe, rxye, rxd,
    pb, pz, yr, fxe, fye, fd, frz, frx, fry, frxe, frye, frd,
    win, gat, early, kidx, lidx, geo, frozen, onehot, ohg, ohs, outs, acc,
    sq, total_row, table,
    hail_four, hail_eight, in_sem, send_sem, recv_sem, total_send, total_recv,
):
    gx, gy, gz = lax.axis_index("gx"), lax.axis_index("gy"), lax.axis_index("gz")
    tiles = groups.shape[0]
    x_ok = {-1: gx > 0, 0: None, 1: gx < nx - 1}
    y_ok = {-1: gy > 0, 0: None, 1: gy < ny - 1}

    def exists(dx, dy):
        if dx == 0 and dy == 0:
            return None
        if dx == 0:
            return y_ok[dy]
        if dy == 0:
            return x_ok[dx]
        return jnp.logical_and(x_ok[dx], y_ok[dy])

    def guarded(cond, fn):
        if cond is None:
            fn()
        else:
            pl.when(cond)(fn)

    def valid(cond, value):
        return value if cond is None else jnp.where(cond, value, 0.0)

    def target(dx, dy, z):
        return (gx + dx, gy + dy, gz if z == 0 else 1 - gz)

    barrier = pltpu.get_barrier_semaphore()

    def greet(device):
        pl.semaphore_signal(barrier, inc=1, device_id=device, device_id_type=MESH)

    for d in DIRS:
        guarded(exists(d[0], d[1]), functools.partial(greet, target(*d)))

    fetches = [
        pltpu.make_async_copy(src, dst, in_sem.at[k])
        for k, (src, dst) in enumerate(
            [
                (utrial_in, uc),
                (tb_in, tb_ref),
                (codes_in, codes),
                (groups_in, groups),
                (uold_in, uold),
                (jac_in, jac),
            ]
        )
    ]
    for fetch in fetches:
        fetch.start()

    def lo_hi(d):
        return 1 if d > 0 else 0

    def displacement_message(it, d):
        dx, dy, z = d
        xi, yi = lo_hi(dx), lo_hi(dy)
        if dx == 0 and dy == 0:
            return uc, rxz.at[it]
        if dy == 0:
            if z:
                return uxe.at[xi], rxxe.at[it, 1 - xi]
            return uc.at[:, 7 * xi], rxx.at[it, 1 - xi]
        if dx == 0:
            if z:
                return uye.at[yi], rxye.at[it, 1 - yi]
            return uy.at[yi], rxy.at[it, 1 - yi]
        return ud.at[xi, yi], rxd.at[it, 1 - xi, 1 - yi, z]

    def force_message(it, d):
        dx, dy, z = d
        xi, yi = lo_hi(dx), lo_hi(dy)
        if dx == 0 and dy == 0:
            return pz.at[:, 1:9], frz.at[it]
        if dy == 0:
            if z:
                return fxe.at[xi], frxe.at[it, 1 - xi]
            return pb.at[:, 9 * xi], frx.at[it, 1 - xi]
        if dx == 0:
            if z:
                return fye.at[yi], frye.at[it, 1 - yi]
            return yr.at[0, yi], fry.at[it, 1 - yi]
        return fd.at[z, xi, yi], frd.at[it, 1 - xi, 1 - yi, z]

    def copy_of(message, it, phase, d):
        src, dst = message(it, d)
        dx, dy, z = d
        return pltpu.make_async_remote_copy(
            src_ref=src,
            dst_ref=dst,
            send_sem=send_sem.at[phase, slot_of(dx, dy, z)],
            recv_sem=recv_sem.at[phase, slot_of(-dx, -dy, z)],
            device_id=target(dx, dy, z),
            device_id_type=MESH,
        )

    def grouped(dirs, act):
        for dx, dy in dict.fromkeys((d[0], d[1]) for d in dirs):

            def both(dx=dx, dy=dy):
                for d in dirs:
                    if (d[0], d[1]) == (dx, dy):
                        act(d)

            guarded(exists(dx, dy), both)

    def start(message, it, phase, dirs):
        grouped(dirs, lambda d: copy_of(message, it, phase, d).start())

    def wait_arrivals(message, it, phase, dirs):
        grouped(dirs, lambda d: copy_of(message, it, phase, (-d[0], -d[1], d[2])).wait_recv())

    def wait_sends(message, it, phase):
        grouped(DIRS, lambda d: copy_of(message, it, phase, d).wait_send())

    row8 = iota((8, 128), 0)
    lane8 = iota((8, 128), 1)

    my_edge = jnp.where(gz == 0, 127, 0)
    other_edge = 127 - my_edge
    my_edge_index = jnp.full((8, 128), my_edge, I32)
    other_edge_index = jnp.full((8, 128), other_edge, I32)
    column_lane = [row8 + 8 * c for c in range(3)]

    def edges(planes, index):
        packed = jnp.zeros((8, 128), F32)
        for c in range(3):
            packed = jnp.where(lane8 == column_lane[c], take(planes[c], index), packed)
        return jnp.sum(packed, axis=0, keepdims=True)

    def column(row, c):
        return take(jnp.broadcast_to(row, (8, 128)), column_lane[c])

    def corner_rows():
        for xi, x in ((0, 0), (1, 7)):
            for yi in range(2):
                for c in range(3):
                    ud[xi, yi, c] = uy[yi, c, x : x + 1, :]

    def send_displacements(it, phase):
        start(displacement_message, it, phase, PLAIN_FAR)
        start(displacement_message, it, phase, PLAIN_NEAR)
        for i in range(2):
            uxe[i] = edges([uc[c, 7 * i] for c in range(3)], my_edge_index)
            uye[i] = edges([uy[i, c] for c in range(3)], my_edge_index)
        start(displacement_message, it, phase, PACKED_FAR)
        start(displacement_message, it, phase, PACKED_NEAR)

    fetches[0].wait()
    for c in range(3):
        for x in range(8):
            plane = uc[c, x]
            uy[0, c, x : x + 1, :] = plane[0:1]
            uy[1, c, x : x + 1, :] = plane[7:8]
    corner_rows()
    beside_x = (gx > 0).astype(I32) + (gx < nx - 1).astype(I32)
    beside_y = (gy > 0).astype(I32) + (gy < ny - 1).astype(I32)
    pl.semaphore_wait(barrier, 2 * (1 + beside_x) * (1 + beside_y) - 1)
    send_displacements(0, 0)

    for fetch in fetches[1:]:
        fetch.wait()
    lane_k = iota((8, 128), 1)
    for g in range(tiles // 8):
        base = jnp.zeros((8, 128), I32)
        for i in range(8):
            base = jnp.where(row8 == i, tb_ref[g * 8 + i], base)
        s = (base >> 4) & 1
        sz = base & 15
        par = sz & 1
        j = sz >> 1
        sx = base >> 5
        i_of = (16 - j - par) & 7
        turn = j + par + jnp.where(s == 0, -2, 2)
        place = s * 16 + par * 8 + i_of
        ohg[g * 8 : g * 8 + 8, :] = jnp.where(
            jnp.logical_and((lane_k >> 6) == sx, (lane_k & 31) == place), 1.0, 0.0
        )
        ohs[g * 8 : g * 8 + 8, :] = jnp.where(lane_k == sx * 32 + place, 1.0, 0.0)
        q0 = codes[0, g * 8 : g * 8 + 8, :]
        q1 = codes[1, g * 8 : g * 8 + 8, :]
        q2 = codes[2, g * 8 : g * 8 + 8, :]
        q3 = codes[3, g * 8 : g * 8 + 8, :]

        def unit(q):
            sign = 1 - 2 * (q & 1)
            axis = q >> 1
            return [jnp.where(axis == k, sign, 0) for k in range(3)]

        e1, e2 = unit(q1), unit(q3)
        off = [((q2 * 57) >> 9) - 1, 0, 0]
        third = (q2 * 43) >> 7
        off[1] = third - 3 * (off[0] + 1) - 1
        off[2] = q2 - 3 * third - 1
        first = [(q0 >> 5) + 2, ((q0 >> 3) & 3) + 2, (q0 & 7) + 2]
        nodes = [first, [first[k] + e1[k] for k in range(3)], [first[k] + off[k] for k in range(3)]]
        nodes.append([nodes[2][k] + e2[k] for k in range(3)])
        for n in range(4):
            x, y, z = nodes[n]
            kidx[n, g * 8 : g * 8 + 8, :] = x
            lidx[n, g * 8 : g * 8 + 8, :] = ((y + turn) & 7) * 16 + z
        for k in range(3):
            a, b = e1[k].astype(F32), e2[k].astype(F32)
            geo[k, g * 8 : g * 8 + 8, :] = a
            geo[3 + k, g * 8 : g * 8 + 8, :] = b
            geo[6 + k, g * 8 : g * 8 + 8, :] = off[k].astype(F32) + 0.5 * b - 0.5 * a
    for c in range(3):
        frozen[c] = jnp.zeros((tiles, 128), F32)
    zero_plane = jnp.zeros((64, 384), BF16)
    win[0] = zero_plane
    win[11] = zero_plane

    row128 = iota((128, 128), 0)

    def make_onehot(t, carry):
        for n in range(2):
            first = lidx[2 * n, pl.ds(t, 1), :]
            second = lidx[2 * n + 1, pl.ds(t, 1), :]
            sign = 1.0 if n else -1.0
            flat = jnp.where(jnp.logical_or(row128 == first, row128 == second), sign, 0.0).astype(BF16)
            onehot[t, n * 128 : (n + 1) * 128, :] = jnp.transpose(flat)
        return carry

    lax.fori_loop(0, tiles, make_onehot, 0, unroll=4)
    pick = ohg[...].astype(BF16)
    spread_t = jnp.transpose(ohs[...])[0:64, 0:tiles].astype(BF16)
    spread = jnp.concatenate([spread_t, spread_t], axis=1)

    group_bits = [((lane8 >> 4) & bit) != 0 for bit in (1, 2, 4)]
    unroll = [(lane8 + 16 * row8 + 2 + 8 * p) & 127 for p in (0, 1)]
    edge_row = {0: row8 == 7, 1: row8 == 0}
    edge_lane = {0: lane8 == 127, 1: lane8 == 0}
    z_ok = {0: gz == 1, 1: gz == 0}
    my_edge_lane = lane8 == other_edge
    at_edge = lane8 == my_edge

    count = 2 * nx * ny
    me = (gx * ny + gy) * 2 + gz

    xs = [lax.rem(gx + a, nx) for a in range(nx)]
    ys = [lax.rem(gy + b, ny) for b in range(ny)]

    def ring(o, n):
        return min(o, n - o)

    offsets = [(a, b, c) for a in range(nx) for b in range(ny) for c in range(2) if (a, b, c) != (0, 0, 0)]
    offsets.sort(
        key=lambda o: -(ring(o[0] // 4, nx // 4) + ring(o[0] % 4, 4) + ring(o[1], ny))
    )

    def send_squares():
        for a, b, c in offsets:
            pltpu.make_async_remote_copy(
                src_ref=total_row,
                dst_ref=table.at[me],
                send_sem=total_send,
                recv_sem=total_recv,
                device_id=(xs[a], ys[b], 1 - gz if c else gz),
                device_id_type=MESH,
            ).start()

    def hail(semaphore, width):
        for dx in (-width, width):
            cond = gx + dx >= 0 if dx < 0 else gx + dx < nx

            def signal(dx=dx):
                pl.semaphore_signal(
                    semaphore, inc=1, device_id=(gx + dx, gy, gz), device_id_type=MESH
                )

            pl.when(cond)(signal)

    def hear(semaphore, width):
        pl.semaphore_wait(semaphore, (gx >= width).astype(I32) + (gx + width < nx).astype(I32))

    def iteration(it, carry):
        wait_arrivals(displacement_message, it, 2 * it, NEAR)

        beyond_rows = [
            [column(valid(y_ok[dy], rxye[it, lo_hi(dy)]), c) for c in range(3)] for dy in (-1, 1)
        ]
        def make_windows(x):
            for c in range(3):
                if 1 <= x <= 8:
                    own, other = uc[c, x - 1], rxz[it, c, x - 1]
                    rows = [
                        [
                            valid(y_ok[dy], rxy[it, lo_hi(dy), c, x - 1 : x, :]),
                            beyond_rows[lo_hi(dy)][c][x - 1 : x],
                        ]
                        for dy in (-1, 1)
                    ]
                else:
                    dx, xi = (-1, 0) if x == 0 else (1, 1)
                    own = valid(x_ok[dx], rxx[it, xi, c])
                    other = column(valid(x_ok[dx], rxxe[it, xi]), c)
                    rows = [
                        [
                            valid(exists(dx, dy), rxd[it, xi, lo_hi(dy), z, c])
                            for z in (0, 1)
                        ]
                        for dy in (-1, 1)
                    ]
                for s in range(2):
                    near = jnp.where(edge_row[s], rows[s][0], own)
                    far = jnp.where(edge_row[s], rows[s][1], other)
                    pair = []
                    for p in range(2):
                        source = jnp.where(edge_lane[p], jnp.where(z_ok[p], far, 0.0), near)
                        v = pltpu.roll(source, 2 + 8 * p, axis=1, stride=16, stride_axis=0)
                        for bit, mask in zip((1, 2, 4), group_bits):
                            v = jnp.where(mask, pltpu.roll(v, 8 - bit, axis=0), v)
                        pair.append(v)
                    both = jnp.concatenate(pair, axis=0)
                    hi, lo = split(both)
                    win[x + 1, s * 16 : s * 16 + 16, c * 128 : (c + 1) * 128] = hi.astype(BF16)
                    win[x + 1, 32 + s * 16 : 48 + s * 16, c * 128 : (c + 1) * 128] = lo.astype(BF16)

        def hand_out(k):
            both = jnp.concatenate([win[k], win[k + 4]], axis=0)
            gat[k] = jnp.dot(pick, both, preferred_element_type=F32)

        def look_up(n, at, planes, found):
            ks = kidx[n, at, :]
            ls = lidx[n, at, :]
            for k in planes:
                for c in range(3):
                    value = take(gat[k, at, c * 128 : (c + 1) * 128], ls)
                    found[c] = value if found[c] is None else jnp.where(ks == k, value, found[c])
            return found

        for x in range(1, 9):
            make_windows(x)
        for k in (0, 2, 3, 4, 5, 7):
            hand_out(k)
        for g in range(tiles // 8):
            at = pl.ds(g * 8, 8)
            for n in range(4):
                planes = (0, 2, 3, 4, 5, 7) if n == 3 else (2, 3, 4, 5)
                found = look_up(n, at, planes, [None] * 3)
                for c in range(3):
                    early[3 * n + c, at, :] = found[c]

        @pl.when(it > 0)
        def _():
            wait_sends(force_message, it - 1, 2 * it - 1)

        wait_arrivals(displacement_message, it, 2 * it, FAR)
        for x in (0, 9):
            make_windows(x)
        for k in (1, 6):
            hand_out(k)

        @pl.when(it == 2)
        def _():
            hear(hail_four, 4)
            hail(hail_eight, 8)

        live_below = jnp.where(it == 0, 2, 1)

        def pair_forces(g):
            at = pl.ds(pl.multiple_of(g * 8, 8), 8)
            points = []
            for n in range(4):
                found = [early[3 * n + c, at, :] for c in range(3)]
                if n > 0:
                    found = look_up(n, at, (1, 6), found)
                points.append(found)
            one = [points[1][c] - points[0][c] + geo[c, at, :] for c in range(3)]
            two = [points[3][c] - points[2][c] + geo[3 + c, at, :] for c in range(3)]
            apart = [
                0.5 * (points[2][c] + points[3][c]) - 0.5 * (points[0][c] + points[1][c])
                + geo[6 + c, at, :]
                for c in range(3)
            ]
            square = apart[0] * apart[0] + apart[1] * apart[1] + apart[2] * apart[2] + 0.5
            dots = one[0] * two[0] + one[1] * two[1] + one[2] * two[2]
            coupling = 0.5 * dots / (square * jnp.sqrt(square))
            fresh = groups[at, :] < live_below
            values = []
            for c in range(3):
                force = jnp.where(fresh, coupling * apart[c], frozen[c, at, :])
                frozen[c, at, :] = force
                values.extend(split(0.5 * force))
            return tuple(values)

        def spread_forces(g, values):
            for i in range(8):
                t = g * 8 + i
                columns = []
                for n in range(2):
                    mask = jnp.logical_or(
                        row8 == kidx[2 * n, pl.ds(t, 1), :], row8 == kidx[2 * n + 1, pl.ds(t, 1), :]
                    )
                    columns.append(
                        jnp.concatenate(
                            [jnp.where(mask, v[i : i + 1], 0.0) for v in values], axis=0
                        ).astype(BF16)
                    )
                lhs = jnp.concatenate(columns, axis=1)
                got = jnp.dot(lhs, onehot[t], preferred_element_type=F32)
                for c in range(3):
                    outs[c, pl.ds(pl.multiple_of(t * 8, 8), 8), :] = (
                        got[16 * c : 16 * c + 8] + got[16 * c + 8 : 16 * c + 16]
                    )

        def group(g, values):
            later = pair_forces(g)
            spread_forces(g - 1, values)
            return later

        values = lax.fori_loop(1, tiles // 8, group, pair_forces(0), unroll=7)
        spread_forces(tiles // 8 - 1, values)

        def collect(k):
            columns = []
            for c in range(3):
                hi, lo = split(outs[c, pl.ds(k, tiles, stride=8), :])
                columns.append(jnp.concatenate([hi, lo], axis=0).astype(BF16))
            acc[k] = jnp.dot(spread, jnp.concatenate(columns, axis=1), preferred_element_type=F32)

        def fold(x):
            for c in range(3):
                cut = slice(c * 128, (c + 1) * 128)
                parts = []
                for s in range(2):
                    line, beyond = None, None
                    for p in range(2):
                        at = s * 16 + p * 8
                        v = None
                        if x + 1 <= 7:
                            v = acc[x + 1, at : at + 8, cut]
                        if x + 1 >= 4:
                            w = acc[x - 3, 32 + at : 40 + at, cut]
                            v = w if v is None else v + w
                        for bit, mask in zip((1, 2, 4), group_bits):
                            v = jnp.where(mask, pltpu.roll(v, bit, axis=0), v)
                        v = take(v, unroll[p])
                        inside = jnp.where(edge_lane[p], 0.0, v)
                        outside = jnp.where(z_ok[p], v, 0.0)
                        line = inside if line is None else line + inside
                        beyond = outside if beyond is None else beyond + outside
                    parts.append((line, jnp.where(my_edge_lane, beyond, 0.0)))
                for z in range(2):
                    (pz if z else pb)[c, x] = jnp.where(edge_row[0], 0.0, parts[0][z]) + jnp.where(
                        edge_row[1], 0.0, parts[1][z]
                    )
                    ends = (parts[0][z][7:8], parts[1][z][0:1])
                    for yi in range(2):
                        if 1 <= x <= 8:
                            yr[z, yi, c, x - 1 : x, :] = ends[yi]
                        else:
                            fd[z, 0 if x == 0 else 1, yi, c] = ends[yi]

        for k in (1, 6):
            collect(k)
        for x in (0, 9):
            fold(x)
        start(force_message, it, 2 * it + 1, PLAIN_FAR)
        for i in range(2):
            fxe[i] = edges([pz[c, 9 * i] for c in range(3)], other_edge_index)
        start(force_message, it, 2 * it + 1, PACKED_FAR)
        for k in (0, 2, 3, 4, 5, 7):
            collect(k)
        for x in range(1, 9):
            fold(x)
        start(force_message, it, 2 * it + 1, PLAIN_NEAR)
        for i in range(2):
            fye[i] = edges([yr[1, i, c] for c in range(3)], other_edge_index)
        start(force_message, it, 2 * it + 1, PACKED_NEAR)
        wait_sends(displacement_message, it, 2 * it)
        wait_arrivals(force_message, it, 2 * it + 1, NEAR)

        lines = []
        for dy in (-1, 1):
            yi = lo_hi(dy)
            lines.append(
                [
                    valid(
                        y_ok[dy],
                        fry[it, yi, c] + jnp.where(at_edge, column(frye[it, yi], c), 0.0),
                    )
                    for c in range(3)
                ]
            )
        def residual_of(x, squares):
            for c in range(3):
                total = pb[c, x + 1] + frz[it, c, x]
                for dx, xe in ((-1, 0), (1, 7)):
                    if x == xe:
                        xi = lo_hi(dx)
                        total = total + valid(
                            x_ok[dx],
                            frx[it, xi, c] + jnp.where(at_edge, column(frxe[it, xi], c), 0.0),
                        )
                for dy in (-1, 1):
                    yi = lo_hi(dy)
                    line = lines[yi][c][x : x + 1]
                    for dx, xe in ((-1, 0), (1, 7)):
                        if x == xe:
                            xi = lo_hi(dx)
                            line = line + valid(
                                exists(dx, dy),
                                frd[it, xi, yi, 0, c] + frd[it, xi, yi, 1, c],
                            )
                    total = total + jnp.where(row8 == (0 if dy < 0 else 7), line, 0.0)
                r = uc[c, x] - uold[c, x] - 0.5 * total
                squares = squares + r * r
                residuals[c, x] = r
            return squares

        def update(x):
            residual = [residuals[c, x] for c in range(3)]
            for a in range(3):
                fix = jac[a, 0, x] * residual[0] + jac[a, 1, x] * residual[1] + jac[a, 2, x] * residual[2]
                new = uc[a, x] - fix
                uc[a, x] = new
                uy[0, a, x : x + 1, :] = new[0:1]
                uy[1, a, x : x + 1, :] = new[7:8]

        squares = jnp.zeros((8, 128), F32)
        for x in range(1, 7):
            squares = residual_of(x, squares)
        for x in range(1, 7):
            update(x)
        wait_arrivals(force_message, it, 2 * it + 1, FAR)

        @pl.when(it == 1)
        def _():
            hail(hail_four, 4)

        @pl.when(it == 2)
        def _():
            hear(hail_eight, 8)

        for x in (0, 7):
            squares = residual_of(x, squares)
        sq[pl.ds(it, 1), :] = jnp.sum(squares, axis=0, keepdims=True)
        for x in (0, 7):
            update(x)

        @pl.when(it == ITERS - 1)
        def _():
            sums = jnp.sum(sq[...], axis=1, keepdims=True)
            row = jnp.sum(jnp.where(row8 == lane8, sums, 0.0), axis=0, keepdims=True)
            total_row[...] = row
            table[me] = row
            send_squares()

        @pl.when(it < ITERS - 1)
        def _():
            corner_rows()
            send_displacements(it + 1, 2 * it + 2)

        return carry

    sq[...] = jnp.zeros((8, 128), F32)
    lax.fori_loop(0, ITERS, iteration, 0)
    store_result = pltpu.make_async_copy(uc, uout, in_sem.at[0])
    store_result.start()
    wait_sends(force_message, ITERS - 1, 2 * ITERS - 1)
    others = table.at[0 : count - 1]
    pltpu.make_async_copy(others, others, total_recv).wait()
    pltpu.make_async_copy(others, others, total_send).wait()
    nout[...] = jnp.sum(table[...], axis=0)
    store_result.wait()


def solution(mesh):
    nx, ny = mesh.shape["gx"], mesh.shape["gy"]

    def step(u_old, u_trial, jacobian_inverse, tile_base, pair_codes, pair_groups):
        tiles = tile_base.shape[0]
        cells = float(3 * 8 * 8 * 128 * nx * ny * mesh.shape["gz"])
        smem = pl.BlockSpec(memory_space=pltpu.SMEM)
        v = pltpu.VMEM
        u_final, total = pl.pallas_call(
            functools.partial(kernel, nx, ny),
            out_shape=(
                jax.ShapeDtypeStruct(u_old.shape, F32),
                jax.ShapeDtypeStruct((1, 128), F32),
            ),
            in_specs=[pl.BlockSpec(memory_space=pltpu.HBM)] * 6,
            out_specs=(pl.BlockSpec(memory_space=pl.ANY), pl.BlockSpec(memory_space=pltpu.VMEM)),
            scratch_shapes=[
                pltpu.SMEM(tile_base.shape, I32),
                v(u_old.shape, F32),
                v(jacobian_inverse.shape, F32),
                v(pair_codes.shape, I32),
                v(pair_groups.shape, I32),
                v(u_old.shape, F32),
                v((3, 8, 8, 128), F32),
                v((2, 3, 8, 128), F32),
                v((2, 1, 128), F32),
                v((2, 1, 128), F32),
                v((2, 2, 3, 1, 128), F32),
                v((ITERS, 3, 8, 8, 128), F32),
                v((ITERS, 2, 3, 8, 128), F32),
                v((ITERS, 2, 3, 8, 128), F32),
                v((ITERS, 2, 1, 128), F32),
                v((ITERS, 2, 1, 128), F32),
                v((ITERS, 2, 2, 2, 3, 1, 128), F32),
                v((3, 10, 8, 128), F32),
                v((3, 10, 8, 128), F32),
                v((2, 2, 3, 8, 128), F32),
                v((2, 1, 128), F32),
                v((2, 1, 128), F32),
                v((2, 2, 2, 3, 1, 128), F32),
                v((ITERS, 3, 8, 8, 128), F32),
                v((ITERS, 2, 3, 8, 128), F32),
                v((ITERS, 2, 3, 8, 128), F32),
                v((ITERS, 2, 1, 128), F32),
                v((ITERS, 2, 1, 128), F32),
                v((ITERS, 2, 2, 2, 3, 1, 128), F32),
                v((12, 64, 384), BF16),
                v((8, tiles, 384), F32),
                v((12, tiles, 128), F32),
                v((4, tiles, 128), I32),
                v((4, tiles, 128), I32),
                v((9, tiles, 128), F32),
                v((3, tiles, 128), F32),
                v((tiles, 256, 128), BF16),
                v((tiles, 128), F32),
                v((tiles, 128), F32),
                v((3, tiles * 8, 128), F32),
                v((8, 64, 384), F32),
                v((8, 128), F32),
                v((1, 128), F32),
                v((2 * nx * ny, 1, 128), F32),
                pltpu.SemaphoreType.REGULAR,
                pltpu.SemaphoreType.REGULAR,
                pltpu.SemaphoreType.DMA((6,)),
                pltpu.SemaphoreType.DMA((2 * ITERS, 18)),
                pltpu.SemaphoreType.DMA((2 * ITERS, 18)),
                pltpu.SemaphoreType.DMA,
                pltpu.SemaphoreType.DMA,
            ],
            compiler_params=pltpu.CompilerParams(
                collective_id=0, has_side_effects=True, vmem_limit_bytes=24 * 2**20
            ),
            name="relax",
        )(
            *(
                pltpu.with_memory_space_constraint(a, pltpu.HBM)
                for a in (tile_base, u_old, u_trial, jacobian_inverse, pair_codes, pair_groups)
            )
        )
        return pl.pallas_call(
            functools.partial(finish, cells),
            out_shape=(
                jax.ShapeDtypeStruct(u_old.shape, F32),
                jax.ShapeDtypeStruct((ITERS,), F32),
            ),
            in_specs=[pl.BlockSpec(memory_space=pl.ANY), pl.BlockSpec(memory_space=pltpu.VMEM)],
            out_specs=(pl.BlockSpec(memory_space=pl.ANY), smem),
            scratch_shapes=[pltpu.SemaphoreType.DMA],
            compiler_params=pltpu.CompilerParams(vmem_limit_bytes=2**20),
            name="finish",
        )(u_final, total)

    everywhere = ("gx", "gy", "gz")
    return jax.shard_map(
        step,
        mesh=mesh,
        in_specs=(
            P(None, "gx", "gy", "gz"),
            P(None, "gx", "gy", "gz"),
            P(None, None, "gx", "gy", "gz"),
            P(everywhere),
            P(None, everywhere, None),
            P(everywhere, None),
        ),
        out_specs=(P(None, "gx", "gy", "gz"), P()),
        check_vma=False,
    )
```

```python
import functools

import jax
import jax.numpy as jnp
from jax import lax
from jax.experimental import pallas as pl
from jax.experimental.pallas import tpu as pltpu
from jax.sharding import PartitionSpec as P

ITERS = 3
MESH = pl.DeviceIdType.MESH
F32 = jnp.float32
BF16 = jnp.bfloat16
I32 = jnp.int32

DIRS = sorted(
    [
        (dx, dy, z)
        for dx in (-1, 0, 1)
        for dy in (-1, 0, 1)
        for z in (0, 1)
        if (dx, dy, z) != (0, 0, 0)
    ],
    key=lambda d: (-2 * abs(d[0]) - abs(d[1]), d),
)


FAR = [d for d in DIRS if d[0] != 0]
NEAR = [d for d in DIRS if d[0] == 0]
PACKED_FAR = [d for d in FAR if d[1] == 0 and d[2] == 1]
PACKED_NEAR = [d for d in NEAR if d[1] != 0 and d[2] == 1]
PLAIN_FAR = [d for d in FAR if d not in PACKED_FAR]
PLAIN_NEAR = [d for d in NEAR if d not in PACKED_NEAR]


def slot_of(dx, dy, z):
    return ((dx + 1) * 3 + dy + 1) * 2 + z


def iota(shape, dim):
    return lax.broadcasted_iota(I32, shape, dim)


def take(x, idx):
    return jnp.take_along_axis(x, idx, axis=1, mode="promise_in_bounds")


def split(x):
    hi = x.astype(BF16).astype(F32)
    return hi, x - hi


def finish(cells, u, total, uout, nout, sem):
    store = pltpu.make_async_copy(u, uout, sem)
    store.start()
    norms = jnp.sqrt(total[...] / cells)
    for k in range(ITERS):
        nout[k] = jnp.sum(norms[:, k : k + 1])
    store.wait()


def kernel(
    nx, ny,
    tb_in, uold_in, utrial_in, jac_in, codes_in, groups_in,
    uout, nout,
    tb_ref, uold, jac, codes, groups, residuals,
    uc, uy, uxe, uye, ud, rxz, rxx, rxy, rxxe, rxye, rxd,
    pb, pz, yr, fxe, fye, fd, frz, frx, fry, frxe, frye, frd,
    win, gat, early, kidx, lidx, geo, frozen, onehot, ohg, ohs, outs, acc,
    sq, total_row, table,
    hail_four, hail_eight, in_sem, send_sem, recv_sem, total_send, total_recv,
):
    gx, gy, gz = lax.axis_index("gx"), lax.axis_index("gy"), lax.axis_index("gz")
    tiles = groups.shape[0]
    x_ok = {-1: gx > 0, 0: None, 1: gx < nx - 1}
    y_ok = {-1: gy > 0, 0: None, 1: gy < ny - 1}

    def exists(dx, dy):
        if dx == 0 and dy == 0:
            return None
        if dx == 0:
            return y_ok[dy]
        if dy == 0:
            return x_ok[dx]
        return jnp.logical_and(x_ok[dx], y_ok[dy])

    def guarded(cond, fn):
        if cond is None:
            fn()
        else:
            pl.when(cond)(fn)

    def valid(cond, value):
        return value if cond is None else jnp.where(cond, value, 0.0)

    def target(dx, dy, z):
        return (gx + dx, gy + dy, gz if z == 0 else 1 - gz)

    barrier = pltpu.get_barrier_semaphore()

    def greet(device):
        pl.semaphore_signal(barrier, inc=1, device_id=device, device_id_type=MESH)

    for d in DIRS:
        guarded(exists(d[0], d[1]), functools.partial(greet, target(*d)))

    fetches = [
        pltpu.make_async_copy(src, dst, in_sem.at[k])
        for k, (src, dst) in enumerate(
            [
                (utrial_in, uc),
                (tb_in, tb_ref),
                (codes_in, codes),
                (groups_in, groups),
                (uold_in, uold),
                (jac_in, jac),
            ]
        )
    ]
    for fetch in fetches:
        fetch.start()

    def lo_hi(d):
        return 1 if d > 0 else 0

    def displacement_message(it, d):
        dx, dy, z = d
        xi, yi = lo_hi(dx), lo_hi(dy)
        if dx == 0 and dy == 0:
            return uc, rxz.at[it]
        if dy == 0:
            if z:
                return uxe.at[xi], rxxe.at[it, 1 - xi]
            return uc.at[:, 7 * xi], rxx.at[it, 1 - xi]
        if dx == 0:
            if z:
                return uye.at[yi], rxye.at[it, 1 - yi]
            return uy.at[yi], rxy.at[it, 1 - yi]
        return ud.at[xi, yi], rxd.at[it, 1 - xi, 1 - yi, z]

    def force_message(it, d):
        dx, dy, z = d
        xi, yi = lo_hi(dx), lo_hi(dy)
        if dx == 0 and dy == 0:
            return pz.at[:, 1:9], frz.at[it]
        if dy == 0:
            if z:
                return fxe.at[xi], frxe.at[it, 1 - xi]
            return pb.at[:, 9 * xi], frx.at[it, 1 - xi]
        if dx == 0:
            if z:
                return fye.at[yi], frye.at[it, 1 - yi]
            return yr.at[0, yi], fry.at[it, 1 - yi]
        return fd.at[z, xi, yi], frd.at[it, 1 - xi, 1 - yi, z]

    def copy_of(message, it, phase, d):
        src, dst = message(it, d)
        dx, dy, z = d
        return pltpu.make_async_remote_copy(
            src_ref=src,
            dst_ref=dst,
            send_sem=send_sem.at[phase, slot_of(dx, dy, z)],
            recv_sem=recv_sem.at[phase, slot_of(-dx, -dy, z)],
            device_id=target(dx, dy, z),
            device_id_type=MESH,
        )

    def grouped(dirs, act):
        for dx, dy in dict.fromkeys((d[0], d[1]) for d in dirs):

            def both(dx=dx, dy=dy):
                for d in dirs:
                    if (d[0], d[1]) == (dx, dy):
                        act(d)

            guarded(exists(dx, dy), both)

    def start(message, it, phase, dirs):
        grouped(dirs, lambda d: copy_of(message, it, phase, d).start())

    def wait_arrivals(message, it, phase, dirs):
        grouped(dirs, lambda d: copy_of(message, it, phase, (-d[0], -d[1], d[2])).wait_recv())

    def wait_sends(message, it, phase):
        grouped(DIRS, lambda d: copy_of(message, it, phase, d).wait_send())

    row8 = iota((8, 128), 0)
    lane8 = iota((8, 128), 1)

    my_edge = jnp.where(gz == 0, 127, 0)
    other_edge = 127 - my_edge
    my_edge_index = jnp.full((8, 128), my_edge, I32)
    other_edge_index = jnp.full((8, 128), other_edge, I32)
    column_lane = [row8 + 8 * c for c in range(3)]

    def edges(planes, index):
        packed = jnp.zeros((8, 128), F32)
        for c in range(3):
            packed = jnp.where(lane8 == column_lane[c], take(planes[c], index), packed)
        return jnp.sum(packed, axis=0, keepdims=True)

    def column(row, c):
        return take(jnp.broadcast_to(row, (8, 128)), column_lane[c])

    def corner_rows():
        for xi, x in ((0, 0), (1, 7)):
            for yi in range(2):
                for c in range(3):
                    ud[xi, yi, c] = uy[yi, c, x : x + 1, :]

    def send_displacements(it, phase):
        start(displacement_message, it, phase, PLAIN_FAR)
        start(displacement_message, it, phase, PLAIN_NEAR)
        for i in range(2):
            uxe[i] = edges([uc[c, 7 * i] for c in range(3)], my_edge_index)
            uye[i] = edges([uy[i, c] for c in range(3)], my_edge_index)
        start(displacement_message, it, phase, PACKED_FAR)
        start(displacement_message, it, phase, PACKED_NEAR)

    fetches[0].wait()
    for c in range(3):
        for x in range(8):
            plane = uc[c, x]
            uy[0, c, x : x + 1, :] = plane[0:1]
            uy[1, c, x : x + 1, :] = plane[7:8]
    corner_rows()
    beside_x = (gx > 0).astype(I32) + (gx < nx - 1).astype(I32)
    beside_y = (gy > 0).astype(I32) + (gy < ny - 1).astype(I32)
    pl.semaphore_wait(barrier, 2 * (1 + beside_x) * (1 + beside_y) - 1)
    send_displacements(0, 0)

    for fetch in fetches[1:]:
        fetch.wait()
    lane_k = iota((8, 128), 1)
    for g in range(tiles // 8):
        base = jnp.zeros((8, 128), I32)
        for i in range(8):
            base = jnp.where(row8 == i, tb_ref[g * 8 + i], base)
        s = (base >> 4) & 1
        sz = base & 15
        par = sz & 1
        j = sz >> 1
        sx = base >> 5
        i_of = (16 - j - par) & 7
        turn = j + par + jnp.where(s == 0, -2, 2)
        place = s * 16 + par * 8 + i_of
        ohg[g * 8 : g * 8 + 8, :] = jnp.where(
            jnp.logical_and((lane_k >> 6) == sx, (lane_k & 31) == place), 1.0, 0.0
        )
        ohs[g * 8 : g * 8 + 8, :] = jnp.where(lane_k == sx * 32 + place, 1.0, 0.0)
        q0 = codes[0, g * 8 : g * 8 + 8, :]
        q1 = codes[1, g * 8 : g * 8 + 8, :]
        q2 = codes[2, g * 8 : g * 8 + 8, :]
        q3 = codes[3, g * 8 : g * 8 + 8, :]

        def unit(q):
            sign = 1 - 2 * (q & 1)
            axis = q >> 1
            return [jnp.where(axis == k, sign, 0) for k in range(3)]

        e1, e2 = unit(q1), unit(q3)
        off = [((q2 * 57) >> 9) - 1, 0, 0]
        third = (q2 * 43) >> 7
        off[1] = third - 3 * (off[0] + 1) - 1
        off[2] = q2 - 3 * third - 1
        first = [(q0 >> 5) + 2, ((q0 >> 3) & 3) + 2, (q0 & 7) + 2]
        nodes = [first, [first[k] + e1[k] for k in range(3)], [first[k] + off[k] for k in range(3)]]
        nodes.append([nodes[2][k] + e2[k] for k in range(3)])
        for n in range(4):
            x, y, z = nodes[n]
            kidx[n, g * 8 : g * 8 + 8, :] = x
            lidx[n, g * 8 : g * 8 + 8, :] = ((y + turn) & 7) * 16 + z
        for k in range(3):
            a, b = e1[k].astype(F32), e2[k].astype(F32)
            geo[k, g * 8 : g * 8 + 8, :] = a
            geo[3 + k, g * 8 : g * 8 + 8, :] = b
            geo[6 + k, g * 8 : g * 8 + 8, :] = off[k].astype(F32) + 0.5 * b - 0.5 * a
    for c in range(3):
        frozen[c] = jnp.zeros((tiles, 128), F32)
    zero_plane = jnp.zeros((64, 384), BF16)
    win[0] = zero_plane
    win[11] = zero_plane

    row128 = iota((128, 128), 0)

    def make_onehot(t, carry):
        for n in range(2):
            first = lidx[2 * n, pl.ds(t, 1), :]
            second = lidx[2 * n + 1, pl.ds(t, 1), :]
            sign = 1.0 if n else -1.0
            flat = jnp.where(jnp.logical_or(row128 == first, row128 == second), sign, 0.0).astype(BF16)
            onehot[t, n * 128 : (n + 1) * 128, :] = jnp.transpose(flat)
        return carry

    lax.fori_loop(0, tiles, make_onehot, 0, unroll=4)
    pick = ohg[...].astype(BF16)
    spread_t = jnp.transpose(ohs[...])[0:64, 0:tiles].astype(BF16)
    spread = jnp.concatenate([spread_t, spread_t], axis=1)

    group_bits = [((lane8 >> 4) & bit) != 0 for bit in (1, 2, 4)]
    unroll = [(lane8 + 16 * row8 + 2 + 8 * p) & 127 for p in (0, 1)]
    edge_row = {0: row8 == 7, 1: row8 == 0}
    edge_lane = {0: lane8 == 127, 1: lane8 == 0}
    z_ok = {0: gz == 1, 1: gz == 0}
    my_edge_lane = lane8 == other_edge
    at_edge = lane8 == my_edge

    count = 2 * nx * ny
    me = (gx * ny + gy) * 2 + gz

    xs = [lax.rem(gx + a, nx) for a in range(nx)]
    ys = [lax.rem(gy + b, ny) for b in range(ny)]

    def ring(o, n):
        return min(o, n - o)

    offsets = [(a, b, c) for a in range(nx) for b in range(ny) for c in range(2) if (a, b, c) != (0, 0, 0)]
    offsets.sort(
        key=lambda o: -(ring(o[0] // 4, nx // 4) + ring(o[0] % 4, 4) + ring(o[1], ny))
    )

    def send_squares():
        for a, b, c in offsets:
            pltpu.make_async_remote_copy(
                src_ref=total_row,
                dst_ref=table.at[me],
                send_sem=total_send,
                recv_sem=total_recv,
                device_id=(xs[a], ys[b], 1 - gz if c else gz),
                device_id_type=MESH,
            ).start()

    def hail(semaphore, width):
        for dx in (-width, width):
            cond = gx + dx >= 0 if dx < 0 else gx + dx < nx

            def signal(dx=dx):
                pl.semaphore_signal(
                    semaphore, inc=1, device_id=(gx + dx, gy, gz), device_id_type=MESH
                )

            pl.when(cond)(signal)

    def hear(semaphore, width):
        pl.semaphore_wait(semaphore, (gx >= width).astype(I32) + (gx + width < nx).astype(I32))

    def iteration(it, carry):
        wait_arrivals(displacement_message, it, 2 * it, NEAR)

        beyond_rows = [
            [column(valid(y_ok[dy], rxye[it, lo_hi(dy)]), c) for c in range(3)] for dy in (-1, 1)
        ]
        def make_windows(x):
            for c in range(3):
                if 1 <= x <= 8:
                    own, other = uc[c, x - 1], rxz[it, c, x - 1]
                    rows = [
                        [
                            valid(y_ok[dy], rxy[it, lo_hi(dy), c, x - 1 : x, :]),
                            beyond_rows[lo_hi(dy)][c][x - 1 : x],
                        ]
                        for dy in (-1, 1)
                    ]
                else:
                    dx, xi = (-1, 0) if x == 0 else (1, 1)
                    own = valid(x_ok[dx], rxx[it, xi, c])
                    other = column(valid(x_ok[dx], rxxe[it, xi]), c)
                    rows = [
                        [
                            valid(exists(dx, dy), rxd[it, xi, lo_hi(dy), z, c])
                            for z in (0, 1)
                        ]
                        for dy in (-1, 1)
                    ]
                for s in range(2):
                    near = jnp.where(edge_row[s], rows[s][0], own)
                    far = jnp.where(edge_row[s], rows[s][1], other)
                    pair = []
                    for p in range(2):
                        source = jnp.where(edge_lane[p], jnp.where(z_ok[p], far, 0.0), near)
                        v = pltpu.roll(source, 2 + 8 * p, axis=1, stride=16, stride_axis=0)
                        for bit, mask in zip((1, 2, 4), group_bits):
                            v = jnp.where(mask, pltpu.roll(v, 8 - bit, axis=0), v)
                        pair.append(v)
                    both = jnp.concatenate(pair, axis=0)
                    hi, lo = split(both)
                    win[x + 1, s * 16 : s * 16 + 16, c * 128 : (c + 1) * 128] = hi.astype(BF16)
                    win[x + 1, 32 + s * 16 : 48 + s * 16, c * 128 : (c + 1) * 128] = lo.astype(BF16)

        def hand_out(k):
            both = jnp.concatenate([win[k], win[k + 4]], axis=0)
            gat[k] = jnp.dot(pick, both, preferred_element_type=F32)

        def look_up(n, at, planes, found):
            ks = kidx[n, at, :]
            ls = lidx[n, at, :]
            for k in planes:
                for c in range(3):
                    value = take(gat[k, at, c * 128 : (c + 1) * 128], ls)
                    found[c] = value if found[c] is None else jnp.where(ks == k, value, found[c])
            return found

        for x in range(1, 9):
            make_windows(x)
        for k in (0, 2, 3, 4, 5, 7):
            hand_out(k)
        for g in range(tiles // 8):
            at = pl.ds(g * 8, 8)
            for n in range(4):
                planes = (0, 2, 3, 4, 5, 7) if n == 3 else (2, 3, 4, 5)
                found = look_up(n, at, planes, [None] * 3)
                for c in range(3):
                    early[3 * n + c, at, :] = found[c]

        @pl.when(it > 0)
        def _():
            wait_sends(force_message, it - 1, 2 * it - 1)

        wait_arrivals(displacement_message, it, 2 * it, FAR)
        for x in (0, 9):
            make_windows(x)
        for k in (1, 6):
            hand_out(k)

        @pl.when(it == 2)
        def _():
            hear(hail_four, 4)
            hail(hail_eight, 8)

        live_below = jnp.where(it == 0, 2, 1)

        def pair_forces(g):
            at = pl.ds(pl.multiple_of(g * 8, 8), 8)
            points = []
            for n in range(4):
                found = [early[3 * n + c, at, :] for c in range(3)]
                if n > 0:
                    found = look_up(n, at, (1, 6), found)
                points.append(found)
            one = [points[1][c] - points[0][c] + geo[c, at, :] for c in range(3)]
            two = [points[3][c] - points[2][c] + geo[3 + c, at, :] for c in range(3)]
            apart = [
                0.5 * (points[2][c] + points[3][c]) - 0.5 * (points[0][c] + points[1][c])
                + geo[6 + c, at, :]
                for c in range(3)
            ]
            square = apart[0] * apart[0] + apart[1] * apart[1] + apart[2] * apart[2] + 0.5
            dots = one[0] * two[0] + one[1] * two[1] + one[2] * two[2]
            coupling = 0.5 * dots / (square * jnp.sqrt(square))
            fresh = groups[at, :] < live_below
            values = []
            for c in range(3):
                force = jnp.where(fresh, coupling * apart[c], frozen[c, at, :])
                frozen[c, at, :] = force
                values.extend(split(0.5 * force))
            return tuple(values)

        def spread_forces(g, values):
            for i in range(8):
                t = g * 8 + i
                columns = []
                for n in range(2):
                    mask = jnp.logical_or(
                        row8 == kidx[2 * n, pl.ds(t, 1), :], row8 == kidx[2 * n + 1, pl.ds(t, 1), :]
                    )
                    columns.append(
                        jnp.concatenate(
                            [jnp.where(mask, v[i : i + 1], 0.0) for v in values], axis=0
                        ).astype(BF16)
                    )
                lhs = jnp.concatenate(columns, axis=1)
                got = jnp.dot(lhs, onehot[t], preferred_element_type=F32)
                for c in range(3):
                    outs[c, pl.ds(pl.multiple_of(t * 8, 8), 8), :] = (
                        got[16 * c : 16 * c + 8] + got[16 * c + 8 : 16 * c + 16]
                    )

        def group(g, values):
            later = pair_forces(g)
            spread_forces(g - 1, values)
            return later

        values = lax.fori_loop(1, tiles // 8, group, pair_forces(0), unroll=7)
        spread_forces(tiles // 8 - 1, values)

        def collect(k):
            columns = []
            for c in range(3):
                hi, lo = split(outs[c, pl.ds(k, tiles, stride=8), :])
                columns.append(jnp.concatenate([hi, lo], axis=0).astype(BF16))
            acc[k] = jnp.dot(spread, jnp.concatenate(columns, axis=1), preferred_element_type=F32)

        def fold(x):
            for c in range(3):
                cut = slice(c * 128, (c + 1) * 128)
                parts = []
                for s in range(2):
                    line, beyond = None, None
                    for p in range(2):
                        at = s * 16 + p * 8
                        v = None
                        if x + 1 <= 7:
                            v = acc[x + 1, at : at + 8, cut]
                        if x + 1 >= 4:
                            w = acc[x - 3, 32 + at : 40 + at, cut]
                            v = w if v is None else v + w
                        for bit, mask in zip((1, 2, 4), group_bits):
                            v = jnp.where(mask, pltpu.roll(v, bit, axis=0), v)
                        v = take(v, unroll[p])
                        inside = jnp.where(edge_lane[p], 0.0, v)
                        outside = jnp.where(z_ok[p], v, 0.0)
                        line = inside if line is None else line + inside
                        beyond = outside if beyond is None else beyond + outside
                    parts.append((line, jnp.where(my_edge_lane, beyond, 0.0)))
                for z in range(2):
                    (pz if z else pb)[c, x] = jnp.where(edge_row[0], 0.0, parts[0][z]) + jnp.where(
                        edge_row[1], 0.0, parts[1][z]
                    )
                    ends = (parts[0][z][7:8], parts[1][z][0:1])
                    for yi in range(2):
                        if 1 <= x <= 8:
                            yr[z, yi, c, x - 1 : x, :] = ends[yi]
                        else:
                            fd[z, 0 if x == 0 else 1, yi, c] = ends[yi]

        for k in (1, 6):
            collect(k)
        for x in (0, 9):
            fold(x)
        start(force_message, it, 2 * it + 1, PLAIN_FAR)
        for i in range(2):
            fxe[i] = edges([pz[c, 9 * i] for c in range(3)], other_edge_index)
        start(force_message, it, 2 * it + 1, PACKED_FAR)
        for k in (0, 2, 3, 4, 5, 7):
            collect(k)
        for x in range(1, 9):
            fold(x)
        start(force_message, it, 2 * it + 1, PLAIN_NEAR)
        for i in range(2):
            fye[i] = edges([yr[1, i, c] for c in range(3)], other_edge_index)
        start(force_message, it, 2 * it + 1, PACKED_NEAR)
        wait_sends(displacement_message, it, 2 * it)
        wait_arrivals(force_message, it, 2 * it + 1, NEAR)

        lines = []
        for dy in (-1, 1):
            yi = lo_hi(dy)
            lines.append(
                [
                    valid(
                        y_ok[dy],
                        fry[it, yi, c] + jnp.where(at_edge, column(frye[it, yi], c), 0.0),
                    )
                    for c in range(3)
                ]
            )
        def residual_of(x, squares):
            for c in range(3):
                total = pb[c, x + 1] + frz[it, c, x]
                for dx, xe in ((-1, 0), (1, 7)):
                    if x == xe:
                        xi = lo_hi(dx)
                        total = total + valid(
                            x_ok[dx],
                            frx[it, xi, c] + jnp.where(at_edge, column(frxe[it, xi], c), 0.0),
                        )
                for dy in (-1, 1):
                    yi = lo_hi(dy)
                    line = lines[yi][c][x : x + 1]
                    for dx, xe in ((-1, 0), (1, 7)):
                        if x == xe:
                            xi = lo_hi(dx)
                            line = line + valid(
                                exists(dx, dy),
                                frd[it, xi, yi, 0, c] + frd[it, xi, yi, 1, c],
                            )
                    total = total + jnp.where(row8 == (0 if dy < 0 else 7), line, 0.0)
                r = uc[c, x] - uold[c, x] - 0.5 * total
                squares = squares + r * r
                residuals[c, x] = r
            return squares

        def update(x):
            residual = [residuals[c, x] for c in range(3)]
            for a in range(3):
                fix = jac[a, 0, x] * residual[0] + jac[a, 1, x] * residual[1] + jac[a, 2, x] * residual[2]
                new = uc[a, x] - fix
                uc[a, x] = new
                uy[0, a, x : x + 1, :] = new[0:1]
                uy[1, a, x : x + 1, :] = new[7:8]

        squares = jnp.zeros((8, 128), F32)
        for x in range(1, 7):
            squares = residual_of(x, squares)
        for x in range(1, 7):
            update(x)
        wait_arrivals(force_message, it, 2 * it + 1, FAR)

        @pl.when(it == 1)
        def _():
            hail(hail_four, 4)

        @pl.when(it == 2)
        def _():
            hear(hail_eight, 8)

        for x in (0, 7):
            squares = residual_of(x, squares)
        sq[pl.ds(it, 1), :] = jnp.sum(squares, axis=0, keepdims=True)
        for x in (0, 7):
            update(x)

        @pl.when(it == ITERS - 1)
        def _():
            sums = jnp.sum(sq[...], axis=1, keepdims=True)
            row = jnp.sum(jnp.where(row8 == lane8, sums, 0.0), axis=0, keepdims=True)
            total_row[...] = row
            table[me] = row
            send_squares()

        @pl.when(it < ITERS - 1)
        def _():
            corner_rows()
            send_displacements(it + 1, 2 * it + 2)

        return carry

    sq[...] = jnp.zeros((8, 128), F32)
    for it in range(ITERS):
        iteration(it, 0)
    store_result = pltpu.make_async_copy(uc, uout, in_sem.at[0])
    store_result.start()
    wait_sends(force_message, ITERS - 1, 2 * ITERS - 1)
    others = table.at[0 : count - 1]
    pltpu.make_async_copy(others, others, total_recv).wait()
    pltpu.make_async_copy(others, others, total_send).wait()
    nout[...] = jnp.sum(table[...], axis=0)
    store_result.wait()


def solution(mesh):
    nx, ny = mesh.shape["gx"], mesh.shape["gy"]

    def step(u_old, u_trial, jacobian_inverse, tile_base, pair_codes, pair_groups):
        tiles = tile_base.shape[0]
        cells = float(3 * 8 * 8 * 128 * nx * ny * mesh.shape["gz"])
        smem = pl.BlockSpec(memory_space=pltpu.SMEM)
        v = pltpu.VMEM
        u_final, total = pl.pallas_call(
            functools.partial(kernel, nx, ny),
            out_shape=(
                jax.ShapeDtypeStruct(u_old.shape, F32),
                jax.ShapeDtypeStruct((1, 128), F32),
            ),
            in_specs=[pl.BlockSpec(memory_space=pltpu.HBM)] * 6,
            out_specs=(pl.BlockSpec(memory_space=pl.ANY), pl.BlockSpec(memory_space=pltpu.VMEM)),
            scratch_shapes=[
                pltpu.SMEM(tile_base.shape, I32),
                v(u_old.shape, F32),
                v(jacobian_inverse.shape, F32),
                v(pair_codes.shape, I32),
                v(pair_groups.shape, I32),
                v(u_old.shape, F32),
                v((3, 8, 8, 128), F32),
                v((2, 3, 8, 128), F32),
                v((2, 1, 128), F32),
                v((2, 1, 128), F32),
                v((2, 2, 3, 1, 128), F32),
                v((ITERS, 3, 8, 8, 128), F32),
                v((ITERS, 2, 3, 8, 128), F32),
                v((ITERS, 2, 3, 8, 128), F32),
                v((ITERS, 2, 1, 128), F32),
                v((ITERS, 2, 1, 128), F32),
                v((ITERS, 2, 2, 2, 3, 1, 128), F32),
                v((3, 10, 8, 128), F32),
                v((3, 10, 8, 128), F32),
                v((2, 2, 3, 8, 128), F32),
                v((2, 1, 128), F32),
                v((2, 1, 128), F32),
                v((2, 2, 2, 3, 1, 128), F32),
                v((ITERS, 3, 8, 8, 128), F32),
                v((ITERS, 2, 3, 8, 128), F32),
                v((ITERS, 2, 3, 8, 128), F32),
                v((ITERS, 2, 1, 128), F32),
                v((ITERS, 2, 1, 128), F32),
                v((ITERS, 2, 2, 2, 3, 1, 128), F32),
                v((12, 64, 384), BF16),
                v((8, tiles, 384), F32),
                v((12, tiles, 128), F32),
                v((4, tiles, 128), I32),
                v((4, tiles, 128), I32),
                v((9, tiles, 128), F32),
                v((3, tiles, 128), F32),
                v((tiles, 256, 128), BF16),
                v((tiles, 128), F32),
                v((tiles, 128), F32),
                v((3, tiles * 8, 128), F32),
                v((8, 64, 384), F32),
                v((8, 128), F32),
                v((1, 128), F32),
                v((2 * nx * ny, 1, 128), F32),
                pltpu.SemaphoreType.REGULAR,
                pltpu.SemaphoreType.REGULAR,
                pltpu.SemaphoreType.DMA((6,)),
                pltpu.SemaphoreType.DMA((2 * ITERS, 18)),
                pltpu.SemaphoreType.DMA((2 * ITERS, 18)),
                pltpu.SemaphoreType.DMA,
                pltpu.SemaphoreType.DMA,
            ],
            compiler_params=pltpu.CompilerParams(
                collective_id=0, has_side_effects=True, vmem_limit_bytes=24 * 2**20
            ),
            name="relax",
        )(
            *(
                pltpu.with_memory_space_constraint(a, pltpu.HBM)
                for a in (tile_base, u_old, u_trial, jacobian_inverse, pair_codes, pair_groups)
            )
        )
        return pl.pallas_call(
            functools.partial(finish, cells),
            out_shape=(
                jax.ShapeDtypeStruct(u_old.shape, F32),
                jax.ShapeDtypeStruct((ITERS,), F32),
            ),
            in_specs=[pl.BlockSpec(memory_space=pl.ANY), pl.BlockSpec(memory_space=pltpu.VMEM)],
            out_specs=(pl.BlockSpec(memory_space=pl.ANY), smem),
            scratch_shapes=[pltpu.SemaphoreType.DMA],
            compiler_params=pltpu.CompilerParams(vmem_limit_bytes=2**20),
            name="finish",
        )(u_final, total)

    everywhere = ("gx", "gy", "gz")
    return jax.shard_map(
        step,
        mesh=mesh,
        in_specs=(
            P(None, "gx", "gy", "gz"),
            P(None, "gx", "gy", "gz"),
            P(None, None, "gx", "gy", "gz"),
            P(everywhere),
            P(None, everywhere, None),
            P(everywhere, None),
        ),
        out_specs=(P(None, "gx", "gy", "gz"), P()),
        check_vma=False,
    )
```
